32 devices in a mesh: rep: 2 (over z, core), dp: 16 (over x, y).
Axes of the slice: x: 4, y: 4, z: 1, core: 2. Of those that a mesh axis runs over, the one named last changes fastest.
The devices are a block of a 4x4x8 slice.
Arguments:
- x: bfloat16 [32, 2048, 512], P(('rep', 'dp')), parts along dimension 0
- dy: bfloat16 [32, 2048, 512], P(('rep', 'dp')), parts along dimension 0
- wq: bfloat16 [2, 512, 512], P(None, 'dp')
- wk: bfloat16 [2, 512, 512], P(None, 'dp')
- wv: bfloat16 [2, 512, 512], P(None, 'dp')
- wo: bfloat16 [2, 512, 512], P(None, 'dp')
- w_gate: bfloat16 [2, 512, 2048], P(None, 'dp')
- w_up: bfloat16 [2, 512, 2048], P(None, 'dp')
- w_down: bfloat16 [2, 2048, 512], P(None, 'dp')
- m_wq: float32 [2, 512, 512], P(None, 'dp')
- m_wk: float32 [2, 512, 512], P(None, 'dp')
- m_wv: float32 [2, 512, 512], P(None, 'dp')
- m_wo: float32 [2, 512, 512], P(None, 'dp')
- m_w_gate: float32 [2, 512, 2048], P(None, 'dp')
- m_w_up: float32 [2, 512, 2048], P(None, 'dp')
- m_w_down: float32 [2, 2048, 512], P(None, 'dp')
- v_wq: float32 [2, 512, 512], P(None, 'dp')
- v_wk: float32 [2, 512, 512], P(None, 'dp')
- v_wv: float32 [2, 512, 512], P(None, 'dp')
- v_wo: float32 [2, 512, 512], P(None, 'dp')
- v_w_gate: float32 [2, 512, 2048], P(None, 'dp')
- v_w_up: float32 [2, 512, 2048], P(None, 'dp')
- v_w_down: float32 [2, 2048, 512], P(None, 'dp')
Outputs:
- output 1: bfloat16 [4, 512, 512], P('rep', 'dp'), parts along dimension 0
- output 2: bfloat16 [4, 512, 512], P('rep', 'dp'), parts along dimension 0
- output 3: bfloat16 [4, 512, 512], P('rep', 'dp'), parts along dimension 0
- output 4: bfloat16 [4, 512, 512], P('rep', 'dp'), parts along dimension 0
- output 5: bfloat16 [4, 512, 2048], P('rep', 'dp'), parts along dimension 0
- output 6: bfloat16 [4, 512, 2048], P('rep', 'dp'), parts along dimension 0
- output 7: bfloat16 [4, 2048, 512], P('rep', 'dp'), parts along dimension 0
- output 8: float32 [4, 512, 512], P('rep', 'dp'), parts along dimension 0
- output 9: float32 [4, 512, 512], P('rep', 'dp'), parts along dimension 0
- output 10: float32 [4, 512, 512], P('rep', 'dp'), parts along dimension 0
- output 11: float32 [4, 512, 512], P('rep', 'dp'), parts along dimension 0
- output 12: float32 [4, 512, 2048], P('rep', 'dp'), parts along dimension 0
- output 13: float32 [4, 512, 2048], P('rep', 'dp'), parts along dimension 0
- output 14: float32 [4, 2048, 512], P('rep', 'dp'), parts along dimension 0
- output 15: float32 [4, 512, 512], P('rep', 'dp'), parts along dimension 0
- output 16: float32 [4, 512, 512], P('rep', 'dp'), parts along dimension 0
- output 17: float32 [4, 512, 512], P('rep', 'dp'), parts along dimension 0
- output 18: float32 [4, 512, 512], P('rep', 'dp'), parts along dimension 0
- output 19: float32 [4, 512, 2048], P('rep', 'dp'), parts along dimension 0
- output 20: float32 [4, 512, 2048], P('rep', 'dp'), parts along dimension 0
- output 21: float32 [4, 2048, 512], P('rep', 'dp'), parts along dimension 0
There are 2 independent parts. The reference program is written for one: setup_inputs(seed, part) draws one part's arguments, and reference() takes and returns one part's arrays. A program takes and returns all parts, laid end to end along the dimension named above; an argument that names none is the same for every part.
All inputs are finite; a program needn't handle non-finite values.
Results may differ from the reference program's by a relative error of at most 0.024.
Values are sent between devices in bfloat16 or wider.
A program may use at most 768 MiB of HBM per device.

```python
import jax
import jax.numpy as jnp
from jax import lax

SEQUENCES = 16
TOKENS = 2048
D = 512
HEADS = 2
KV_HEADS = 2
HEAD = 256
FF = 2048
LAYERS = 2
THETA = 10000
NAMES = ("wq", "wk", "wv", "wo", "w_gate", "w_up", "w_down")
SHAPES = {
    "wq": (LAYERS, D, HEADS * HEAD),
    "wk": (LAYERS, D, KV_HEADS * HEAD),
    "wv": (LAYERS, D, KV_HEADS * HEAD),
    "wo": (LAYERS, HEADS * HEAD, D),
    "w_gate": (LAYERS, D, FF),
    "w_up": (LAYERS, D, FF),
    "w_down": (LAYERS, FF, D),
}


def bump(key, n, height):
    away = (jnp.arange(n, dtype=jnp.int32) - jax.random.randint(key, (), 0, n, jnp.int32)) % n
    return jnp.where(away < n // 8, height, 1.0)


def together(key, own, strength):
    shared = jax.random.normal(key, own.shape[1:], jnp.float32)
    return (own + strength * shared) * lax.rsqrt(1 + strength * strength)


def setup_inputs(seed: int = 0, part: int = 0) -> dict:
    kx, kdy, ka, kb, kz, kf, kh, kl, *keys = jax.random.split(jax.random.key(seed), 8 + 3 * len(NAMES))
    kx, kdy, ka, kb = (jax.random.fold_in(k, part) for k in (kx, kdy, ka, kb))
    kw, km, kv = (keys[i::3] for i in range(3))
    shape = (SEQUENCES, TOKENS, D)
    much_x, much_dy = jax.random.uniform(kz, (2,), jnp.float32, 0.0, 1.0)
    loud = 2.0 ** jax.random.uniform(jax.random.fold_in(kz, 1), (), jnp.float32, -1.0, 2.0)
    layers = 2.0 ** jax.random.uniform(kl, (LAYERS, 1, 1), jnp.float32, -1.0, 1.0)
    times = {"wq": 1.0, "wk": 1.0, "wv": 2.0, "wo": layers, "w_gate": 1.0, "w_up": bump(kh, FF, 4.0), "w_down": layers}
    x = together(ka, jax.random.normal(kx, shape, jnp.float32), much_x) * bump(kf, D, 4.0)
    dy = together(kb, jax.random.normal(kdy, shape, jnp.float32), much_dy)
    drawn = {"x": x.astype(jnp.bfloat16), "dy": (loud * dy * (SEQUENCES * TOKENS) ** -0.5).astype(jnp.bfloat16)}
    for key, name in zip(kw, NAMES, strict=True):
        drawn[name] = (jax.random.normal(key, SHAPES[name], jnp.float32) * SHAPES[name][1] ** -0.5 * times[name]).astype(jnp.bfloat16)
    for key, name in zip(km, NAMES, strict=True):
        drawn[f"m_{name}"] = 0.1 * jax.random.normal(key, SHAPES[name], jnp.float32)
    for key, name in zip(kv, NAMES, strict=True):
        drawn[f"v_{name}"] = jax.random.uniform(key, SHAPES[name], jnp.float32, 0.02, 0.06)
    return drawn


def matmul(a, w):
    return jnp.dot(a, w, preferred_element_type=jnp.float32).astype(jnp.bfloat16)


def normed(h):
    wide = h.astype(jnp.float32)
    scale = lax.rsqrt(jnp.mean(wide**2, -1, keepdims=True) + 1e-6)
    return (wide * scale).astype(jnp.bfloat16)


def turned(t, theta):
    half = t.shape[-1] // 2
    angle = jnp.arange(t.shape[0], dtype=jnp.float32)[:, None] * theta ** (-jnp.arange(half, dtype=jnp.float32) / half)
    cos, sin = jnp.cos(angle)[:, None], jnp.sin(angle)[:, None]
    a, b = t[..., :half].astype(jnp.float32), t[..., half:].astype(jnp.float32)
    return jnp.concatenate([a * cos - b * sin, b * cos + a * sin], -1).astype(jnp.bfloat16)


def seen_by(q, k, v):
    tokens, kv = q.shape[0], k.shape[1]
    q = q.reshape(tokens, kv, -1, q.shape[-1])
    scores = jnp.einsum("tgsd,ugd->gstu", q.astype(jnp.float32), k.astype(jnp.float32)) * q.shape[-1] ** -0.5
    place = jnp.arange(tokens)
    weights = jax.nn.softmax(jnp.where(place[:, None] >= place, scores, -jnp.inf), -1).astype(jnp.bfloat16)
    return jnp.einsum("gstu,ugd->tgsd", weights.astype(jnp.float32), v.astype(jnp.float32)).astype(jnp.bfloat16).reshape(tokens, -1)


def layer(h, w):
    a = normed(h)
    q, k = (turned(matmul(a, w[name]).reshape(h.shape[0], -1, HEAD), THETA) for name in ("wq", "wk"))
    h = h + matmul(seen_by(q, k, matmul(a, w["wv"]).reshape(h.shape[0], -1, HEAD)), w["wo"])
    b = normed(h)
    gate = jnp.dot(b, w["w_gate"], preferred_element_type=jnp.float32)
    up = jnp.dot(b, w["w_up"], preferred_element_type=jnp.float32)
    return h + matmul((jax.nn.silu(gate) * up).astype(jnp.bfloat16), w["w_down"])


def adamw(w, m, v, g):
    m = 0.9 * m + 0.1 * g
    v = 0.95 * v + 0.05 * g * g
    step = m * lax.rsqrt(v + 1e-8) + 0.1 * w
    return (w - 0.02 * step).astype(jnp.bfloat16), m, v


def clipped(gradients, sum_of_squares, count):
    factor = jnp.minimum(1.0, 0.5 * lax.rsqrt(sum_of_squares / count + 1e-30))
    return [g * factor for g in gradients]


def stack(weights, h):
    return lax.scan(lambda h, w: (layer(h, w), None), h, weights)[0]


def reference(x, dy, wq, wk, wv, wo, w_gate, w_up, w_down, m_wq, m_wk, m_wv, m_wo, m_w_gate, m_w_up, m_w_down, v_wq, v_wk, v_wv, v_wo, v_w_gate, v_w_up, v_w_down):
    weights = dict(zip(NAMES, (wq, wk, wv, wo, w_gate, w_up, w_down), strict=True))

    def take(so_far, sequence):
        h, by_y = sequence
        _, back = jax.vjp(stack, weights, h)
        by_weights, by_h = back(by_y)
        return jax.tree.map(lambda total, term: total + term.astype(jnp.float32), so_far, by_weights), by_h

    none_yet = {name: jnp.zeros(w.shape, jnp.float32) for name, w in weights.items()}
    by_weights, by_x = lax.scan(take, none_yet, (x, dy))
    gradients = [by_weights[name].astype(jnp.bfloat16).astype(jnp.float32) for name in NAMES]
    gradients = clipped(gradients, sum(jnp.sum(g * g) for g in gradients), sum(g.size for g in gradients))
    first = (m_wq, m_wk, m_wv, m_wo, m_w_gate, m_w_up, m_w_down)
    second = (v_wq, v_wk, v_wv, v_wo, v_w_gate, v_w_up, v_w_down)
    new = [adamw(weights[name].astype(jnp.float32), m, v, g) for name, m, v, g in zip(NAMES, first, second, gradients, strict=True)]
    return tuple(one[which] for which in range(3) for one in new)
```

```python
import functools
import jax
import jax.numpy as jnp
import numpy as np
from jax import lax
from jax.experimental import pallas as pl
from jax.experimental.pallas import tpu as pltpu

HEAD = 256
THETA = 10000
LOG2E = 1.4426950408889634
VMEM = 60 * 2**20
EPS = 1e-6
F32, BF16 = jnp.float32, jnp.bfloat16


def dot(a, b, ca=1, cb=0):
    return lax.dot_general(a, b, (((ca,), (cb,)), ((), ())), preferred_element_type=F32)


def scale_of(h):
    return lax.rsqrt(jnp.mean(h * h, -1, keepdims=True) + EPS)


def rotated(t, cos, sin):
    half = t.shape[-1] // 2
    a, b = t[:, :half], t[:, half:]
    return jnp.concatenate([a * cos - b * sin, b * cos + a * sin], -1)


def heads_of(width):
    return [slice(at, at + HEAD) for at in range(0, width, HEAD)]


def hidden(rows, cols):
    return lax.broadcasted_iota(jnp.int32, (rows, cols), 0) > lax.broadcasted_iota(jnp.int32, (rows, cols), 1)


MESH = pl.DeviceIdType.MESH
ANY = pl.BlockSpec(memory_space=pl.ANY)


class Place:
    def __init__(self, side):
        rep, me = lax.axis_index("rep"), lax.axis_index("dp")
        self.side, self.x, self.y, self.core = side, lax.div(me, side), lax.rem(me, side), lax.rem(rep, 2)
        self.partner = {"rep": rep + 1 - 2 * self.core}

    def on(self, axis, k):
        at = lax.rem((self.x, self.y)[axis] + k, self.side)
        return at, {"dp": at * self.side + self.y if axis == 0 else self.x * self.side + at}


def remote(src, dst, send, recv, device):
    return pltpu.make_async_remote_copy(src_ref=src, dst_ref=dst, send_sem=send, recv_sem=recv, device_id=device, device_id_type=MESH)


class Gather:
    stages = 5

    def __init__(self, side, layer, pieces, by_rows):
        self.side, self.pieces, self.by_rows = side, pieces, by_rows
        self.ins = [p for group in pieces for p in group]
        self.in_specs = [pl.BlockSpec((1, *p.shape[1:]), functools.partial(lambda layer, *_: (layer, 0, 0), layer)) for p in self.ins]
        self.outs = [jax.ShapeDtypeStruct((side, side, g[0].shape[1], sum(p.shape[2] for p in g)), g[0].dtype) for g in pieces]
        self.peers = side - 1
        n = len(pieces)
        self.scratch = [pltpu.SemaphoreType.DMA((len(self.ins),)), pltpu.SemaphoreType.DMA((n, 2, 4, self.peers)),
                        pltpu.SemaphoreType.DMA((n, 2, 4, self.peers))]
        self.partner = True

    def results(self, outs):
        return [o.reshape(-1, o.shape[-1]) for o in outs]

    def run(self, stage, place, ins, outs, scratch):
        local, send, recv = scratch
        copies = []
        at = 0
        for group, out in zip(self.pieces, outs, strict=True):
            column = 0
            for p in group:
                copies.append((ins[at].at[0], out.at[place.x, place.y, :, column : column + p.shape[2]], local.at[at]))
                column, at = column + p.shape[2], at + 1
        if stage == 0:
            for c in copies:
                pltpu.make_async_copy(*c).start()
            return
        first, second, near, far = [], [], [], []
        come = [[], [], [], []]
        for n, out in enumerate(outs):
            size = out.shape[2] if self.by_rows[n] else out.shape[3]
            for q in range(2):
                def view(x, y, core, out=out, n=n, q=q, size=size):
                    piece = pl.ds(pl.multiple_of(core * (size // 2) + q * (size // 4), size // 4), size // 4)
                    return out.at[x, y, piece, :] if self.by_rows[n] else out.at[x, y, :, piece]

                a, b = q, 1 - q
                every = slice(None)
                here = view(place.x, place.y, place.core)
                line = (every, place.y) if a == 0 else (place.x, every)
                for k in range(1, self.side):
                    s = lambda kind: (send.at[n, q, kind, k - 1], recv.at[n, q, kind, k - 1])
                    _, to = place.on(a, k)
                    first.append((here, here, *s(0), to))
                    back, _ = place.on(a, self.side - k)
                    got = view(*((back, place.y) if a == 0 else (place.x, back)), place.core)
                    come[0].append((got, got, *s(0), to))
                    near.append((got, got, *s(2), place.partner))
                    got = view(*((back, place.y) if a == 0 else (place.x, back)), 1 - place.core)
                    come[2].append((got, got, *s(2), place.partner))
                    _, to = place.on(b, k)
                    mine = view(*line, place.core)
                    second.append((mine, mine, *s(1), to))
                    back, _ = place.on(b, self.side - k)
                    got = view(*((every, back) if a == 0 else (back, every)), place.core)
                    come[1].append((got, got, *s(1), to))
                    far.append((got, got, *s(3), place.partner))
                    got = view(*((every, back) if a == 0 else (back, every)), 1 - place.core)
                    come[3].append((got, got, *s(3), place.partner))
        if stage == 1:
            for c in copies:
                pltpu.make_async_copy(*c).wait()
            for c in first:
                remote(*c).start()
        elif stage == 2:
            for c in come[0]:
                remote(*c).wait_recv()
            for c in second + near:
                remote(*c).start()
        elif stage == 3:
            for c, f in zip(come[1], far, strict=True):
                remote(*c).wait_recv()
                remote(*f).start()
        else:
            for c in come[2] + come[3]:
                remote(*c).wait_recv()
            for c in first + second + near + far:
                remote(*c).wait_send()


class Scatter:
    stages = 2
    partner = False

    def __init__(self, side, arrays):
        self.side = side
        self.first = [not isinstance(a, tuple) for a in arrays]
        self.ins = [part for a in arrays for part in (a if isinstance(a, tuple) else (a,))]
        self.in_specs = [ANY] * len(self.ins)
        self.outs = []
        for a in arrays:
            if isinstance(a, tuple):
                self.outs += [jax.ShapeDtypeStruct((side - 1, *p.shape[1:]), p.dtype) for p in a]
            else:
                self.outs += [jax.ShapeDtypeStruct((side - 1, side, a.shape[2], a.shape[3] // 2), a.dtype)] * 2
        n = len(arrays)
        self.scratch = [pltpu.SemaphoreType.DMA((n, 2, side - 1)), pltpu.SemaphoreType.DMA((n, 2, side - 1))]

    def results(self, outs):
        return [tuple(outs[n : n + 2]) for n in range(0, len(outs), 2)]

    def run(self, stage, place, ins, outs, scratch):
        send, recv = scratch
        copies, at = [], 0
        for n, first in enumerate(self.first):
            for q in range(2):
                for k in range(1, self.side):
                    there, to = place.on(q if first else 1 - q, k)
                    if first:
                        half = ins[at].shape[3] // 2
                        columns = slice(q * half, (q + 1) * half)
                        src = ins[at].at[there, :, :, columns] if q == 0 else ins[at].at[:, there, :, columns]
                    else:
                        src = ins[at + q].at[there]
                    copies.append(remote(src, outs[2 * n + q].at[k - 1], send.at[n, q, k - 1], recv.at[n, q, k - 1], to))
            at += 1 if first else 2
        for c in copies:
            c.start() if stage == 0 else c.wait()


def call(body, side, cid, *, grid, ins, in_specs, outs, out_specs, scratch, name, comms=(), barrier=0):
    steps = grid[0]
    parts = [c for c, _ in comms]
    counts = [len(ins), *(len(c.ins) for c in parts), len(outs), *(len(c.outs) for c in parts), len(scratch), *(len(c.scratch) for c in parts)]
    partner = any(c.partner for c in parts)

    def kernel(*refs):
        split, at = [], 0
        for n in counts:
            split.append(refs[at : at + n])
            at += n
        m = len(parts)
        my_in, c_in, my_out, c_out, my_s, c_s = (split[0], split[1 : m + 1], split[m + 1], split[m + 2 : 2 * m + 2], split[2 * m + 2], split[2 * m + 3 :])
        step = pl.program_id(0)

        def events(now):
            todo = [(n, s) for n, (_, when) in enumerate(comms) for s, t in enumerate(when) if t == now]
            if not comms or not (todo or now in (0, barrier)):
                return

            @pl.when(step == int(now))
            def _():
                place = Place(side)
                devices = [place.on(axis, k)[1] for axis in (0, 1) for k in range(1, side)] + [place.partner] * partner
                if now == 0:
                    for device in devices:
                        pl.semaphore_signal(pltpu.get_barrier_semaphore(), inc=1, device_id=device, device_id_type=MESH)
                early = [(n, s) for n, s in todo if s == 0 and parts[n].stages > 2]
                for n, s in early:
                    parts[n].run(s, place, c_in[n], c_out[n], c_s[n])
                if now == barrier:
                    pl.semaphore_wait(pltpu.get_barrier_semaphore(), len(devices))
                for n, s in todo:
                    if (n, s) not in early:
                        parts[n].run(s, place, c_in[n], c_out[n], c_s[n])

        for s in range(steps):
            events(s)
        if body is not None:
            body(*my_in, *my_out, *my_s)
        for s in range(steps):
            events(s + 0.5)

    got = pl.pallas_call(
        kernel,
        grid=grid,
        in_specs=[*in_specs, *(s for c in parts for s in c.in_specs)],
        out_specs=[*out_specs, *([ANY] * sum(len(c.outs) for c in parts))],
        out_shape=[*outs, *(o for c in parts for o in c.outs)],
        scratch_shapes=[*scratch, *(s for c in parts for s in c.scratch)],
        compiler_params=pltpu.CompilerParams(dimension_semantics=("arbitrary",), vmem_limit_bytes=VMEM, has_side_effects=bool(comms),
                                             **({"collective_id": cid} if comms else {})),
        name=name,
    )(*ins, *(a for c in parts for a in c.ins))
    given, at, results = list(got[: len(outs)]), len(outs), []
    for c in parts:
        results.append(c.results(got[at : at + len(c.outs)]))
        at += len(c.outs)
    return given, results


def attn_fwd_body(h_ref, w_ref, cos_ref, sin_ref, qkv_ref, o_ref, lse_ref, k_s, vt_s, top_s, mix_s):
    i = pl.program_id(0)
    bq, d = h_ref.shape
    width = o_ref.shape[1]
    hs = heads_of(width)

    @pl.when(i == 0)
    def _():
        for n in range(len(hs)):
            vt_s[n, HEAD:, :] = jnp.ones((8, vt_s.shape[2]), BF16)

    h = h_ref[...].astype(F32)
    a = (h * scale_of(h)).astype(BF16)
    t = dot(a, w_ref[:, : 3 * width]).astype(BF16)
    cos, sin = cos_ref[...], sin_ref[...]
    here = pl.ds(pl.multiple_of(i * bq, bq), bq)
    qs = []
    for n, at in enumerate(hs):
        q = rotated(t[:, at].astype(F32), cos, sin).astype(BF16) * jnp.asarray(HEAD**-0.5, BF16)
        k = rotated(t[:, width + at.start : width + at.stop].astype(F32), cos, sin).astype(BF16)
        v = t[:, 2 * width + at.start : 2 * width + at.stop]
        qkv_ref[:, at] = q
        qkv_ref[:, width + at.start : width + at.stop] = k
        qkv_ref[:, 2 * width + at.start : 2 * width + at.stop] = v
        k_s[here, at] = k
        vt_s[n, :HEAD, here] = v.T
        qs.append(q)

    def block(j, first):
        keys = pl.ds(pl.multiple_of(j * bq, bq), bq)
        scores = [dot(k_s[keys, at], q, 1, 1) for at, q in zip(hs, qs)]
        ps, keeps = [], []
        for n, s in enumerate(scores):
            if first:
                s = jnp.where(hidden(bq, bq), -1e30, s)
                top = s.max(0, keepdims=True)
            else:
                old = top_s[n : n + 1, :]
                top = jnp.maximum(old, s.max(0, keepdims=True))
                keeps.append(jnp.exp2((old - top) * LOG2E))
            top_s[n : n + 1, :] = top
            ps.append(jnp.exp2((s - top) * LOG2E).astype(BF16))
        for n, p in enumerate(ps):
            new = dot(vt_s[n, :, keys], p)
            mix_s[n] = new if first else mix_s[n] * keeps[n] + new

    block(i, True)
    lax.fori_loop(0, i, lambda j, _: block(j, False), None)
    for n, at in enumerate(hs):
        total = mix_s[n, HEAD : HEAD + 1, :]
        o_ref[:, at] = (mix_s[n, :HEAD, :] * (1 / total)).T.astype(BF16)
        lse_ref[n : n + 1, :] = top_s[n : n + 1, :] * LOG2E + jnp.log2(total)


def whole(shape):
    return pl.BlockSpec(shape, lambda *_: (0,) * len(shape), pipeline_mode=pl.Buffered(1))


def rows(n, width, back=None):
    return pl.BlockSpec((n, width), (lambda i: (i, 0)) if back is None else (lambda i: (back - 1 - i, 0)))


def attn_fwd(run, h, w, cos, sin, bq=512, **kw):
    t, d = h.shape
    width = w.shape[1] // 4
    nh = width // HEAD
    sd = jax.ShapeDtypeStruct
    return run(
        attn_fwd_body,
        grid=(t // bq,),
        ins=[h, w, cos, sin],
        in_specs=[rows(bq, d), whole(w.shape), rows(bq, HEAD // 2), rows(bq, HEAD // 2)],
        outs=[sd((t, 3 * width), BF16), sd((t, width), BF16), sd((nh, t), F32)],
        out_specs=[rows(bq, 3 * width), rows(bq, width), pl.BlockSpec((nh, bq), lambda i: (0, i))],
        scratch=[pltpu.VMEM((t, width), BF16), pltpu.VMEM((nh, HEAD + 8, t), BF16), pltpu.VMEM((nh, bq), F32),
                 pltpu.VMEM((nh, HEAD + 8, bq), F32)],
        name="attn_fwd",
        **kw,
    )


def ffn_fwd_body(h_ref, o_ref, wa_ref, wgu_ref, wd_ref, h1_ref, h2_ref, act_s, *, step):
    width, f = o_ref.shape[1], wd_ref.shape[0]
    h1 = h_ref[...] + dot(o_ref[...], wa_ref[:, 3 * width :]).astype(BF16)
    h1_ref[...] = h1
    wide = h1.astype(F32)
    b = (wide * scale_of(wide)).astype(BF16)
    for c in range(0, f, step):
        gate = dot(b, wgu_ref[:, c : c + step])
        up = dot(b, wgu_ref[:, f + c : f + c + step])
        act_s[:, c : c + step] = (gate * jax.nn.sigmoid(gate) * up).astype(BF16)
    h2_ref[...] = h1 + dot(act_s[...], wd_ref[...]).astype(BF16)


def ffn_fwd(run, h, o, wa, wgu, wd, bq=512, step=512, **kw):
    t, d = h.shape
    f = wd.shape[0]
    return run(
        functools.partial(ffn_fwd_body, step=step),
        grid=(t // bq,),
        ins=[h, o, wa, wgu, wd],
        in_specs=[rows(bq, d), rows(bq, o.shape[1]), whole(wa.shape), whole(wgu.shape), whole(wd.shape)],
        outs=[jax.ShapeDtypeStruct((t, d), BF16)] * 2,
        out_specs=[rows(bq, d), rows(bq, d)],
        scratch=[pltpu.VMEM((bq, f), BF16)],
        name="ffn_fwd",
        **kw,
    )


def normed_bwd(y, r, by):
    return r * (by - y * jnp.mean(by * y, -1, keepdims=True))


def ffn_bwd_body(h_ref, o_ref, g_ref, wa_ref, wgu_ref, wd_ref, dh1_ref, do_ref, dwo_ref, dwgu_ref, dwd_ref, act_s, dgu_s, wo_a, wgu_a, wd_a,
                 *, step, fwd):
    width, f = o_ref.shape[1], wd_ref.shape[0]
    i = pl.program_id(0)
    first = i == 0

    @pl.when(first)
    def _():
        wo_a[...] = jnp.zeros_like(wo_a)
        wgu_a[...] = jnp.zeros_like(wgu_a)
        wd_a[...] = jnp.zeros_like(wd_a)

    wo = wa_ref[:, 3 * width :]
    h1 = h_ref[...]
    if fwd:
        h1 = h1 + dot(o_ref[...], wo).astype(BF16)
    wide = h1.astype(F32)
    r = scale_of(wide)
    y = wide * r
    b = y.astype(BF16)
    g = g_ref[...]
    for c in range(0, f, step):
        gate = dot(b, wgu_ref[:, c : c + step])
        up = dot(b, wgu_ref[:, f + c : f + c + step])
        dact = dot(g, wd_ref[c : c + step, :], 1, 1)
        sig = jax.nn.sigmoid(gate)
        silu = gate * sig
        act_s[:, c : c + step] = (silu * up).astype(BF16)
        dgu_s[:, c : c + step] = (dact * up * (sig + silu * (1 - sig))).astype(BF16)
        dgu_s[:, f + c : f + c + step] = (dact * silu).astype(BF16)
    by = dot(dgu_s[...], wgu_ref[...], 1, 1)
    bt, gt = b.T, g.T
    for c in range(0, 2 * f, step):
        wgu_a[:, c : c + step] += dot(bt, dgu_s[:, c : c + step])
    for c in range(0, f, step):
        wd_a[:, c : c + step] += dot(gt, act_s[:, c : c + step])
    dh1 = (g.astype(F32) + normed_bwd(y, r, by)).astype(BF16)
    dh1_ref[...] = dh1
    do_ref[...] = dot(dh1, wo, 1, 1).astype(BF16)
    wo_a[...] += dot(o_ref[...].T, dh1)

    @pl.when(i == pl.num_programs(0) - 1)
    def _():
        dwo_ref[...] = wo_a[...].astype(BF16)
        dwgu_ref[...] = wgu_a[...].astype(BF16)
        for c in range(0, f, step):
            dwd_ref[c : c + step, :] = wd_a[:, c : c + step].T.astype(BF16)


def ffn_bwd(run, h, o, g, wa, wgu, wd, fwd, bq=512, step=512, **kw):
    t, d = h.shape
    f, width = wd.shape[0], o.shape[1]
    sd = jax.ShapeDtypeStruct
    return run(
        functools.partial(ffn_bwd_body, step=step, fwd=fwd),
        grid=(t // bq,),
        ins=[h, o, g, wa, wgu, wd],
        in_specs=[rows(bq, d), rows(bq, width), rows(bq, d), whole(wa.shape), whole(wgu.shape), whole(wd.shape)],
        out_specs=[rows(bq, d), rows(bq, width), whole((width, d)), whole(wgu.shape), whole(wd.shape)],
        outs=[sd((t, d), BF16), sd((t, width), BF16), sd((width, d), BF16), sd(wgu.shape, BF16), sd(wd.shape, BF16)],
        scratch=[pltpu.VMEM((bq, f), BF16), pltpu.VMEM((bq, 2 * f), BF16), pltpu.VMEM((width, d), F32), pltpu.VMEM(wgu.shape, F32),
                 pltpu.VMEM((d, f), F32)],
        name="ffn_bwd",
        **kw,
    )


def attn_bwd_body(qkv_ref, h_ref, dh1_ref, o_ref, do_ref, lse_ref, w_ref, cos_ref, sin_ref, *rest, more):
    dh_ref, rest = (rest[0], rest[1:]) if more else (None, rest)
    dw_ref, kt_s, dq_s, dk_s, dv_s, dt_s, dw_a = rest
    step, n = pl.program_id(0), pl.num_programs(0)
    i = n - 1 - step
    bq, d = h_ref.shape
    width = o_ref.shape[1]
    hs = heads_of(width)

    @pl.when(step == 0)
    def _():
        dk_s[...] = jnp.zeros_like(dk_s)
        dv_s[...] = jnp.zeros_like(dv_s)
        dw_a[...] = jnp.zeros_like(dw_a)
        for j in range(0, kt_s.shape[2], bq):
            for m, at in enumerate(hs):
                kt_s[m, :, j : j + bq] = qkv_ref[j : j + bq, width + at.start : width + at.stop].T

    here = pl.ds(pl.multiple_of(i * bq, bq), bq)
    qs = [qkv_ref[here, at] for at in hs]
    dos = [do_ref[:, at] for at in hs]
    deltas = []
    for m, at in enumerate(hs):
        delta = (dos[m].astype(F32) * o_ref[:, at].astype(F32)).sum(-1, keepdims=True)
        deltas.append(jnp.broadcast_to(delta, (bq, 128)).T[:1, :])
    lses = [lse_ref[m : m + 1, :] for m in range(len(hs))]

    def block(j, first):
        keys = pl.ds(pl.multiple_of(j * bq, bq), bq)
        scores = [dot(qkv_ref[keys, width + at.start : width + at.stop], q, 1, 1) for at, q in zip(hs, qs)]
        dps = [dot(qkv_ref[keys, 2 * width + at.start : 2 * width + at.stop], x, 1, 1) for at, x in zip(hs, dos)]
        for m, at in enumerate(hs):
            p = jnp.exp2(scores[m] * LOG2E - lses[m])
            if first:
                p = jnp.where(hidden(bq, bq), 0.0, p)
            ds = (p * (dps[m] - deltas[m])).astype(BF16)
            dv_s[keys, at] += dot(p.astype(BF16), dos[m])
            dk_s[keys, at] += dot(ds, qs[m])
            dq = dot(kt_s[m, :, keys], ds)
            dq_s[m] = dq if first else dq_s[m] + dq

    block(i, True)
    lax.fori_loop(0, i, lambda j, _: block(j, False), None)
    cos, sin = cos_ref[...], -sin_ref[...]
    for m, at in enumerate(hs):
        dt_s[:, at] = rotated((dq_s[m] * HEAD**-0.5).T, cos, sin).astype(BF16)
        dt_s[:, width + at.start : width + at.stop] = rotated(dk_s[here, at], cos, sin).astype(BF16)
        dt_s[:, 2 * width + at.start : 2 * width + at.stop] = dv_s[here, at].astype(BF16)
    h = h_ref[...].astype(F32)
    r = scale_of(h)
    y = h * r
    dw_a[...] += dot(y.astype(BF16).T, dt_s[...])
    if more:
        by = dot(dt_s[...], w_ref[:, : 3 * width], 1, 1)
        dh_ref[...] = (dh1_ref[...].astype(F32) + normed_bwd(y, r, by)).astype(BF16)

    @pl.when(step == n - 1)
    def _():
        dw_ref[...] = dw_a[...].astype(BF16)


def attn_bwd(run, qkv, h, dh1, o, do, lse, w, cos, sin, more, bq=512, **kw):
    t, d = h.shape
    width = o.shape[1]
    nh, n = width // HEAD, t // bq
    sd = jax.ShapeDtypeStruct
    back = lambda wd: rows(bq, wd, n)
    out, got = run(
        functools.partial(attn_bwd_body, more=more),
        grid=(n,),
        ins=[qkv, h, dh1, o, do, lse, w, cos, sin],
        in_specs=[whole(qkv.shape), back(d), back(d), back(width), back(width), pl.BlockSpec((nh, bq), lambda i: (0, n - 1 - i)), whole(w.shape),
                  back(HEAD // 2), back(HEAD // 2)],
        out_specs=[back(d)] * more + [whole((d, 3 * width))],
        outs=[sd((t, d), BF16)] * more + [sd((d, 3 * width), BF16)],
        scratch=[pltpu.VMEM((nh, HEAD, t), BF16), pltpu.VMEM((nh, HEAD, bq), F32), pltpu.VMEM((t, width), F32), pltpu.VMEM((t, width), F32),
                        pltpu.VMEM((bq, 3 * width), BF16), pltpu.VMEM((d, 3 * width), F32)],
        name="attn_bwd",
        **kw,
    )
    return ([] if more else [None]) + out, got


def tables(tokens):
    half = HEAD // 2
    angle = np.arange(tokens, dtype=np.float32)[:, None] * np.float32(THETA) ** (-np.arange(half, dtype=np.float32) / np.float32(half))
    return jnp.asarray(np.cos(angle), F32), jnp.asarray(np.sin(angle), F32)


from jax.sharding import PartitionSpec as P

NAMES = ("wq", "wk", "wv", "wo", "w_gate", "w_up", "w_down")


def shared_sum(run, part, n):
    def body(part_ref, total_ref, slots, send, recv):
        me = lax.axis_index("dp")
        others = [{"dp": lax.rem(me + k, n)} for k in range(1, n)]
        barrier = pltpu.get_barrier_semaphore()
        for device in others:
            pl.semaphore_signal(barrier, inc=1, device_id=device, device_id_type=MESH)
        pl.semaphore_wait(barrier, n - 1)
        copies = [remote(part_ref, slots.at[me], send.at[k], recv.at[k], device) for k, device in enumerate(others)]
        for c in copies:
            c.start()
        slots[me] = part_ref[...]
        for k, c in enumerate(copies):
            remote(part_ref, slots.at[lax.rem(me + n - k - 1, n)], send.at[k], recv.at[k], others[k]).wait_recv()
            c.wait_send()
        total_ref[...] = slots[...].sum(0)

    return pl.pallas_call(
        body,
        in_specs=[pl.BlockSpec(memory_space=pltpu.VMEM)],
        out_specs=pl.BlockSpec(memory_space=pltpu.VMEM),
        out_shape=jax.ShapeDtypeStruct(part.shape, F32),
        scratch_shapes=[pltpu.VMEM((n, *part.shape), F32), pltpu.SemaphoreType.DMA((n - 1,)), pltpu.SemaphoreType.DMA((n - 1,))],
        compiler_params=pltpu.CompilerParams(collective_id=run, has_side_effects=True),
        name="shared_sum",
    )(part)


def adamw(w, m, v, g):
    m = 0.9 * m + 0.1 * g
    v = 0.95 * v + 0.05 * g * g
    step = m * lax.rsqrt(v + 1e-8) + 0.1 * w
    return (w - 0.02 * step).astype(BF16), m, v


def solution(mesh):
    group = mesh.shape["dp"]
    side = int(round(group**0.5))

    def step(x, dy, *arrays):
        weights, m, v = (arrays[i : i + 7] for i in (0, 7, 14))
        wq, wk, wv, wo, w_gate, w_up, w_down = weights
        x, dy = x[0], dy[0]
        cos, sin = tables(x.shape[0])
        ids = iter(range(100))

        def run(body, comms=(), **kw):
            return call(body, side, next(ids) if comms else None, comms=comms, **kw)

        nothing = dict(ins=[], in_specs=[], outs=[], out_specs=[], scratch=[], grid=(1,))

        def split(g):
            return g.reshape(side, side, g.shape[0] // group, g.shape[1])

        def lines(g, got):
            x, y = lax.div(lax.axis_index("dp"), side), lax.rem(lax.axis_index("dp"), side)
            half = g.shape[3] // 2
            own = lax.dynamic_index_in_dim(g, x, 0, False)[..., :half], lax.dynamic_index_in_dim(g, y, 1, False)[..., half:]
            return tuple((o.astype(F32) + r.astype(F32).sum(0)).astype(BF16) for o, r in zip(own, got, strict=True))

        def block(g, one, two):
            x, y = lax.div(lax.axis_index("dp"), side), lax.rem(lax.axis_index("dp"), side)
            half = g.shape[3] // 2
            own = lax.dynamic_slice(g, (x, y, 0, 0), (1, 1, *g.shape[2:]))[0, 0].astype(F32)
            near = [lax.dynamic_index_in_dim(r, at, 1, False).astype(F32).sum(0) for r, at in zip(one, (y, x), strict=True)]
            far = [r.astype(F32).sum(0) for r in two]
            return jnp.concatenate([own[:, :half] + near[0] + far[0], own[:, half:] + near[1] + far[1]], -1).astype(BF16)

        a_of = lambda n: Gather(side, n, [[wq, wk, wv, wo]], [False])
        gu_of = lambda n: Gather(side, n, [[w_gate, w_up]], [False])
        d_of = lambda n: Gather(side, n, [[w_down]], [True])
        _, [[a0]] = run(None, comms=[(a_of(0), (0,) * 5)], name="gather", **nothing)
        (qkv0, o0, lse0), [[gu0], [d0]] = attn_fwd(run, x, a0, cos, sin, comms=[(gu_of(0), (0, 0, 1.5, 3.5, 3.5)), (d_of(0), (0, 0, 1.5, 3.5, 3.5))])
        (h1, h2), [[a1], [d1]] = ffn_fwd(run, x, o0, a0, gu0, d0, comms=[(a_of(1), (0, 0, 0.5, 3, 3.5)), (d_of(1), (0, 0, 0.5, 3, 3.5))])
        (qkv1, o1, lse1), [[gu1]] = attn_fwd(run, h2, a1, cos, sin, comms=[(gu_of(1), (0, 0, 1.5, 3.5, 3.5))])
        (dh3, do1, *dffn1), _ = ffn_bwd(run, h2, o1, dy, a1, gu1, d1, True)
        dffn1 = [split(g) for g in dffn1]
        (dh2, dqkv1), [one_f1] = attn_bwd(run, qkv1, h2, dh3, o1, do1, lse1, a1, cos, sin, True, comms=[(Scatter(side, dffn1), (0, 3.5))])
        dqkv1 = split(dqkv1)
        sums = [lines(g, r) for g, r in zip(dffn1, one_f1)]
        (dh1, do0, *dffn0), [two_f1, one_q1] = ffn_bwd(run, h1, o0, dh2, a0, gu0, d0, False,
                                                       comms=[(Scatter(side, sums), (0, 3.5)), (Scatter(side, [dqkv1]), (0, 3.5))])
        dffn0 = [split(g) for g in dffn0]
        sums = [lines(dqkv1, one_q1[0])]
        (_, dqkv0), [two_q1, one_f0] = attn_bwd(run, qkv0, x, dh1, o0, do0, lse0, a0, cos, sin, False,
                                                comms=[(Scatter(side, sums), (0, 3.5)), (Scatter(side, dffn0), (0, 3.5))])
        dqkv0 = split(dqkv0)
        sums = [lines(g, r) for g, r in zip(dffn0, one_f0)]
        _, [one_q0, two_f0] = run(None, comms=[(Scatter(side, [dqkv0]), (0, 0)), (Scatter(side, sums), (0, 0))], name="tail", **nothing)
        sums = [lines(dqkv0, one_q0[0])]
        _, [two_q0] = run(None, comms=[(Scatter(side, sums), (0, 0))], name="tail", **nothing)
        mine = []
        for dq, dffn, one_q, two_q, one_f, two_f in ((dqkv0, dffn0, one_q0, two_q0, one_f0, two_f0), (dqkv1, dffn1, one_q1, two_q1, one_f1, two_f1)):
            q = block(dq, one_q[0], two_q[0])
            o, gu, d = (block(*z) for z in zip(dffn, one_f, two_f, strict=True))
            third, half = q.shape[1] // 3, gu.shape[1] // 2
            mine.append([q[:, :third], q[:, third : 2 * third], q[:, 2 * third :], o, gu[:, :half], gu[:, half:], d])
        gradients = [jnp.stack(layers).astype(F32) for layers in zip(*mine, strict=True)]
        squares = shared_sum(next(ids), jnp.broadcast_to(sum(jnp.sum(g * g) for g in gradients), (8, 128)), group)[0, 0]
        factor = jnp.minimum(1.0, 0.5 * lax.rsqrt(squares / (group * sum(g.size for g in gradients)) + 1e-30))
        new = [adamw(w.astype(F32), m, v, g * factor) for w, m, v, g in zip(weights, m, v, gradients, strict=True)]
        return tuple(one[which] for which in range(3) for one in new)

    states, cut = P(("rep", "dp"), None, None), P(None, "dp", None)
    return jax.shard_map(
        step,
        mesh=mesh,
        in_specs=(states, states) + (cut,) * 21,
        out_specs=(P("rep", "dp", None),) * 21,
        check_vma=False,
    )
```

```python
import functools
import jax
import jax.numpy as jnp
import numpy as np
from jax import lax
from jax.experimental import pallas as pl
from jax.experimental.pallas import tpu as pltpu

HEAD = 256
THETA = 10000
LOG2E = 1.4426950408889634
VMEM = 60 * 2**20
EPS = 1e-6
F32, BF16 = jnp.float32, jnp.bfloat16


def dot(a, b, ca=1, cb=0):
    return lax.dot_general(a, b, (((ca,), (cb,)), ((), ())), preferred_element_type=F32)


def scale_of(h):
    return lax.rsqrt(jnp.mean(h * h, -1, keepdims=True) + EPS)


def rotated(t, cos, sin):
    half = t.shape[-1] // 2
    a, b = t[:, :half], t[:, half:]
    return jnp.concatenate([a * cos - b * sin, b * cos + a * sin], -1)


def heads_of(width):
    return [slice(at, at + HEAD) for at in range(0, width, HEAD)]


def hidden(rows, cols):
    return lax.broadcasted_iota(jnp.int32, (rows, cols), 0) > lax.broadcasted_iota(jnp.int32, (rows, cols), 1)


MESH = pl.DeviceIdType.MESH
ANY = pl.BlockSpec(memory_space=pl.ANY)


class Place:
    def __init__(self, side):
        rep, me = lax.axis_index("rep"), lax.axis_index("dp")
        self.side, self.x, self.y, self.core = side, lax.div(me, side), lax.rem(me, side), lax.rem(rep, 2)
        self.partner = {"rep": rep + 1 - 2 * self.core}

    def on(self, axis, k):
        at = lax.rem((self.x, self.y)[axis] + k, self.side)
        return at, {"dp": at * self.side + self.y if axis == 0 else self.x * self.side + at}


def remote(src, dst, send, recv, device):
    return pltpu.make_async_remote_copy(src_ref=src, dst_ref=dst, send_sem=send, recv_sem=recv, device_id=device, device_id_type=MESH)


class Gather:
    early = 1

    def __init__(self, side, layer, pieces, by_rows):
        self.side, self.pieces, self.by_rows = side, pieces, by_rows
        self.ins = [p for group in pieces for p in group]
        self.in_specs = [pl.BlockSpec((1, *p.shape[1:]), functools.partial(lambda layer, *_: (layer, 0, 0), layer)) for p in self.ins]
        self.outs = [jax.ShapeDtypeStruct((side, side, g[0].shape[1], sum(p.shape[2] for p in g)), g[0].dtype) for g in pieces]
        self.peers = side - 1
        n = len(pieces)
        self.scratch = [pltpu.SemaphoreType.DMA((len(self.ins),)), pltpu.SemaphoreType.DMA((n, 2, 4, self.peers)),
                        pltpu.SemaphoreType.DMA((n, 2, 4, self.peers))]
        self.partner = True
        self.out_specs = [ANY] * len(self.outs)

    def results(self, outs):
        return [o.reshape(-1, o.shape[-1]) for o in outs]

    def run(self, stage, place, ins, outs, scratch, owner):
        local, send, recv = scratch
        copies = []
        at = 0
        for group, out in zip(self.pieces, outs, strict=True):
            column = 0
            for p in group:
                copies.append((ins[at].at[0], out.at[place.x, place.y, :, column : column + p.shape[2]], local.at[at]))
                column, at = column + p.shape[2], at + 1
        if stage == 0:
            for c in copies:
                pltpu.make_async_copy(*c).start()
            return
        first, second, near, far = [], [], [], []
        come = [[], [], [], []]
        for n, out in enumerate(outs):
            size = out.shape[2] if self.by_rows[n] else out.shape[3]
            for q in range(2):
                def view(x, y, core, out=out, n=n, q=q, size=size):
                    piece = pl.ds(pl.multiple_of(core * (size // 2) + q * (size // 4), size // 4), size // 4)
                    return out.at[x, y, piece, :] if self.by_rows[n] else out.at[x, y, :, piece]

                a, b = q, 1 - q
                every = slice(None)
                here = view(place.x, place.y, place.core)
                line = (every, place.y) if a == 0 else (place.x, every)
                for k in range(1, self.side):
                    s = lambda kind: (send.at[n, q, kind, k - 1], recv.at[n, q, kind, k - 1])
                    _, to = place.on(a, k)
                    first.append((here, here, *s(0), to))
                    back, _ = place.on(a, self.side - k)
                    got = view(*((back, place.y) if a == 0 else (place.x, back)), place.core)
                    come[0].append((got, got, *s(0), to))
                    near.append((got, got, *s(2), place.partner))
                    got = view(*((back, place.y) if a == 0 else (place.x, back)), 1 - place.core)
                    come[2].append((got, got, *s(2), place.partner))
                    _, to = place.on(b, k)
                    mine = view(*line, place.core)
                    second.append((mine, mine, *s(1), to))
                    back, _ = place.on(b, self.side - k)
                    got = view(*((every, back) if a == 0 else (back, every)), place.core)
                    come[1].append((got, got, *s(1), to))
                    far.append((got, got, *s(3), place.partner))
                    got = view(*((every, back) if a == 0 else (back, every)), 1 - place.core)
                    come[3].append((got, got, *s(3), place.partner))
        if stage == 1:
            for c in copies:
                pltpu.make_async_copy(*c).wait()
            for c in first:
                remote(*c).start()
        elif stage == 2:
            for c in come[0]:
                remote(*c).wait_recv()
            for c in second + near:
                remote(*c).start()
        elif stage == 3:
            for c, f in zip(come[1], far, strict=True):
                remote(*c).wait_recv()
                remote(*f).start()
        else:
            for c in come[2] + come[3]:
                remote(*c).wait_recv()
            for c in first + second + near + far:
                remote(*c).wait_send()


class Sum:
    partner, early = False, 0

    def __init__(self, side, rows, width, given=None, scratch=None, line=None):
        self.side, self.width, self.line, self.at = side, width, line, scratch
        self.ins = [] if given is None else [given]
        self.in_specs = [whole(a.shape) for a in self.ins]
        self.outs = [jax.ShapeDtypeStruct((rows, width), BF16)]
        self.out_specs = [whole((rows, width))]
        n = side - 1
        if line is None:
            shapes = [((2, n, side, rows, width // 2), BF16), ((2, side, rows, width // 2), BF16), ((2, n, rows, width // 2), BF16), ((2, rows, width // 2), F32)]
            sems = (2, 2, n)
        else:
            shapes = [((n, rows, width), BF16), ((rows, width), BF16), ((n, rows, width), BF16), ((rows, width), F32)]
            sems = (2, n)
        self.scratch = [pltpu.VMEM(*s) for s in shapes] + [pltpu.SemaphoreType.DMA(sems)] * 2

    def results(self, outs):
        return outs[0]

    def run(self, stage, place, ins, outs, scratch, owner):
        src = ins[0] if self.at is None else owner[self.at[0]].at[self.at[1]]
        (self.crossed if self.line is None else self.lined)(stage, place, src, outs[0], *scratch)

    def crossed(self, stage, place, src, out, one, mid, two, own, send, recv):
        n, half = self.side - 1, self.width // 2
        mine = (place.x, place.y)

        def firsts():
            for q in range(2):
                for k in range(n):
                    there, to = place.on(q, k + 1)
                    view = src.at[there, :, :, :half] if q == 0 else src.at[:, there, :, half:]
                    yield remote(view, one.at[q, k], send.at[0, q, k], recv.at[0, q, k], to)

        def seconds():
            for q in range(2):
                for k in range(n):
                    there, to = place.on(1 - q, k + 1)
                    yield remote(mid.at[q, there], two.at[q, k], send.at[1, q, k], recv.at[1, q, k], to)

        def total(q, j):
            t = (src[place.x, j, :, :half] if q == 0 else src[j, place.y, :, half:]).astype(F32)
            for k in range(n):
                t += one[q, k, j].astype(F32)
            return t

        if stage == 0:
            for c in firsts():
                c.start()
        elif stage == 1:
            for c in firsts():
                c.wait()
            for q in range(2):

                def add(j, _):
                    mid[q, j] = total(q, j).astype(BF16)

                lax.fori_loop(0, self.side, add, None)
                own[q] = total(q, mine[1 - q])
            for c in seconds():
                c.start()
        else:
            for c in seconds():
                c.wait()
            for q in range(2):
                t = own[q]
                for k in range(n):
                    t += two[q, k].astype(F32)
                out[:, q * half : (q + 1) * half] = t.astype(BF16)

    def lined(self, stage, place, src, out, one, mid, two, own, send, recv):
        n = self.side - 1
        ahead = lax.rem(self.line - place.x + self.side, self.side)

        def firsts():
            for k in range(n):
                there, to = place.on(1, k + 1)
                yield remote(src.at[there], one.at[k], send.at[0, k], recv.at[0, k], to)

        def second():
            return remote(mid, two.at[ahead - 1], send.at[1, 0], recv.at[1, ahead - 1], place.on(0, ahead)[1])

        if stage == 0:
            for c in firsts():
                c.start()
        elif stage == 1:
            for c in firsts():
                c.wait()
            t = src[place.y].astype(F32)
            for k in range(n):
                t += one[k].astype(F32)
            own[...] = t
            mid[...] = t.astype(BF16)

            @pl.when(ahead != 0)
            def _():
                second().start()
        else:

            @pl.when(ahead != 0)
            def _():
                second().wait_send()

            @pl.when(ahead == 0)
            def _():
                t = own[...]
                for k in range(n):
                    remote(mid, two.at[k], send.at[1, 0], recv.at[1, k], place.on(0, 0)[1]).wait_recv()
                    t += two[k].astype(F32)
                out[...] = t.astype(BF16)


def call(body, side, cid, *, grid, ins, in_specs, outs, out_specs, scratch, name, comms=(), barrier=0):
    steps = grid[0]
    parts = [c for c, _ in comms]
    counts = [len(ins), *(len(c.ins) for c in parts), len(outs), *(len(c.outs) for c in parts), len(scratch), *(len(c.scratch) for c in parts)]
    partner = any(c.partner for c in parts)

    def kernel(*refs):
        split, at = [], 0
        for n in counts:
            split.append(refs[at : at + n])
            at += n
        m = len(parts)
        my_in, c_in, my_out, c_out, my_s, c_s = (split[0], split[1 : m + 1], split[m + 1], split[m + 2 : 2 * m + 2], split[2 * m + 2], split[2 * m + 3 :])
        step = pl.program_id(0)

        def events(now):
            todo = sorted((s, n) for n, (_, when) in enumerate(comms) for s, t in enumerate(when) if t == now)
            if not comms or not (todo or now in (0, barrier)):
                return

            @pl.when(step == int(now))
            def _():
                place = Place(side)
                devices = [place.on(axis, k)[1] for axis in (0, 1) for k in range(1, side)] + [place.partner] * partner
                if now == 0:
                    for device in devices:
                        pl.semaphore_signal(pltpu.get_barrier_semaphore(), inc=1, device_id=device, device_id_type=MESH)
                early = [(s, n) for s, n in todo if s < parts[n].early]
                for s, n in early:
                    parts[n].run(s, place, c_in[n], c_out[n], c_s[n], my_s)
                if now == barrier:
                    pl.semaphore_wait(pltpu.get_barrier_semaphore(), len(devices))
                for s, n in todo:
                    if (s, n) not in early:
                        parts[n].run(s, place, c_in[n], c_out[n], c_s[n], my_s)

        for s in range(steps):
            events(s)
        if body is not None:
            body(*my_in, *my_out, *my_s)
        for s in range(steps):
            events(s + 0.5)

    got = pl.pallas_call(
        kernel,
        grid=grid,
        in_specs=[*in_specs, *(s for c in parts for s in c.in_specs)],
        out_specs=[*out_specs, *(s for c in parts for s in c.out_specs)],
        out_shape=[*outs, *(o for c in parts for o in c.outs)],
        scratch_shapes=[*scratch, *(s for c in parts for s in c.scratch)],
        compiler_params=pltpu.CompilerParams(dimension_semantics=("arbitrary",), vmem_limit_bytes=VMEM, has_side_effects=bool(comms),
                                             **({"collective_id": cid} if comms else {})),
        name=name,
    )(*ins, *(a for c in parts for a in c.ins))
    given, at, results = list(got[: len(outs)]), len(outs), []
    for c in parts:
        results.append(c.results(got[at : at + len(c.outs)]))
        at += len(c.outs)
    return given, results


def attn_fwd_body(h_ref, w_ref, cos_ref, sin_ref, qkv_ref, o_ref, lse_ref, k_s, vt_s, top_s, mix_s):
    i = pl.program_id(0)
    bq, d = h_ref.shape
    width = o_ref.shape[1]
    hs = heads_of(width)

    @pl.when(i == 0)
    def _():
        for n in range(len(hs)):
            vt_s[n, HEAD:, :] = jnp.ones((8, vt_s.shape[2]), BF16)

    h = h_ref[...].astype(F32)
    a = (h * scale_of(h)).astype(BF16)
    t = dot(a, w_ref[:, : 3 * width]).astype(BF16)
    cos, sin = cos_ref[...], sin_ref[...]
    here = pl.ds(pl.multiple_of(i * bq, bq), bq)
    qs = []
    for n, at in enumerate(hs):
        q = rotated(t[:, at].astype(F32), cos, sin).astype(BF16) * jnp.asarray(HEAD**-0.5, BF16)
        k = rotated(t[:, width + at.start : width + at.stop].astype(F32), cos, sin).astype(BF16)
        v = t[:, 2 * width + at.start : 2 * width + at.stop]
        qkv_ref[:, at] = q
        qkv_ref[:, width + at.start : width + at.stop] = k
        qkv_ref[:, 2 * width + at.start : 2 * width + at.stop] = v
        k_s[here, at] = k
        vt_s[n, :HEAD, here] = v.T
        qs.append(q)

    def block(j, first):
        keys = pl.ds(pl.multiple_of(j * bq, bq), bq)
        scores = [dot(k_s[keys, at], q, 1, 1) for at, q in zip(hs, qs)]
        ps, keeps = [], []
        for n, s in enumerate(scores):
            if first:
                s = jnp.where(hidden(bq, bq), -1e30, s)
                top = s.max(0, keepdims=True)
            else:
                old = top_s[n : n + 1, :]
                top = jnp.maximum(old, s.max(0, keepdims=True))
                keeps.append(jnp.exp2((old - top) * LOG2E))
            top_s[n : n + 1, :] = top
            ps.append(jnp.exp2((s - top) * LOG2E).astype(BF16))
        for n, p in enumerate(ps):
            new = dot(vt_s[n, :, keys], p)
            mix_s[n] = new if first else mix_s[n] * keeps[n] + new

    block(i, True)
    lax.fori_loop(0, i, lambda j, _: block(j, False), None)
    for n, at in enumerate(hs):
        total = mix_s[n, HEAD : HEAD + 1, :]
        o_ref[:, at] = (mix_s[n, :HEAD, :] * (1 / total)).T.astype(BF16)
        lse_ref[n : n + 1, :] = top_s[n : n + 1, :] * LOG2E + jnp.log2(total)


def whole(shape):
    return pl.BlockSpec(shape, lambda *_: (0,) * len(shape), pipeline_mode=pl.Buffered(1))


def rows(n, width, back=None):
    return pl.BlockSpec((n, width), (lambda i: (i, 0)) if back is None else (lambda i: (back - 1 - i, 0)))


def attn_fwd(run, h, w, cos, sin, bq=512, **kw):
    t, d = h.shape
    width = w.shape[1] // 4
    nh = width // HEAD
    sd = jax.ShapeDtypeStruct
    return run(
        attn_fwd_body,
        grid=(t // bq,),
        ins=[h, w, cos, sin],
        in_specs=[rows(bq, d), whole(w.shape), rows(bq, HEAD // 2), rows(bq, HEAD // 2)],
        outs=[sd((t, 3 * width), BF16), sd((t, width), BF16), sd((nh, t), F32)],
        out_specs=[rows(bq, 3 * width), rows(bq, width), pl.BlockSpec((nh, bq), lambda i: (0, i))],
        scratch=[pltpu.VMEM((t, width), BF16), pltpu.VMEM((nh, HEAD + 8, t), BF16), pltpu.VMEM((nh, bq), F32),
                 pltpu.VMEM((nh, HEAD + 8, bq), F32)],
        name="attn_fwd",
        **kw,
    )


def ffn_fwd_body(h_ref, o_ref, wa_ref, wgu_ref, wd_ref, h1_ref, h2_ref, act_s, *, step):
    width, f = o_ref.shape[1], wd_ref.shape[0]
    h1 = h_ref[...] + dot(o_ref[...], wa_ref[:, 3 * width :]).astype(BF16)
    h1_ref[...] = h1
    wide = h1.astype(F32)
    b = (wide * scale_of(wide)).astype(BF16)
    for c in range(0, f, step):
        gate = dot(b, wgu_ref[:, c : c + step])
        up = dot(b, wgu_ref[:, f + c : f + c + step])
        act_s[:, c : c + step] = (gate * jax.nn.sigmoid(gate) * up).astype(BF16)
    h2_ref[...] = h1 + dot(act_s[...], wd_ref[...]).astype(BF16)


def ffn_fwd(run, h, o, wa, wgu, wd, bq=512, step=512, **kw):
    t, d = h.shape
    f = wd.shape[0]
    return run(
        functools.partial(ffn_fwd_body, step=step),
        grid=(t // bq,),
        ins=[h, o, wa, wgu, wd],
        in_specs=[rows(bq, d), rows(bq, o.shape[1]), whole(wa.shape), whole(wgu.shape), whole(wd.shape)],
        outs=[jax.ShapeDtypeStruct((t, d), BF16)] * 2,
        out_specs=[rows(bq, d), rows(bq, d)],
        scratch=[pltpu.VMEM((bq, f), BF16)],
        name="ffn_fwd",
        **kw,
    )


def normed_bwd(y, r, by):
    return r * (by - y * jnp.mean(by * y, -1, keepdims=True))


def ffn_bwd_body(h_ref, o_ref, g_ref, wo_ref, wg_ref, wu_ref, wd_ref, dh1_ref, do_ref, dwo_ref, dgu_ref, dd_ref, *scratch, side, fwd, sub):
    b_s, bt_s, g_s, gt_s, by_s, h1_s, act_s, dgu_s, gu_o, d_o, wo_a = scratch
    step = pl.program_id(0)
    bq, d = h_ref.shape
    t, cut = act_s.shape
    tiles = t // bq

    @pl.when(step < tiles)
    def _():
        here = pl.ds(pl.multiple_of(step * bq, bq), bq)
        h1 = h_ref[...]
        if fwd:
            h1 = h1 + dot(o_ref[...], wo_ref[...]).astype(BF16)
            h1_s[here, :] = h1
        wide = h1.astype(F32)
        b = (wide * scale_of(wide)).astype(BF16)
        b_s[here, :] = b
        bt_s[:, here] = b.T
        g_s[here, :] = g_ref[...]
        gt_s[:, here] = g_ref[...].T

    @pl.when((step >= tiles) & (step < tiles + side))
    def _():
        chunk = step - tiles

        def tile(n, _):
            here = pl.ds(pl.multiple_of(n * bq, bq), bq)
            b, g = b_s[here, :], g_s[here, :]
            for c in range(0, cut, sub):
                cols = slice(c, c + sub)
                gate, up = dot(b, wg_ref[:, cols]), dot(b, wu_ref[:, cols])
                dact = dot(g, wd_ref[cols, :], 1, 1)
                sig = jax.nn.sigmoid(gate)
                silu = gate * sig
                act_s[here, cols] = (silu * up).astype(BF16)
                dgu_s[here, cols] = (dact * up * (sig + silu * (1 - sig))).astype(BF16)
                dgu_s[here, cut + c : cut + c + sub] = (dact * silu).astype(BF16)
            by = dot(dgu_s[here, :cut], wg_ref[...], 1, 1) + dot(dgu_s[here, cut:], wu_ref[...], 1, 1)

            @pl.when(chunk == 0)
            def _():
                by_s[here, :] = by

            @pl.when(chunk > 0)
            def _():
                by_s[here, :] += by

        lax.fori_loop(0, tiles, tile, None)
        slot = lax.rem(chunk, 2)
        for c in range(0, 2 * cut, cut):
            gu_o[slot, :, :, :, c : c + cut] = dot(bt_s[...], dgu_s[:, c : c + cut]).astype(BF16).reshape(*gu_o.shape[1:4], cut)
        d_o[slot] = dot(gt_s[...], act_s[...]).T.astype(BF16).reshape(d_o.shape[1:])

        @pl.when(chunk == side - 1)
        def _():
            dgu_ref[...] = gu_o[slot]
            dd_ref[...] = d_o[slot]

    @pl.when(step >= tiles + side)
    def _():
        n = step - tiles - side
        here = pl.ds(pl.multiple_of(n * bq, bq), bq)
        h1 = (h1_s[here, :] if fwd else h_ref[...]).astype(F32)
        r = scale_of(h1)
        dh1 = (g_s[here, :].astype(F32) + normed_bwd(h1 * r, r, by_s[here, :])).astype(BF16)
        dh1_ref[...] = dh1
        do_ref[...] = dot(dh1, wo_ref[...], 1, 1).astype(BF16)
        by_wo = dot(o_ref[...].T, dh1)

        @pl.when(n == 0)
        def _():
            wo_a[...] = by_wo

        @pl.when(n > 0)
        def _():
            wo_a[...] += by_wo

        @pl.when(n == tiles - 1)
        def _():
            dwo_ref[...] = wo_a[...].astype(BF16).reshape(dwo_ref.shape)


GU, DD = 8, 9


def ffn_bwd(run, h, o, g, wa, wgu, wd, fwd, side, bq=512, sub=256, **kw):
    t, d = h.shape
    f, width = wd.shape[0], o.shape[1]
    sd = jax.ShapeDtypeStruct
    tiles, cut = t // bq, f // side
    at = lambda i: jnp.clip(i - tiles, 0, side - 1)
    two = lambda w: pl.BlockSpec((bq, w), lambda i: (jnp.where(i < tiles + side, jnp.minimum(i, tiles - 1), i - tiles - side), 0))
    end = lambda w: pl.BlockSpec((bq, w), lambda i: (jnp.maximum(i - tiles - side, 0), 0))
    gu, dd, dwo = (side, side, d // side**2, 2 * cut), (side, cut // side, d), (side, side, width // side**2, d)
    return run(
        functools.partial(ffn_bwd_body, side=side, fwd=fwd, sub=sub),
        grid=(2 * tiles + side,),
        ins=[h, o, g, wa, wgu, wgu, wd],
        in_specs=[two(d), two(width), pl.BlockSpec((bq, d), lambda i: (jnp.minimum(i, tiles - 1), 0)), pl.BlockSpec((d, width), lambda i: (0, 3)),
                  pl.BlockSpec((d, cut), lambda i: (0, at(i))), pl.BlockSpec((d, cut), lambda i: (0, side + at(i))),
                  pl.BlockSpec((cut, d), lambda i: (at(i), 0))],
        outs=[sd((t, d), BF16), sd((t, width), BF16), sd(dwo, BF16), sd(gu, BF16), sd(dd, BF16)],
        out_specs=[end(d), end(width), whole(dwo), whole(gu), whole(dd)],
        scratch=[pltpu.VMEM((t, d), BF16), pltpu.VMEM((d, t), BF16), pltpu.VMEM((t, d), BF16), pltpu.VMEM((d, t), BF16), pltpu.VMEM((t, d), F32),
                 pltpu.VMEM((t, d) if fwd else (16, 128), BF16), pltpu.VMEM((t, cut), BF16), pltpu.VMEM((t, 2 * cut), BF16),
                 pltpu.VMEM((2, *gu), BF16), pltpu.VMEM((2, *dd), BF16), pltpu.VMEM((width, d), F32)],
        name="ffn_bwd",
        **kw,
    )


def attn_bwd_body(qkv_ref, h_ref, dh1_ref, o_ref, do_ref, lse_ref, w_ref, cos_ref, sin_ref, *rest, more):
    dh_ref, rest = (rest[0], rest[1:]) if more else (None, rest)
    dw_ref, kt_s, dq_s, dk_s, dv_s, dt_s, dw_a = rest
    step, n = pl.program_id(0), pl.num_programs(0)
    i = n - 1 - step
    bq, d = h_ref.shape
    width = o_ref.shape[1]
    hs = heads_of(width)

    @pl.when(step == 0)
    def _():
        dk_s[...] = jnp.zeros_like(dk_s)
        dv_s[...] = jnp.zeros_like(dv_s)
        dw_a[...] = jnp.zeros_like(dw_a)
        for j in range(0, kt_s.shape[2], bq):
            for m, at in enumerate(hs):
                kt_s[m, :, j : j + bq] = qkv_ref[j : j + bq, width + at.start : width + at.stop].T

    here = pl.ds(pl.multiple_of(i * bq, bq), bq)
    qs = [qkv_ref[here, at] for at in hs]
    dos = [do_ref[:, at] for at in hs]
    deltas = []
    for m, at in enumerate(hs):
        delta = (dos[m].astype(F32) * o_ref[:, at].astype(F32)).sum(-1, keepdims=True)
        deltas.append(jnp.broadcast_to(delta, (bq, 128)).T[:1, :])
    lses = [lse_ref[m : m + 1, :] for m in range(len(hs))]

    def block(j, first):
        keys = pl.ds(pl.multiple_of(j * bq, bq), bq)
        scores = [dot(qkv_ref[keys, width + at.start : width + at.stop], q, 1, 1) for at, q in zip(hs, qs)]
        dps = [dot(qkv_ref[keys, 2 * width + at.start : 2 * width + at.stop], x, 1, 1) for at, x in zip(hs, dos)]
        for m, at in enumerate(hs):
            p = jnp.exp2(scores[m] * LOG2E - lses[m])
            if first:
                p = jnp.where(hidden(bq, bq), 0.0, p)
            ds = (p * (dps[m] - deltas[m])).astype(BF16)
            dv_s[keys, at] += dot(p.astype(BF16), dos[m])
            dk_s[keys, at] += dot(ds, qs[m])
            dq = dot(kt_s[m, :, keys], ds)
            dq_s[m] = dq if first else dq_s[m] + dq

    block(i, True)
    lax.fori_loop(0, i, lambda j, _: block(j, False), None)
    cos, sin = cos_ref[...], -sin_ref[...]
    for m, at in enumerate(hs):
        dt_s[:, at] = rotated((dq_s[m] * HEAD**-0.5).T, cos, sin).astype(BF16)
        dt_s[:, width + at.start : width + at.stop] = rotated(dk_s[here, at], cos, sin).astype(BF16)
        dt_s[:, 2 * width + at.start : 2 * width + at.stop] = dv_s[here, at].astype(BF16)
    h = h_ref[...].astype(F32)
    r = scale_of(h)
    y = h * r
    dw_a[...] += dot(y.astype(BF16).T, dt_s[...])
    if more:
        by = dot(dt_s[...], w_ref[:, : 3 * width], 1, 1)
        dh_ref[...] = (dh1_ref[...].astype(F32) + normed_bwd(y, r, by)).astype(BF16)

    @pl.when(step == n - 1)
    def _():
        dw_ref[...] = dw_a[...].astype(BF16).reshape(dw_ref.shape)


def attn_bwd(run, qkv, h, dh1, o, do, lse, w, cos, sin, more, side, bq=512, **kw):
    t, d = h.shape
    width = o.shape[1]
    nh, n = width // HEAD, t // bq
    sd = jax.ShapeDtypeStruct
    back = lambda wd: rows(bq, wd, n)
    dw = (side, side, d // side**2, 3 * width)
    out, got = run(
        functools.partial(attn_bwd_body, more=more),
        grid=(n,),
        ins=[qkv, h, dh1, o, do, lse, w, cos, sin],
        in_specs=[whole(qkv.shape), back(d), back(d), back(width), back(width), pl.BlockSpec((nh, bq), lambda i: (0, n - 1 - i)), whole(w.shape),
                  back(HEAD // 2), back(HEAD // 2)],
        out_specs=[back(d)] * more + [whole(dw)],
        outs=[sd((t, d), BF16)] * more + [sd(dw, BF16)],
        scratch=[pltpu.VMEM((nh, HEAD, t), BF16), pltpu.VMEM((nh, HEAD, bq), F32), pltpu.VMEM((t, width), F32), pltpu.VMEM((t, width), F32),
                        pltpu.VMEM((bq, 3 * width), BF16), pltpu.VMEM((d, 3 * width), F32)],
        name="attn_bwd",
        **kw,
    )
    return ([] if more else [None]) + out, got


def tables(tokens):
    half = HEAD // 2
    angle = np.arange(tokens, dtype=np.float32)[:, None] * np.float32(THETA) ** (-np.arange(half, dtype=np.float32) / np.float32(half))
    return jnp.asarray(np.cos(angle), F32), jnp.asarray(np.sin(angle), F32)


from jax.sharding import PartitionSpec as P

NAMES = ("wq", "wk", "wv", "wo", "w_gate", "w_up", "w_down")


def square(g):
    wide = g.astype(F32)
    return jnp.sum(jnp.sum(wide * wide, 0, keepdims=True), 1, keepdims=True)


def finish(cid, side, last, done, downs):
    n = side * side
    task = Sum(side, last.shape[2], last.shape[3], given=last)
    ins = [last, *done, *(d for group in downs for d in group)]

    def body(*refs):
        last_ref, refs = refs[0], refs[1:]
        done_refs, refs = refs[: len(done)], refs[len(done) :]
        down_refs, (out, total_ref, slots, part, send, recv, *scratch) = refs[: side * len(downs)], refs[side * len(downs) :]
        place = Place(side)
        me = place.x * side + place.y
        others = [{"dp": lax.rem(me + k, n)} for k in range(1, n)]
        barrier = pltpu.get_barrier_semaphore()
        for device in others:
            pl.semaphore_signal(barrier, inc=1, device_id=device, device_id_type=MESH)
        pl.semaphore_wait(barrier, n - 1)
        task.run(0, place, [last_ref], [out], scratch, None)
        mine = sum(square(r[...]) for r in done_refs)
        for c, r in enumerate(down_refs):
            mine += jnp.where(place.x == c % side, square(r[...]), 0.0)
        task.run(1, place, [last_ref], [out], scratch, None)
        task.run(2, place, [last_ref], [out], scratch, None)
        mine = jnp.broadcast_to(mine + square(out[...]), part.shape)
        part[...] = mine
        slots[me] = mine
        copies = [remote(part, slots.at[me], send.at[k], recv.at[k], device) for k, device in enumerate(others)]
        for c in copies:
            c.start()
        for k in range(n - 1):
            remote(part, slots.at[lax.rem(me + n - k - 1, n)], send.at[k], recv.at[k], others[k]).wait()
        total_ref[...] = slots[...].sum(0)

    return pl.pallas_call(
        body,
        grid=(1,),
        in_specs=[whole(a.shape) for a in ins],
        out_specs=[*task.out_specs, whole((8, 128))],
        out_shape=[*task.outs, jax.ShapeDtypeStruct((8, 128), F32)],
        scratch_shapes=[pltpu.VMEM((n, 8, 128), F32), pltpu.VMEM((8, 128), F32), pltpu.SemaphoreType.DMA((n - 1,)), pltpu.SemaphoreType.DMA((n - 1,)),
                        *task.scratch],
        compiler_params=pltpu.CompilerParams(collective_id=cid, has_side_effects=True, vmem_limit_bytes=VMEM),
        name="finish",
    )(*ins)


def adamw(side, total, count, weights, m, v, gradients):
    layers = len(gradients)
    flat = [a for qkv, o, gu, down in gradients for a in (qkv, o, *gu, *down)]
    each = len(flat) // layers

    def body(total_ref, *refs):
        grads = refs[: len(flat)]
        w_refs, m_refs, v_refs, wn_refs, mn_refs, vn_refs = (refs[i : i + 7] for i in range(len(flat), len(refs), 7))
        factor = jnp.minimum(1.0, 0.5 * lax.rsqrt(total_ref[0:1, 0:1] / count + 1e-30))
        x = lax.div(lax.axis_index("dp"), side)

        def update(i, columns, g):
            g = g.astype(F32) * factor
            at = (0, slice(None), columns)
            mn = 0.9 * m_refs[i][at] + 0.1 * g
            vn = 0.95 * v_refs[i][at] + 0.05 * g * g
            mn_refs[i][at], vn_refs[i][at] = mn, vn
            w = w_refs[i][at].astype(F32)
            wn_refs[i][at] = (w - 0.02 * (mn * lax.rsqrt(vn + 1e-8) + 0.1 * w)).astype(BF16)

        def layer(grads):
            qkv, o, gu, down = grads[0], grads[1], grads[2 : 2 + side], grads[2 + side :]
            wide = o.shape[1]
            for i in range(3):
                update(i, slice(None), qkv[:, i * wide : (i + 1) * wide])
            update(3, slice(None), o[...])
            for c, g in enumerate(gu):
                cut = g.shape[1] // 2
                update(4, slice(c * cut, (c + 1) * cut), g[:, :cut])
                update(5, slice(c * cut, (c + 1) * cut), g[:, cut:])
            g = down[0][...]
            for c in range(1, side):
                g = jnp.where(x == c, down[c][...], g)
            update(6, slice(None), g)

        for l in range(layers):
            pl.when(pl.program_id(0) == l)(functools.partial(layer, grads[l * each : (l + 1) * each]))

    own = [pl.BlockSpec((1, *a.shape[1:]), lambda l: (l, 0, 0)) for a in weights]
    sd = jax.ShapeDtypeStruct
    return pl.pallas_call(
        body,
        grid=(layers,),
        in_specs=[whole(total.shape), *(whole(a.shape) for a in flat), *own * 3],
        out_specs=own * 3,
        out_shape=[*(sd(a.shape, BF16) for a in weights), *(sd(a.shape, F32) for a in (*m, *v))],
        compiler_params=pltpu.CompilerParams(dimension_semantics=("arbitrary",), vmem_limit_bytes=VMEM),
        name="adamw",
    )(total, *flat, *weights, *m, *v)


def solution(mesh):
    group = mesh.shape["dp"]
    side = int(round(group**0.5))

    def step(x, dy, *arrays):
        weights, m, v = (arrays[i : i + 7] for i in (0, 7, 14))
        wq, wk, wv, wo, w_gate, w_up, w_down = weights
        x, dy = x[0], dy[0]
        cos, sin = tables(x.shape[0])
        ids = iter(range(100))

        def run(body, comms=(), **kw):
            return call(body, side, next(ids) if comms else None, comms=comms, **kw)

        nothing = dict(ins=[], in_specs=[], outs=[], out_specs=[], scratch=[], grid=(1,))

        a_of = lambda n: Gather(side, n, [[wq, wk, wv, wo]], [False])
        gu_of = lambda n: Gather(side, n, [[w_gate, w_up]], [False])
        d_of = lambda n: Gather(side, n, [[w_down]], [True])
        _, [[a0]] = run(None, comms=[(a_of(0), (0,) * 5)], name="gather", **nothing)
        (qkv0, o0, lse0), [[gu0], [d0]] = attn_fwd(run, x, a0, cos, sin, comms=[(gu_of(0), (0, 0, 1.5, 3.5, 3.5)), (d_of(0), (0, 0, 1.5, 3.5, 3.5))])
        (h1, h2), [[a1], [d1]] = ffn_fwd(run, x, o0, a0, gu0, d0, comms=[(a_of(1), (0, 0, 0.5, 3, 3.5)), (d_of(1), (0, 0, 0.5, 3, 3.5))])
        (qkv1, o1, lse1), [[gu1]] = attn_fwd(run, h2, a1, cos, sin, comms=[(gu_of(1), (0, 0, 1.5, 3.5, 3.5))])
        tiles = x.shape[0] // 512

        def chunked(f):
            tasks = []
            for c in range(side - 1):
                when = tuple(tiles + min(c + later, side - 1) + 0.5 for later in range(2)) + (tiles + c + 2.5 if c + 2 < side else 2 * tiles + side - 0.5,)
                tasks.append((Sum(side, x.shape[1] // group, 2 * f // side, scratch=(GU, c % 2)), when))
                tasks.append((Sum(side, f // group, x.shape[1], scratch=(DD, c % 2), line=c), when))
            return tasks

        def late(dwo, dgu, dd, when):
            return [(Sum(side, g.shape[-2], g.shape[-1], given=g, line=line), when) for g, line in ((dgu, None), (dd, side - 1), (dwo, None))]

        f = gu0.shape[1] // 2
        (dh3, do1, *left), got1 = ffn_bwd(run, h2, o1, dy, a1, gu1, d1, True, side, comms=chunked(f), barrier=tiles - 1)
        (dh2, dqkv1), (gu_l1, dd_l1, wo1) = attn_bwd(run, qkv1, h2, dh3, o1, do1, lse1, a1, cos, sin, True, side, comms=late(*left, (0, 2, 3.5)))
        tasks = [*chunked(f), (Sum(side, dqkv1.shape[-2], dqkv1.shape[-1], given=dqkv1), (1, tiles + 0.5, tiles + 1.5))]
        (dh1, do0, *left), (*got0, qkv_1) = ffn_bwd(run, h1, o0, dh2, a0, gu0, d0, False, side, comms=tasks, barrier=1)
        (_, dqkv0), (gu_l0, dd_l0, wo0) = attn_bwd(run, qkv0, x, dh1, o0, do0, lse0, a0, cos, sin, False, side, comms=late(*left, (0, 2, 3.5)))
        gus, downs = [[*got0[::2], gu_l0], [*got1[::2], gu_l1]], [[*got0[1::2], dd_l0], [*got1[1::2], dd_l1]]
        qkv_0, total = finish(next(ids), side, dqkv0, [qkv_1, wo0, wo1, *gus[0], *gus[1]], downs)
        count = group * sum(w.size for w in weights)
        return adamw(side, total, count, weights, m, v, [(qkv_0, wo0, gus[0], downs[0]), (qkv_1, wo1, gus[1], downs[1])])

    states, cut = P(("rep", "dp"), None, None), P(None, "dp", None)
    return jax.shard_map(
        step,
        mesh=mesh,
        in_specs=(states, states) + (cut,) * 21,
        out_specs=(P("rep", "dp", None),) * 21,
        check_vma=False,
    )
```

```python
import functools

import jax
import jax.numpy as jnp
import numpy as np
from jax import lax
from jax.experimental import pallas as pl
from jax.experimental.pallas import tpu as pltpu
from jax.sharding import PartitionSpec as P

HEAD = 256
THETA = 10000
LOG2E = 1.4426950408889634
VMEM = 67_000_000
EPS = 1e-6
F32, BF16 = jnp.float32, jnp.bfloat16
MESH = pl.DeviceIdType.MESH
ANY = pl.BlockSpec(memory_space=pl.ANY)
ROWS = 512
sds = jax.ShapeDtypeStruct


def dot(a, b, ca=1, cb=0):
    return lax.dot_general(a, b, (((ca,), (cb,)), ((), ())), preferred_element_type=F32)


def scale_of(h):
    return lax.rsqrt(jnp.mean(h * h, -1, keepdims=True) + EPS)


def normed_bwd(y, r, by):
    return r * (by - y * jnp.mean(by * y, -1, keepdims=True))


def tables(tokens):
    half = HEAD // 2
    rate = np.float32(THETA) ** (-np.arange(half, dtype=np.float32) / np.float32(half))
    angles = [np.arange(0, stop, step, dtype=np.float32)[:, None].astype(np.float64) * rate.astype(np.float64) for stop, step in ((ROWS, 1), (tokens, ROWS))]
    return [jnp.asarray(f(a), F32) for a in angles for f in (np.cos, np.sin)]


def angles(refs, tile):
    near_c, near_s, far_c, far_s = refs
    c, s = far_c[pl.ds(tile, 1), :], far_s[pl.ds(tile, 1), :]
    return c * near_c[...] - s * near_s[...], s * near_c[...] + c * near_s[...]


def rotated(t, cos, sin):
    half = t.shape[-1] // 2
    a, b = t[:, :half], t[:, half:]
    return jnp.concatenate([a * cos - b * sin, b * cos + a * sin], -1)


def hidden(size):
    return lax.broadcasted_iota(jnp.int32, (size, size), 0) > lax.broadcasted_iota(jnp.int32, (size, size), 1)


def tile_at(n, size=ROWS):
    return pl.ds(pl.multiple_of(n * size, size), size)


def whole(shape):
    return pl.BlockSpec(shape, lambda *_: (0,) * len(shape), pipeline_mode=pl.Buffered(1))


def side_of(group):
    return int(round(group**0.5))


class Place:
    def __init__(self, side):
        rep, me = lax.axis_index("rep"), lax.axis_index("dp")
        self.side, self.me, self.x, self.y, self.core = side, me, lax.div(me, side), lax.rem(me, side), lax.rem(rep, 2)
        self.partner = {"rep": rep + 1 - 2 * self.core}

    def on(self, axis, k):
        at = lax.rem((self.x, self.y)[axis] + k, self.side)
        return at, {"dp": at * self.side + self.y if axis == 0 else self.x * self.side + at}

    def line(self):
        return [self.on(axis, k)[1] for axis in (0, 1) for k in range(1, self.side)]

    def others(self):
        n = self.side**2
        return [{"dp": lax.rem(self.me + k, n)} for k in range(1, n)]


def greet(devices):
    for device in devices:
        pl.semaphore_signal(pltpu.get_barrier_semaphore(), inc=1, device_id=device, device_id_type=MESH)


def remote(src, dst, send, recv, device):
    return pltpu.make_async_remote_copy(src_ref=src, dst_ref=dst, send_sem=send, recv_sem=recv, device_id=device, device_id_type=MESH)


class Gather:
    def __init__(self, side, rows, widths, by_rows):
        self.side, self.widths, self.by_rows = side, widths, by_rows
        n = side - 1
        self.shape = (side, side, rows, sum(widths))
        self.scratch = [pltpu.VMEM(self.shape, BF16), pltpu.SemaphoreType.DMA((len(widths) + 1,)), pltpu.SemaphoreType.DMA((2, 4, n)),
                        pltpu.SemaphoreType.DMA((2, 4, n))]

    def run(self, stage, place, layer, shards, result, scratch):
        out, local, send, recv = scratch
        copies, column = [], 0
        for n, (shard, width) in enumerate(zip(shards, self.widths, strict=True)):
            copies.append((shard.at[layer], out.at[place.x, place.y, :, column : column + width], local.at[n]))
            column += width
        copied = (out, result.at[layer], local.at[len(shards)])
        if stage == 0:
            for c in copies:
                pltpu.make_async_copy(*c).start()
            return
        first, second, near, far = [], [], [], []
        come = [[], [], [], []]
        size = out.shape[2] if self.by_rows else out.shape[3]
        every = slice(None)
        for q in range(2):

            def view(at, core):
                piece = pl.ds(pl.multiple_of(core * (size // 2) + q * (size // 4), size // 4), size // 4)
                return out.at[at[0], at[1], piece, :] if self.by_rows else out.at[at[0], at[1], :, piece]

            def along(at):
                return (at, place.y) if q == 0 else (place.x, at)

            def across(at):
                return (every, at) if q == 0 else (at, every)

            for k in range(1, self.side):
                sems = lambda kind: (send.at[q, kind, k - 1], recv.at[q, kind, k - 1])
                _, to = place.on(q, k)
                back, _ = place.on(q, self.side - k)
                here, got, theirs = view((place.x, place.y), place.core), view(along(back), place.core), view(along(back), 1 - place.core)
                first.append((here, here, *sems(0), to))
                come[0].append((got, got, *sems(0), to))
                near.append((got, got, *sems(2), place.partner))
                come[2].append((theirs, theirs, *sems(2), place.partner))
                _, to = place.on(1 - q, k)
                back, _ = place.on(1 - q, self.side - k)
                mine, got, theirs = view(across(place.y if q == 0 else place.x), place.core), view(across(back), place.core), view(across(back), 1 - place.core)
                second.append((mine, mine, *sems(1), to))
                come[1].append((got, got, *sems(1), to))
                far.append((got, got, *sems(3), place.partner))
                come[3].append((theirs, theirs, *sems(3), place.partner))
        if stage == 1:
            for c in copies:
                pltpu.make_async_copy(*c).wait()
            for c in first:
                remote(*c).start()
        elif stage == 2:
            for c in come[0]:
                remote(*c).wait_recv()
            for c in second + near:
                remote(*c).start()
        elif stage == 3:
            for c, f in zip(come[1], far, strict=True):
                remote(*c).wait_recv()
                remote(*f).start()
        elif stage == 4:
            for c in come[2] + come[3]:
                remote(*c).wait_recv()
            pltpu.make_async_copy(*copied).start()
        else:
            pltpu.make_async_copy(*copied).wait()
            for c in first + second + near + far:
                remote(*c).wait_send()


class Crossed:
    def __init__(self, side, rows, width):
        self.side, self.width = side, width
        n, half = side - 1, width // 2
        self.scratch = [pltpu.VMEM((2, n, side, rows, half), BF16), pltpu.VMEM((2, side, rows, half), BF16), pltpu.VMEM((2, n, rows, half), BF16),
                        pltpu.VMEM((2, rows, half), F32), pltpu.SemaphoreType.DMA((2, 2, n)), pltpu.SemaphoreType.DMA((2, 2, n))]

    def run(self, stage, place, src, out, scratch):
        one, mid, two, own, send, recv = scratch
        n, half = self.side - 1, self.width // 2
        pairs = [(q, k, *place.on(q, k + 1)) for q in range(2) for k in range(n)]
        if stage < 2:
            firsts = [remote(src.at[there, :, :, :half] if q == 0 else src.at[:, there, :, half:], one.at[q, k], send.at[0, q, k], recv.at[0, q, k], to)
                      for q, k, there, to in pairs]
        if stage > 0:
            pairs = [(q, k, *place.on(1 - q, k + 1)) for q in range(2) for k in range(n)]
            seconds = [remote(mid.at[q, there], two.at[q, k], send.at[1, q, k], recv.at[1, q, k], to) for q, k, there, to in pairs]
        if stage == 0:
            for c in firsts:
                c.start()
        elif stage == 1:
            for c in firsts:
                c.wait()
            for q in range(2):

                def total(j):
                    t = (src[place.x, j, :, :half] if q == 0 else src[j, place.y, :, half:]).astype(F32)
                    for k in range(n):
                        t += one[q, k, j].astype(F32)
                    return t

                def add(j, _):
                    mid[q, j] = total(j).astype(BF16)

                lax.fori_loop(0, self.side, add, None)
                own[q] = total(place.y if q == 0 else place.x)
            for c in seconds:
                c.start()
        else:
            for c in seconds:
                c.wait()
            for q in range(2):
                t = own[q]
                for k in range(n):
                    t += two[q, k].astype(F32)
                out[:, q * half : (q + 1) * half] = t.astype(BF16)


class Lined:
    def __init__(self, side, rows, width):
        self.side = side
        n = side - 1
        self.scratch = [pltpu.VMEM((n, rows, width), BF16), pltpu.VMEM((rows, width), BF16), pltpu.VMEM((n, rows, width), BF16),
                        pltpu.VMEM((rows, width), F32), pltpu.SemaphoreType.DMA((2, n)), pltpu.SemaphoreType.DMA((2, n))]

    def run(self, stage, place, line, src, out, scratch):
        one, mid, two, own, send, recv = scratch
        n = self.side - 1
        ahead = lax.rem(line - place.x + self.side, self.side)

        def firsts():
            for k in range(n):
                there, to = place.on(1, k + 1)
                yield remote(src.at[there], one.at[k], send.at[0, k], recv.at[0, k], to)

        def second():
            return remote(mid, two.at[ahead - 1], send.at[1, 0], recv.at[1, ahead - 1], place.on(0, ahead)[1])

        if stage == 0:
            for c in firsts():
                c.start()
        elif stage == 1:
            for c in firsts():
                c.wait()
            t = src[place.y].astype(F32)
            for k in range(n):
                t += one[k].astype(F32)
            own[...] = t
            mid[...] = t.astype(BF16)
            pl.when(ahead != 0)(lambda: second().start())
        else:
            pl.when(ahead != 0)(lambda: second().wait_send())

            @pl.when(ahead == 0)
            def _():
                t = own[...]
                for k in range(n):
                    remote(mid, two.at[k], send.at[1, 0], recv.at[1, k], place.on(0, 0)[1]).wait_recv()
                    t += two[k].astype(F32)
                out[...] = t.astype(BF16)


def taken(refs, *counts):
    out, at = [], 0
    for n in counts:
        out.append(refs[at : at + n])
        at += n
    return out


def forward(cid, side, x, weights):
    t, d = x.shape
    layers, width = weights[0].shape[0], weights[0].shape[2]
    f = weights[4].shape[2]
    nh, n = width // HEAD, t // ROWS
    shard = d // side**2
    tasks = [Gather(side, shard, [width] * 4, False), Gather(side, shard, [f, f], False), Gather(side, f // side**2, [d], True)]
    flat = [s for _ in range(layers) for task in tasks for s in task.scratch]
    own = [pltpu.VMEM((t, width), BF16), pltpu.VMEM((nh, HEAD + 8, t), BF16), pltpu.VMEM((nh, ROWS), F32), pltpu.VMEM((nh, HEAD + 8, ROWS), F32),
           pltpu.VMEM((t, width), BF16), pltpu.VMEM((t, d), BF16), pltpu.VMEM((ROWS, f), BF16)]
    tabs = tables(t)

    def body(*refs):
        (x_ref, *rest) = refs
        tab, shards, outs, scratch, moved = taken(rest, 4, 7, 7, len(own), len(flat))
        qkv_ref, o_ref, lse_ref, h_ref, *wholes = outs
        k_s, vt_s, top_s, mix_s, o_s, h2_s, act_s = scratch
        moved = [taken(m, 4, 4, 4) for m in taken(moved, 12, 12)]
        parts = [shards[:4], shards[4:6], shards[6:]]
        step = pl.program_id(0)

        def go(layer, kind, *stages):
            for stage in stages:
                tasks[kind].run(stage, Place(side), layer, parts[kind], wholes[kind], moved[layer][kind])

        def at(number):
            return pl.when(step == number)

        @at(0)
        def _():
            place = Place(side)
            peers = [*place.line(), place.partner]
            greet(peers)
            for layer in range(layers):
                for kind in range(3):
                    go(layer, kind, 0)
            pl.semaphore_wait(pltpu.get_barrier_semaphore(), len(peers))
            go(0, 0, 1, 2)
            go(0, 1, 1)
            go(0, 2, 1)
            go(0, 0, 3, 4)
            for m in range(nh):
                vt_s[m, HEAD:, :] = jnp.ones((8, t), BF16)

        @at(n)
        def _():
            for stage in (3, 4):
                go(0, 1, stage)
                go(0, 2, stage)

        def matrix(layer, kind):
            return moved[layer][kind][0]

        second = step >= 2 * n

        @pl.when((step < n) | second)
        def _():
            i = lax.rem(step, n)
            here = tile_at(i)

            def project(h, w):
                h = h.astype(F32)
                a = (h * scale_of(h)).astype(BF16)
                qkv_ref[0] = dot(a, w[:, :, :, : 3 * width].reshape(d, 3 * width)).astype(BF16)

            @pl.when(~second)
            def _():
                h_ref[0] = x_ref[...]
                project(x_ref[...], matrix(0, 0))

            pl.when(second)(lambda: project(h2_s[here, :], matrix(1, 0)))
            cos, sin = angles(tab, i)
            qs = []
            for m in range(nh):
                at = slice(m * HEAD, (m + 1) * HEAD)
                key = slice(width + at.start, width + at.stop)
                value = slice(2 * width + at.start, 2 * width + at.stop)
                q = rotated(qkv_ref[0, :, at].astype(F32), cos, sin).astype(BF16) * jnp.asarray(HEAD**-0.5, BF16)
                k = rotated(qkv_ref[0, :, key].astype(F32), cos, sin).astype(BF16)
                vt_s[m, :HEAD, here] = qkv_ref[0, :, value].T
                qkv_ref[0, :, at], qkv_ref[0, :, key] = q, k
                k_s[here, at] = k
                qs.append(q)

            def block(j, first):
                keys = tile_at(j)
                scores = [dot(k_s[keys, m * HEAD : (m + 1) * HEAD], q, 1, 1) for m, q in enumerate(qs)]
                ps, keeps = [], []
                for m, s in enumerate(scores):
                    if first:
                        s = jnp.where(hidden(ROWS), -1e30, s)
                        top = s.max(0, keepdims=True)
                    else:
                        old = top_s[m : m + 1, :]
                        top = jnp.maximum(old, s.max(0, keepdims=True))
                        keeps.append(jnp.exp2((old - top) * LOG2E))
                    top_s[m : m + 1, :] = top
                    ps.append(jnp.exp2((s - top) * LOG2E).astype(BF16))
                for m, p in enumerate(ps):
                    new = dot(vt_s[m, :, keys], p)
                    mix_s[m] = new if first else mix_s[m] * keeps[m] + new

            block(i, True)
            lax.fori_loop(0, i, lambda j, _: block(j, False), None)
            for m in range(nh):
                total = mix_s[m, HEAD : HEAD + 1, :]
                o = (mix_s[m, :HEAD, :] * (1 / total)).T.astype(BF16)
                o_ref[0, :, m * HEAD : (m + 1) * HEAD] = o
                o_s[here, m * HEAD : (m + 1) * HEAD] = o
                lse_ref[0, m : m + 1, :] = top_s[m : m + 1, :] * LOG2E + jnp.log2(total)

        @pl.when((step >= n) & ~second)
        def _():
            here = tile_at(step - n)
            wa, wgu, wd = (matrix(0, kind) for kind in range(3))
            h1 = x_ref[...] + dot(o_s[here, :], wa[:, :, :, 3 * width :].reshape(d, width)).astype(BF16)
            wide = h1.astype(F32)
            b = (wide * scale_of(wide)).astype(BF16)
            cut = f // side
            for c in range(0, f, cut):
                gate = dot(b, wgu[:, :, :, c : c + cut].reshape(d, cut))
                up = dot(b, wgu[:, :, :, f + c : f + c + cut].reshape(d, cut))
                act_s[:, c : c + cut] = (gate * jax.nn.sigmoid(gate) * up).astype(BF16)
            h2 = h1 + dot(act_s[...], wd[...].reshape(f, d)).astype(BF16)
            h_ref[0] = h2
            h2_s[here, :] = h2

        @at(0)
        def _():
            go(0, 1, 2)
            go(0, 2, 2)
            for kind in range(3):
                go(1, kind, 1)

        @at(n)
        def _():
            for kind in range(3):
                go(1, kind, 2)

        @at(2 * n - 2)
        def _():
            go(1, 0, 3)

        @at(2 * n - 1)
        def _():
            go(1, 0, 4)

        @at(3 * n - 3)
        def _():
            go(1, 1, 3)
            go(1, 2, 3)

        @at(3 * n - 2)
        def _():
            go(1, 1, 4)
            go(1, 2, 4)

        @at(3 * n - 1)
        def _():
            for layer in range(layers):
                for kind in range(3):
                    go(layer, kind, 5)

    tile = lambda s: jnp.where(s < 2 * n, jnp.minimum(s, n - 1), s - 2 * n)
    by_layer = lambda w: pl.BlockSpec((1, ROWS, w), lambda s: (s // (2 * n), tile(s), 0))
    got = pl.pallas_call(
        body,
        grid=(3 * n,),
        in_specs=[pl.BlockSpec((ROWS, d), lambda s: (jnp.where(s < 2 * n, lax.rem(s, n), n - 1), 0)), *(whole(a.shape) for a in tabs), *[ANY] * 7],
        out_specs=[by_layer(3 * width), by_layer(width), pl.BlockSpec((1, nh, ROWS), lambda s: (s // (2 * n), 0, tile(s))),
                   pl.BlockSpec((1, ROWS, d), lambda s: (jnp.where(s < n, 0, 1), jnp.where(s < 2 * n, lax.rem(s, n), n - 1), 0)), *[ANY] * 3],
        out_shape=[sds((layers, t, 3 * width), BF16), sds((layers, t, width), BF16), sds((layers, nh, t), F32), sds((layers, t, d), BF16),
                   *(sds((layers, *task.shape), BF16) for task in tasks)],
        scratch_shapes=[*own, *flat],
        compiler_params=pltpu.CompilerParams(dimension_semantics=("arbitrary",), vmem_limit_bytes=VMEM, has_side_effects=True, collective_id=cid),
        name="forward",
    )(x, *tabs, *weights)
    return [*got[:4], *(w.reshape(layers, -1, w.shape[-1]) for w in got[4:])]


def square(g):
    wide = g.astype(F32)
    return jnp.sum(jnp.sum(wide * wide, 0, keepdims=True), 1, keepdims=True)


def backward(cid, side, h, dy, qkv, o, lse, wa, wgu, wd):
    layers, t, d = h.shape
    width = o.shape[2]
    f = wd.shape[1]
    n, nh, cut, group = t // ROWS, width // HEAD, f // side, side * side
    per = 3 * n + side
    gu_shape, d_shape = (side, side, d // group, 2 * cut), (side, f // group, d)
    o_shape, q_shape = (side, side, width // group, d), (side, side, d // group, 3 * width)
    gu_task, d_task = Crossed(side, gu_shape[2], gu_shape[3]), Lined(side, d_shape[1], d)
    o_task, q_task = Crossed(side, o_shape[2], d), Crossed(side, q_shape[2], 3 * width)
    moved = [*gu_task.scratch * 2, *d_task.scratch * 2, *o_task.scratch, *q_task.scratch]
    own = [pltpu.VMEM((t, d), BF16), pltpu.VMEM((d, t), BF16), pltpu.VMEM((t, d), BF16), pltpu.VMEM((d, t), BF16), pltpu.VMEM((t, d), F32),
           pltpu.VMEM((t, d), BF16), pltpu.VMEM((t, cut), BF16), pltpu.VMEM((t, 2 * cut), BF16), pltpu.VMEM((2, *gu_shape), BF16),
           pltpu.VMEM((2, *d_shape), BF16), pltpu.VMEM((width, d), F32), pltpu.VMEM(o_shape, BF16), pltpu.VMEM(q_shape, BF16),
           pltpu.VMEM((t, 3 * width), BF16), pltpu.VMEM((t, width), F32), pltpu.VMEM((d, 3 * width), F32), pltpu.SemaphoreType.DMA((2,)),
           pltpu.VMEM((group, 8, 128), F32), pltpu.VMEM((8, 128), F32), pltpu.SemaphoreType.DMA((group - 1,)), pltpu.SemaphoreType.DMA((group - 1,))]
    tabs = tables(t)

    def body(*refs):
        ins, tab, outs, scratch, moved = taken(refs, 10, 4, 5, len(own), 36)
        h_ref, o_ref, lse_ref, wo_ref, wqkv_ref, wg_ref, wu_ref, wd_ref, dy_ref, qkv_ref = ins
        gq_ref, go_ref, ggu_ref, gd_ref, total_ref = outs
        (b_s, bt_s, g_s, gt_s, by_s, h1_s, act_s, dgu_s, gu_o, d_o, sum_s, wo_o, wqkv_o, qkv_s, dv_s, dw_s, load, slots, part, send, recv) = scratch
        gu_m, gu_m2, d_m, d_m2, o_m, q_m = taken(moved, 6, 6, 6, 6, 6, 6)
        gu_m, d_m = (gu_m, gu_m2), (d_m, d_m2)
        step = pl.program_id(0)
        layer = layers - 1 - lax.div(step, per)
        phase = lax.rem(step, per)
        top = layer == layers - 1
        last = n + side
        load_dy = lambda: pltpu.make_async_copy(dy_ref, g_s, load.at[0])
        load_qkv = lambda: pltpu.make_async_copy(qkv_ref.at[layer], qkv_s, load.at[1])

        def at(number, more=True):
            return pl.when((phase == number) & more)

        @pl.when(step == 0)
        def _():
            load_dy().start()
            greet(Place(side).others())
            load_dy().wait()

        at(0)(lambda: load_qkv().start())

        @pl.when(phase < n)
        def _():
            here = tile_at(phase)
            h1 = h_ref[0] + dot(o_ref[0], wo_ref[0]).astype(BF16)
            h1_s[here, :] = h1
            wide = h1.astype(F32)
            b = (wide * scale_of(wide)).astype(BF16)
            b_s[here, :] = b
            bt_s[:, here] = b.T
            gt_s[:, here] = g_s[here, :].T

        @pl.when((phase >= n) & (phase < last))
        def _():
            chunk = phase - n
            wg, wu = wg_ref[0], wu_ref[0]

            def tile(number, _):
                here = tile_at(number)
                b, g = b_s[here, :], g_s[here, :]
                sub = HEAD
                for c in range(0, cut, sub):
                    cols = slice(c, c + sub)
                    gate, up = dot(b, wg_ref[0, :, cols]), dot(b, wu_ref[0, :, cols])
                    dact = dot(g, wd_ref[0, cols, :], 1, 1)
                    sig = jax.nn.sigmoid(gate)
                    silu = gate * sig
                    act_s[here, cols] = (silu * up).astype(BF16)
                    dgu_s[here, cols] = (dact * up * (sig + silu * (1 - sig))).astype(BF16)
                    dgu_s[here, cut + c : cut + c + sub] = (dact * silu).astype(BF16)
                by = dot(dgu_s[here, :cut], wg, 1, 1) + dot(dgu_s[here, cut:], wu, 1, 1)

                @pl.when(chunk == 0)
                def _():
                    by_s[here, :] = by

                @pl.when(chunk > 0)
                def _():
                    by_s[here, :] += by

            lax.fori_loop(0, n, tile, None)
            slot = lax.rem(chunk, 2)
            for c in range(0, 2 * cut, cut):
                gu_o[slot, :, :, :, c : c + cut] = dot(bt_s[...], dgu_s[:, c : c + cut]).astype(BF16).reshape(*gu_shape[:3], cut)
            d_o[slot] = dot(gt_s[...], act_s[...]).T.astype(BF16).reshape(d_shape)

        do_s, dt_s, kt_s, dk_s, dq_s = h1_s, b_s, bt_s, by_s, sum_s

        @pl.when((phase >= last) & (phase < last + n))
        def _():
            number = phase - last
            here = tile_at(number)
            h1 = h1_s[here, :].astype(F32)
            r = scale_of(h1)
            dh1 = (g_s[here, :].astype(F32) + normed_bwd(h1 * r, r, by_s[here, :])).astype(BF16)
            g_s[here, :] = dh1
            do_s[here, :] = dot(dh1, wo_ref[0], 1, 1).astype(BF16)
            by_wo = dot(o_ref[0].T, dh1)

            @pl.when(number == 0)
            def _():
                sum_s[...] = by_wo

            @pl.when(number > 0)
            def _():
                sum_s[...] += by_wo

            @pl.when(number == n - 1)
            def _():
                wo_o[...] = sum_s[...].astype(BF16).reshape(o_shape)

        heads = [slice(m * HEAD, (m + 1) * HEAD) for m in range(nh)]

        @at(last + n)
        def _():
            load_qkv().wait()
            dk_s[...] = jnp.zeros_like(dk_s)
            dv_s[...] = jnp.zeros_like(dv_s)
            dw_s[...] = jnp.zeros_like(dw_s)
            for j in range(0, t, ROWS):
                for h in heads:
                    kt_s[h, j : j + ROWS] = qkv_s[j : j + ROWS, width + h.start : width + h.stop].T

        @pl.when(phase >= last + n)
        def _():
            i = per - 1 - phase
            here = tile_at(i)
            qs = [qkv_s[here, h] for h in heads]
            dos = [do_s[here, h] for h in heads]
            deltas = []
            for m, h in enumerate(heads):
                delta = (dos[m].astype(F32) * o_ref[0, :, h].astype(F32)).sum(-1, keepdims=True)
                deltas.append(jnp.broadcast_to(delta, (ROWS, 128)).T[:1, :])
            lses = [lse_ref[0, m : m + 1, :] for m in range(nh)]

            def block(j, first):
                keys = tile_at(j)
                scores = [dot(qkv_s[keys, width + h.start : width + h.stop], q, 1, 1) for h, q in zip(heads, qs)]
                dps = [dot(qkv_s[keys, 2 * width + h.start : 2 * width + h.stop], g, 1, 1) for h, g in zip(heads, dos)]
                for m, h in enumerate(heads):
                    p = jnp.exp2(scores[m] * LOG2E - lses[m])
                    if first:
                        p = jnp.where(hidden(ROWS), 0.0, p)
                    ds = (p * (dps[m] - deltas[m])).astype(BF16)
                    dv_s[keys, h] += dot(p.astype(BF16), dos[m])
                    dk_s[keys, h] += dot(ds, qs[m])
                    dq = dot(kt_s[h, keys], ds)
                    dq_s[h, :] = dq if first else dq_s[h, :] + dq

            block(i, True)
            lax.fori_loop(0, i, lambda j, _: block(j, False), None)
            cos, sin = angles(tab, i)
            for h in heads:
                dt_s[:ROWS, h] = rotated((dq_s[h, :] * HEAD**-0.5).T, cos, -sin).astype(BF16)
                dt_s[ROWS : 2 * ROWS, h] = rotated(dk_s[here, h], cos, -sin).astype(BF16)
                dt_s[2 * ROWS : 3 * ROWS, h] = dv_s[here, h].astype(BF16)
            wide = h_ref[0].astype(F32)
            r = scale_of(wide)
            y = wide * r
            yt = y.astype(BF16).T
            thirds = [(slice(k * ROWS, (k + 1) * ROWS), slice(k * width, (k + 1) * width)) for k in range(3)]
            for rows, cols in thirds:
                dw_s[:, cols] += dot(yt, dt_s[rows, :])

            @pl.when(top)
            def _():
                by = sum(dot(dt_s[rows, :], wqkv_ref[0, :, cols], 1, 1) for rows, cols in thirds)
                g_s[here, :] = (g_s[here, :].astype(F32) + normed_bwd(y, r, by)).astype(BF16)

        @at(per - 1)
        def _():
            wqkv_o[...] = dw_s[...].astype(BF16).reshape(q_shape)


        def gu(chunk, *stages):
            for stage in stages:
                gu_task.run(stage, Place(side), gu_o.at[chunk % 2], ggu_ref.at[layer, chunk], gu_m[chunk % 2])

        def down(chunk, *stages):
            for stage in stages:
                d_task.run(stage, Place(side), chunk, d_o.at[chunk % 2], gd_ref.at[layer], d_m[chunk % 2])

        def out(stage):
            o_task.run(stage, Place(side), wo_o, go_ref.at[layer], o_m)

        def qkvs(stage, of):
            q_task.run(stage, Place(side), wqkv_o, gq_ref.at[of], q_m)

        @pl.when(step == n)
        def _():
            pl.semaphore_wait(pltpu.get_barrier_semaphore(), group - 1)

        for c in range(side):

            @at(n + c)
            def _():
                if c >= 2:
                    gu(c - 2, 2)
                    down(c - 2, 2)
                gu(c, 0)
                down(c, 0)
                if c >= 1:
                    down(c - 1, 1)
                    gu(c - 1, 1)

        at(n, ~top)(lambda: qkvs(1, layer + 1))
        at(n + 1, ~top)(lambda: qkvs(2, layer + 1))
        at(last + n - 1)(lambda: out(0))

        @at(last + n)
        def _():
            down(side - 1, 1)
            gu(side - 1, 1)
            gu(side - 2, 2)
            down(side - 2, 2)

        at(last + n + 1)(lambda: out(1))

        @at(last + n + 2)
        def _():
            gu(side - 1, 2)
            down(side - 1, 2)

        @at(per - 1)
        def _():
            out(2)
            qkvs(0, layer)

        @pl.when(step == layers * per - 1)
        def _():
            place = Place(side)
            mine = sum(square(gq_ref[k]) for k in range(1, layers))
            for k in range(layers):
                mine += square(go_ref[k]) + square(gd_ref[k])
                for c in range(side):
                    mine += square(ggu_ref[k, c])
            qkvs(1, 0)
            qkvs(2, 0)
            mine = jnp.broadcast_to(mine + square(gq_ref[0]), part.shape)
            part[...] = mine
            slots[place.me] = mine
            copies = [(part, slots.at[place.me], send.at[k], recv.at[k], device) for k, device in enumerate(place.others())]
            for c in copies:
                remote(*c).start()
            for k, (_, _, s, r, device) in enumerate(copies):
                remote(part, slots.at[lax.rem(place.me + group - k - 1, group)], s, r, device).wait()
            total_ref[...] = slots[...].sum(0)

    layer_of = lambda s: layers - 1 - s // per

    def tile(s, phases):
        p = lax.rem(s, per)
        back = per - 1 - p
        late = jnp.where(p < n + side + n, n - 1, back)
        at_epilogue = jnp.clip(p - n - side, 0, n - 1)
        early = jnp.where(p < n, p, n - 1)
        if phases == "ends":
            return jnp.where(p < n, p, late)
        if phases == "all":
            return jnp.where(p < n, p, jnp.where(p < n + side + n, at_epilogue, back))
        return late

    def chunk(s):
        return jnp.clip(lax.rem(s, per) - n, 0, side - 1)

    cut_of = lambda w, c: pl.BlockSpec((1, d, w), lambda s: (layer_of(s), 0, c(s)))
    single = dict(pipeline_mode=pl.Buffered(1))
    outs = [sds((layers, q_shape[2], 3 * width), BF16), sds((layers, o_shape[2], d), BF16), sds((layers, side, *gu_shape[2:]), BF16),
            sds((layers, *d_shape[1:]), BF16), sds((8, 128), F32)]
    return pl.pallas_call(
        body,
        grid=(layers * per,),
        in_specs=[pl.BlockSpec((1, ROWS, d), lambda s: (layer_of(s), tile(s, "ends"), 0)),
                  pl.BlockSpec((1, ROWS, width), lambda s: (layer_of(s), tile(s, "all"), 0)),
                  pl.BlockSpec((1, nh, ROWS), lambda s: (layer_of(s), 0, tile(s, "late"))),
                  pl.BlockSpec((1, d, width), lambda s: (layer_of(s), 0, 3), **single),
                  pl.BlockSpec((1, d, 3 * width), lambda s: (layer_of(s), 0, 0), **single),
                  cut_of(cut, chunk), cut_of(cut, lambda s: side + chunk(s)), pl.BlockSpec((1, cut, d), lambda s: (layer_of(s), chunk(s), 0)),
                  ANY, ANY, *(whole(a.shape) for a in tabs)],
        out_specs=[whole(a.shape) for a in outs],
        out_shape=outs,
        scratch_shapes=[*own, *moved],
        compiler_params=pltpu.CompilerParams(dimension_semantics=("arbitrary",), vmem_limit_bytes=VMEM, has_side_effects=True, collective_id=cid),
        name="backward",
    )(h, o, lse, wa, wa, wgu, wgu, wd, dy, qkv, *tabs)


def adamw(total, count, weights, m, v, gq, go, ggu, gd):
    layers, side = ggu.shape[:2]

    def body(total_ref, gq_ref, go_ref, ggu_ref, gd_ref, *refs):
        w_refs, m_refs, v_refs, wn_refs, mn_refs, vn_refs = taken(refs, *[7] * 6)
        factor = jnp.minimum(1.0, 0.5 * lax.rsqrt(total_ref[0:1, 0:1] / count + 1e-30))

        def update(i, columns, g):
            g = g.astype(F32) * factor
            at = (0, slice(None), columns)
            mn = 0.9 * m_refs[i][at] + 0.1 * g
            vn = 0.95 * v_refs[i][at] + 0.05 * g * g
            mn_refs[i][at], vn_refs[i][at] = mn, vn
            w = w_refs[i][at].astype(F32)
            wn_refs[i][at] = (w - 0.02 * (mn * lax.rsqrt(vn + 1e-8) + 0.1 * w)).astype(BF16)

        every = slice(None)
        wide = gq_ref.shape[2] // 3
        for i in range(3):
            update(i, every, gq_ref[0, :, i * wide : (i + 1) * wide])
        update(3, every, go_ref[0])
        cut = ggu_ref.shape[3] // 2
        for c in range(side):
            for i in range(2):
                update(4 + i, slice(c * cut, (c + 1) * cut), ggu_ref[0, c, :, i * cut : (i + 1) * cut])
        update(6, every, gd_ref[0])

    one = lambda a: pl.BlockSpec((1, *a.shape[1:]), lambda l: (l,) + (0,) * (a.ndim - 1))
    own = [one(a) for a in weights]
    return pl.pallas_call(
        body,
        grid=(layers,),
        in_specs=[whole(total.shape), *(one(a) for a in (gq, go, ggu, gd)), *own * 3],
        out_specs=own * 3,
        out_shape=[*(sds(a.shape, BF16) for a in weights), *(sds(a.shape, F32) for a in (*m, *v))],
        compiler_params=pltpu.CompilerParams(dimension_semantics=("arbitrary",), vmem_limit_bytes=VMEM),
        name="adamw",
    )(total, gq, go, ggu, gd, *weights, *m, *v)


def solution(mesh):
    group = mesh.shape["dp"]
    side = side_of(group)

    def step(x, dy, *arrays):
        weights, m, v = (arrays[i : i + 7] for i in (0, 7, 14))
        x, dy = x[0], dy[0]
        qkv, o, lse, h, wa, wgu, wd = forward(0, side, x, weights)
        *grads, total = backward(1, side, h, dy, qkv, o, lse, wa, wgu, wd)
        return tuple(adamw(total, group * sum(w.size for w in weights), weights, m, v, *grads))

    states, cut = P(("rep", "dp"), None, None), P(None, "dp", None)
    return jax.shard_map(
        step,
        mesh=mesh,
        in_specs=(states, states) + (cut,) * 21,
        out_specs=(P("rep", "dp", None),) * 21,
        check_vma=False,
    )
```

```python
import functools

import jax
import jax.numpy as jnp
import numpy as np
from jax import lax
from jax.experimental import pallas as pl
from jax.experimental.pallas import tpu as pltpu
from jax.sharding import PartitionSpec as P

HEAD = 256
THETA = 10000
LOG2E = 1.4426950408889634
VMEM = 67_000_000
EPS = 1e-6
F32, BF16 = jnp.float32, jnp.bfloat16
MESH = pl.DeviceIdType.MESH
ANY = pl.BlockSpec(memory_space=pl.ANY)
ROWS = 512
SLOTS = 3
sds = jax.ShapeDtypeStruct


def dot(a, b, ca=1, cb=0):
    return lax.dot_general(a, b, (((ca,), (cb,)), ((), ())), preferred_element_type=F32)


def scale_of(h):
    return lax.rsqrt(jnp.mean(h * h, -1, keepdims=True) + EPS)


def normed_bwd(y, r, by):
    return r * (by - y * jnp.mean(by * y, -1, keepdims=True))


def table(tokens):
    half = HEAD // 2
    rate = np.float32(THETA) ** (-np.arange(half, dtype=np.float32) / np.float32(half))
    places = [np.arange(0, ROWS), np.arange(0, tokens, ROWS)]
    return jnp.asarray(np.concatenate([f(p[:, None] * rate.astype(np.float64)) for p in places for f in (np.cos, np.sin)]), F32)


def angles(ref, tile):
    n = ref.shape[0] // 2 - ROWS
    near_c, near_s = ref[:ROWS, :], ref[ROWS : 2 * ROWS, :]
    c, s = ref[pl.ds(2 * ROWS + tile, 1), :], ref[pl.ds(2 * ROWS + n + tile, 1), :]
    return c * near_c - s * near_s, s * near_c + c * near_s


def rotated(t, cos, sin):
    half = t.shape[-1] // 2
    a, b = t[:, :half], t[:, half:]
    return jnp.concatenate([a * cos - b * sin, b * cos + a * sin], -1)


def hidden(size):
    return lax.broadcasted_iota(jnp.int32, (size, size), 0) > lax.broadcasted_iota(jnp.int32, (size, size), 1)


def tile_at(n, size=ROWS):
    return pl.ds(pl.multiple_of(n * size, size), size)


def whole(shape):
    return pl.BlockSpec(shape, lambda *_: (0,) * len(shape), pipeline_mode=pl.Buffered(1))


def side_of(group):
    return int(round(group**0.5))


class Place:
    def __init__(self, side):
        rep, me = lax.axis_index("rep"), lax.axis_index("dp")
        self.side, self.me, self.x, self.y, self.core = side, me, lax.div(me, side), lax.rem(me, side), lax.rem(rep, 2)
        self.partner = {"rep": rep + 1 - 2 * self.core}

    def on(self, axis, k):
        at = lax.rem((self.x, self.y)[axis] + k, self.side)
        return at, {"dp": at * self.side + self.y if axis == 0 else self.x * self.side + at}

    def line(self):
        return [self.on(axis, k)[1] for axis in (0, 1) for k in range(1, self.side)]

    def others(self):
        n = self.side**2
        return [{"dp": lax.rem(self.me + k, n)} for k in range(1, n)]


def greet(devices):
    for device in devices:
        pl.semaphore_signal(pltpu.get_barrier_semaphore(), inc=1, device_id=device, device_id_type=MESH)


def remote(src, dst, send, recv, device):
    return pltpu.make_async_remote_copy(src_ref=src, dst_ref=dst, send_sem=send, recv_sem=recv, device_id=device, device_id_type=MESH)


def arrive(ref, sem):
    pltpu.make_async_copy(ref, ref, sem).wait()


def arrived(ref, send, recv, device):
    c = remote(ref, ref, recv if send is None else send, send if recv is None else recv, device)
    if recv is not None:
        c.wait_recv()
    if send is not None:
        c.wait_send()


class Gather:
    def __init__(self, side, rows, widths, by_rows, relayed):
        self.side, self.widths, self.by_rows, self.relayed = side, widths, by_rows, relayed
        n = side - 1
        self.shape = (side, side, rows, sum(widths))
        self.matrix = pltpu.VMEM(self.shape, BF16)
        self.sems = [pltpu.SemaphoreType.DMA((k,)) for k in (len(widths) + 1, 2, 2, 2 * n, 2, 2)]

    def run(self, stage, place, layer, shards, result, out, sems):
        local, send, come, across, near, far = sems
        n = self.side - 1
        copies, column = [], 0
        for k, (shard, width) in enumerate(zip(shards, self.widths, strict=True)):
            copies.append((shard.at[layer], out.at[place.x, place.y, :, column : column + width], local.at[k]))
            column += width
        copied = (out, result.at[layer], local.at[len(shards)])
        if stage == 0:
            for c in copies:
                pltpu.make_async_copy(*c).start()
        elif stage == 1:
            for c in copies:
                pltpu.make_async_copy(*c).wait()
        elif stage == 6:
            pltpu.make_async_copy(*copied).wait()
            arrived(out.at[0, :n], send.at[0], None, place.partner)
            arrived(out.at[:n], send.at[1], None, place.partner)
        size = out.shape[2] if self.by_rows else out.shape[3]
        every = slice(None)
        for q in range(2):

            def view(at, core=place.core):
                piece = pl.ds(pl.multiple_of(core * (size // 2) + q * (size // 4), size // 4), size // 4)
                return out.at[at[0], at[1], piece, :] if self.by_rows else out.at[at[0], at[1], :, piece]

            along = lambda at: (at, place.y) if q == 0 else (place.x, at)
            over = lambda at: (every, at) if q == 0 else (at, every)
            here, line = view((place.x, place.y)), view(over(place.y if q == 0 else place.x))
            if stage == 1:
                for k in range(1, n + 1):
                    remote(here, here, send.at[0], come.at[q], place.on(q, k)[1]).start()
            elif stage == 2:
                arrived(view((0, slice(0, n))), None, come.at[q], place.partner)
                for k in (1, n) if self.relayed else range(1, n + 1):
                    remote(line, line, send.at[1], across.at[q * n + k - 1], place.on(1 - q, k)[1]).start()
                for k in range(1, n + 1):
                    got = view(along(place.on(q, k)[0]))
                    remote(got, got, send.at[0], near.at[q], place.partner).start()
            elif stage in (3, 4):
                for k in ((1, n) if stage == 3 else (2,)) if self.relayed else range(1, n + 1) if stage == 3 else ():
                    at = place.on(1 - q, self.side - k)[0]
                    got = view(over(at))
                    arrived(got, None, across.at[q * n + k - 1], place.partner)
                    if self.relayed and stage == 3:
                        half = slice(0, self.side // 2) if k == 1 else slice(self.side // 2, self.side)
                        part = view((half, at) if q == 0 else (at, half))
                        remote(part, part, send.at[1], across.at[q * n + 1], place.on(1 - q, k)[1]).start()
                    remote(got, got, send.at[1], far.at[q], place.partner).start()
            elif stage == 5:
                arrived(view((0, slice(0, n))), None, near.at[q], place.partner)
                arrived(view((slice(0, n), every)), None, far.at[q], place.partner)
        if stage == 5:
            pltpu.make_async_copy(*copied).start()


class Ring:
    def __init__(self, half):
        self.scratch = [pltpu.VMEM((2, *half), BF16), pltpu.VMEM((2, *half), BF16), pltpu.VMEM((2, 2, *half), BF16), pltpu.SemaphoreType.DMA((2,)),
                        pltpu.SemaphoreType.DMA((2,))]

    def start(self, place, axis, blocks, scratch, last=False):
        far, mid, near, send, recv = scratch
        opposite, _ = place.on(axis, 2)
        for relayed in (True, False):
            for d, k in enumerate((1, place.side - 1)):
                there, to = place.on(axis, k)
                if last:
                    if relayed:
                        remote(mid.at[d], near.at[d, d], send.at[1], recv.at[1], to).start()
                elif relayed:
                    remote(blocks(opposite, d), far.at[d], send.at[0], recv.at[0], to).start()
                else:
                    remote(blocks(there, 1 - d), near.at[d, 1 - d], send.at[1], recv.at[1], to).start()

    def middle(self, place, axis, blocks, scratch):
        far, mid, near, send, recv = scratch
        arrived(far, send.at[0], recv.at[0], place.on(axis, 1)[1])
        for d, k in enumerate((1, place.side - 1)):
            there, _ = place.on(axis, k)
            mid[d] = (blocks(there, d)[...].astype(F32) + far[d].astype(F32)).astype(BF16)
        self.start(place, axis, blocks, scratch, True)

    def end(self, place, axis, blocks, scratch):
        far, mid, near, send, recv = scratch
        arrived(near, send.at[1], recv.at[1], place.on(axis, 1)[1])

    def total(self, blocks, scratch, at, cut):
        near = scratch[2]
        return blocks(at, cut)[...].astype(F32) + near[0, cut].astype(F32) + near[1, cut].astype(F32)


class Crossed:
    def __init__(self, side, rows, width):
        self.side, self.width = side, width
        n, half = side - 1, width // 2
        self.ring = Ring((side // 2, rows, half))
        self.scratch = [*self.ring.scratch * 2, pltpu.VMEM((2, side, rows, half), BF16), pltpu.VMEM((2, n, rows, half), BF16),
                        pltpu.VMEM((2, rows, half), F32), pltpu.SemaphoreType.DMA((1,)), pltpu.SemaphoreType.DMA((1,))]

    def run(self, stage, place, src, out, scratch):
        *rings, (mid, two, own, send, recv) = taken(scratch, 5, 5, 5)
        n, half, cut = self.side - 1, self.width // 2, self.side // 2
        along = (lambda j, h: src.at[j, h * cut : (h + 1) * cut, :, :half]), (lambda j, h: src.at[h * cut : (h + 1) * cut, j, :, half:])
        for q in range(2):
            at = (place, q, along[q], rings[q])
            if stage == 0:
                self.ring.start(*at)
            elif stage == 1:
                self.ring.middle(*at)
            elif stage == 2:
                self.ring.end(*at)
                for h in range(2):
                    mid[q, h * cut : (h + 1) * cut] = self.ring.total(along[q], rings[q], (place.x, place.y)[q], h).astype(BF16)
                j = (place.y, place.x)[q]
                mine = (src[place.x, place.y, :, :half] if q == 0 else src[place.x, place.y, :, half:]).astype(F32)
                own[q] = mine + sum(rings[q][2][d, lax.div(j, cut), lax.rem(j, cut)].astype(F32) for d in range(2))
        if stage == 2:
            for q in range(2):
                for k in range(n):
                    there, to = place.on(1 - q, k + 1)
                    remote(mid.at[q, there], two.at[q, k], send.at[0], recv.at[0], to).start()
        elif stage == 3:
            arrived(two, send.at[0], recv.at[0], place.on(0, 1)[1])
            for q in range(2):
                t = own[q]
                for k in range(n):
                    t += two[q, k].astype(F32)
                out[:, q * half : (q + 1) * half] = t.astype(BF16)


class Lined:
    def __init__(self, side, rows, width):
        self.side, self.rows = side, rows
        n = side - 1
        self.ring = Ring((rows // 2, width))
        self.scratch = [*self.ring.scratch, pltpu.VMEM((rows, width), BF16), pltpu.VMEM((n, rows, width), BF16),
                        pltpu.VMEM((rows, width), F32), pltpu.SemaphoreType.DMA((1,)), pltpu.SemaphoreType.DMA((1,))]

    def run(self, stage, place, line, src, out, scratch):
        ring, (mid, two, own, send, recv) = taken(scratch, 5, 5)
        n, cut = self.side - 1, self.rows // 2
        ahead = lax.rem(line - place.x + self.side, self.side)
        at = (place, 1, lambda j, h: src.at[j, h * cut : (h + 1) * cut, :], ring)

        def second():
            return remote(mid, two.at[ahead - 1], send.at[0], recv.at[0], place.on(0, ahead)[1])

        if stage == 0:
            self.ring.start(*at)
        elif stage == 1:
            self.ring.middle(*at)
        elif stage == 2:
            self.ring.end(*at)
            for h in range(2):
                t = self.ring.total(at[2], ring, place.y, h)
                own[h * cut : (h + 1) * cut, :] = t
                mid[h * cut : (h + 1) * cut, :] = t.astype(BF16)
            pl.when(ahead != 0)(lambda: second().start())
        else:
            pl.when(ahead != 0)(lambda: second().wait_send())

            @pl.when(ahead == 0)
            def _():
                arrived(two, None, recv.at[0], place.on(0, 1)[1])
                t = own[...]
                for k in range(n):
                    t += two[k].astype(F32)
                out[...] = t.astype(BF16)


def taken(refs, *counts):
    out, at = [], 0
    for n in counts:
        out.append(refs[at : at + n])
        at += n
    return out


def forward(cid, side, x, weights):
    t, d = x.shape
    layers, width = weights[0].shape[0], weights[0].shape[2]
    f = weights[4].shape[2]
    nh, n = width // HEAD, t // ROWS
    shard = d // side**2
    tasks = [Gather(side, shard, [width] * 3, False, False), Gather(side, shard, [width], False, True), Gather(side, shard, [f, f], False, True),
             Gather(side, f // side**2, [d], True, True)]
    kinds = len(tasks)
    flat = [task.matrix for _ in range(layers) for task in tasks]
    sems = [s for layer in range(layers) for task in (tasks[1:] if layer else tasks) for s in task.sems]
    own = [pltpu.VMEM((t, width), BF16), pltpu.VMEM((nh, HEAD + 8, t), BF16), pltpu.VMEM((nh, ROWS), F32), pltpu.VMEM((nh, HEAD + 8, ROWS), F32),
           pltpu.VMEM((t, width), BF16), pltpu.VMEM((t, d), BF16), pltpu.VMEM((ROWS, f), BF16)]
    tab = table(t)

    def body(*refs):
        (x_ref, *rest) = refs
        (tab_ref,), shards, outs, scratch, moved = taken(rest, 1, 7, 4 + kinds, len(own), len(flat) + len(sems))
        qkv_ref, o_ref, lse_ref, h_ref, *wholes = outs
        k_s, vt_s, top_s, mix_s, o_s, h2_s, act_s = scratch
        matrices = taken(moved, *[kinds] * layers)
        flags = taken(moved[kinds * layers :], *[6] * (layers * (kinds - 1) + 1))
        parts = [shards[:3], shards[3:4], shards[4:6], shards[6:]]
        step = pl.program_id(0)

        def go(layer, which, *stages):
            for stage in stages:
                for kind in which:
                    tasks[kind].run(stage, Place(side), layer, parts[kind], wholes[kind], matrices[layer][kind], flags[kind + (kinds - 1) * layer * (kind > 0)])

        def at(number):
            return pl.when(step == number)

        attention, ffn = (0,), (1, 2, 3)

        @at(0)
        def _():
            place = Place(side)
            peers = [*place.line(), place.partner]
            greet(peers)
            go(0, attention + ffn, 0)
            for m in range(nh):
                vt_s[m, HEAD:, :] = jnp.ones((8, t), BF16)
            pl.semaphore_wait(pltpu.get_barrier_semaphore(), len(peers))
            go(0, attention, 1, 2)
            go(0, ffn, 1)
            go(0, attention, 3, 5)

        @at(n)
        def _():
            go(0, ffn, 4, 5)

        def matrix(layer, kind):
            return matrices[layer][kind]

        second = step >= 2 * n

        @pl.when((step < n) | second)
        def _():
            i = lax.rem(step, n)
            here = tile_at(i)

            def project(h, w):
                h = h.astype(F32)
                a = (h * scale_of(h)).astype(BF16)
                qkv_ref[0] = dot(a, w[...].reshape(d, 3 * width)).astype(BF16)

            @pl.when(~second)
            def _():
                h_ref[0] = x_ref[...]
                project(x_ref[...], matrix(0, 0))

            pl.when(second)(lambda: project(h2_s[here, :], matrix(1, 0)))
            cos, sin = angles(tab_ref, i)
            qs = []
            for m in range(nh):
                at = slice(m * HEAD, (m + 1) * HEAD)
                key = slice(width + at.start, width + at.stop)
                value = slice(2 * width + at.start, 2 * width + at.stop)
                q = rotated(qkv_ref[0, :, at].astype(F32), cos, sin).astype(BF16) * jnp.asarray(HEAD**-0.5, BF16)
                k = rotated(qkv_ref[0, :, key].astype(F32), cos, sin).astype(BF16)
                vt_s[m, :HEAD, here] = qkv_ref[0, :, value].T
                qkv_ref[0, :, at], qkv_ref[0, :, key] = q, k
                k_s[here, at] = k
                qs.append(q)

            def block(j, first):
                keys = tile_at(j)
                scores = [dot(k_s[keys, m * HEAD : (m + 1) * HEAD], q, 1, 1) for m, q in enumerate(qs)]
                ps, keeps = [], []
                for m, s in enumerate(scores):
                    if first:
                        s = jnp.where(hidden(ROWS), -1e30, s)
                        top = s.max(0, keepdims=True)
                    else:
                        old = top_s[m : m + 1, :]
                        top = jnp.maximum(old, s.max(0, keepdims=True))
                        keeps.append(jnp.exp2((old - top) * LOG2E))
                    top_s[m : m + 1, :] = top
                    ps.append(jnp.exp2((s - top) * LOG2E).astype(BF16))
                for m, p in enumerate(ps):
                    new = dot(vt_s[m, :, keys], p)
                    mix_s[m] = new if first else mix_s[m] * keeps[m] + new

            block(i, True)
            lax.fori_loop(0, i, lambda j, _: block(j, False), None)
            for m in range(nh):
                total = mix_s[m, HEAD : HEAD + 1, :]
                o = (mix_s[m, :HEAD, :] * (1 / total)).T.astype(BF16)
                o_ref[0, :, m * HEAD : (m + 1) * HEAD] = o
                o_s[here, m * HEAD : (m + 1) * HEAD] = o
                lse_ref[0, m : m + 1, :] = top_s[m : m + 1, :] * LOG2E + jnp.log2(total)

        @pl.when((step >= n) & ~second)
        def _():
            here = tile_at(step - n)
            wo, wgu, wd = (matrix(0, kind) for kind in ffn)
            h1 = x_ref[...] + dot(o_s[here, :], wo[...].reshape(width, d)).astype(BF16)
            wide = h1.astype(F32)
            b = (wide * scale_of(wide)).astype(BF16)
            cut = f // side
            for c in range(0, f, cut):
                gate = dot(b, wgu[:, :, :, c : c + cut].reshape(d, cut))
                up = dot(b, wgu[:, :, :, f + c : f + c + cut].reshape(d, cut))
                act_s[:, c : c + cut] = (gate * jax.nn.sigmoid(gate) * up).astype(BF16)
            h2 = h1 + dot(act_s[...], wd[...].reshape(f, d)).astype(BF16)
            h_ref[0] = h2
            h2_s[here, :] = h2

        plan = {0: [(0, ffn, 2), (0, attention, 6), (1, attention + ffn, 0)], n - 2: [(0, ffn, 3), (1, attention + ffn, 1)],
                n: [(1, attention + ffn, 2)], n + 2: [(1, attention, 3)], 2 * n - 1: [(1, attention, 5), (1, ffn, 3)],
                2 * n + 1: [(1, ffn, 4)], 3 * n - 2: [(1, ffn, 5)], 3 * n - 1: [(0, ffn, 6), (1, attention + ffn, 6)]}
        for number, todo in plan.items():

            @at(number)
            def _():
                for what in todo:
                    go(*what)

    tile = lambda s: jnp.where(s < 2 * n, jnp.minimum(s, n - 1), s - 2 * n)
    by_layer = lambda w: pl.BlockSpec((1, ROWS, w), lambda s: (s // (2 * n), tile(s), 0))
    got = pl.pallas_call(
        body,
        grid=(3 * n,),
        in_specs=[pl.BlockSpec((ROWS, d), lambda s: (jnp.where(s < 2 * n, lax.rem(s, n), n - 1), 0)), whole(tab.shape), *[ANY] * 7],
        out_specs=[by_layer(3 * width), by_layer(width), pl.BlockSpec((1, nh, ROWS), lambda s: (s // (2 * n), 0, tile(s))),
                   pl.BlockSpec((1, ROWS, d), lambda s: (jnp.where(s < n, 0, 1), jnp.where(s < 2 * n, lax.rem(s, n), n - 1), 0)), *[ANY] * kinds],
        out_shape=[sds((layers, t, 3 * width), BF16), sds((layers, t, width), BF16), sds((layers, nh, t), F32), sds((layers, t, d), BF16),
                   *(sds((layers, *task.shape), BF16) for task in tasks)],
        scratch_shapes=[*own, *flat, *sems],
        compiler_params=pltpu.CompilerParams(dimension_semantics=("arbitrary",), vmem_limit_bytes=VMEM, has_side_effects=True, collective_id=cid),
        name="forward",
    )(x, tab, *weights)
    return [*got[:4], *(w.reshape(layers, -1, w.shape[-1]) for w in got[4:])]


def square(g):
    wide = g.astype(F32)
    return jnp.sum(jnp.sum(wide * wide, 0, keepdims=True), 1, keepdims=True)


def backward(cid, side, h, dy, qkv, o, lse, wqkv, wo, wgu, wd):
    layers, t, d = h.shape
    width = o.shape[2]
    f = wd.shape[1]
    n, nh, cut, group = t // ROWS, width // HEAD, f // side, side * side
    per = 3 * n + 2 * side
    gu_shape, d_shape = (side, side, d // group, 2 * cut), (side, f // group, d)
    o_shape, q_shape = (side, side, width // group, d), (side, side, d // group, 3 * width)
    gu_task, d_task = Crossed(side, gu_shape[2], gu_shape[3]), Lined(side, d_shape[1], d)
    o_task, q_task = Crossed(side, o_shape[2], d), Crossed(side, q_shape[2], 3 * width)
    moves = [*gu_task.scratch * SLOTS, *d_task.scratch * SLOTS, *o_task.scratch, *q_task.scratch]
    own = [pltpu.VMEM((t, d), BF16), pltpu.VMEM((d, t), BF16), pltpu.VMEM((t, d), BF16), pltpu.VMEM((d, t), BF16), pltpu.VMEM((t, d), F32),
           pltpu.VMEM((t, d), BF16), pltpu.VMEM((t, max(3 * cut, 3 * width)), BF16), pltpu.VMEM((2, *gu_shape), BF16),
           pltpu.VMEM((2, *d_shape), BF16), pltpu.VMEM((width, d), F32), pltpu.VMEM(o_shape, BF16), pltpu.VMEM(q_shape, BF16),
           pltpu.VMEM((t, width), F32), pltpu.VMEM((d, 3 * width), F32), pltpu.SemaphoreType.DMA((n + 7,)),
           pltpu.VMEM((group, 8, 128), F32), pltpu.VMEM((8, 128), F32), pltpu.SemaphoreType.DMA((1,)), pltpu.SemaphoreType.DMA((1,)),
           pltpu.VMEM((d, 3 * width), BF16), pltpu.VMEM((2 * (ROWS + n), HEAD // 2), F32), pltpu.VMEM((2, d, 2 * cut), BF16), pltpu.VMEM((2, cut, d), BF16)]
    tab = table(t)

    def body(*refs):
        ins, outs, scratch, moved = taken(refs, 10, 5, len(own), len(moves))
        h_ref, o_ref, lse_ref, wo_ref, wqkv_hbm, wgu_hbm, wd_hbm, dy_ref, qkv_ref, tab_hbm = ins
        gq_ref, go_ref, ggu_ref, gd_ref, total_ref = outs
        (b_s, bt_s, g_s, gt_s, by_s, h1_s, wide_s, gu_o, d_o, sum_s, wo_o, wqkv_o, dv_s, dw_s, load, slots, part, send, recv, wqkv_s, tab_ref, wgu_s, wd_s) = scratch
        dgu_s, act_s, qkv_s = wide_s, wide_s, wide_s
        *pairs, o_m, q_m = taken(moved, *[len(gu_task.scratch)] * SLOTS, *[len(d_task.scratch)] * SLOTS, len(o_task.scratch), len(q_task.scratch))
        gu_m, d_m = pairs[:SLOTS], pairs[SLOTS:]
        step = pl.program_id(0)
        layer = layers - 1 - lax.div(step, per)
        phase = lax.rem(step, per)
        top = layer == layers - 1
        last = n + 2 * side
        load_dy = lambda number: pltpu.make_async_copy(dy_ref.at[tile_at(number)], g_s.at[tile_at(number)], load.at[1 + number])

        def load_late():
            return pltpu.make_async_copy(wqkv_hbm.at[layers - 1], wqkv_s, load.at[1 + n]), pltpu.make_async_copy(tab_hbm, tab_ref, load.at[2 + n])

        def load_chunk(layer, chunk, slot):
            for k in range(2):
                cols = pl.ds(pl.multiple_of(k * f + chunk * cut, cut), cut)
                yield pltpu.make_async_copy(wgu_hbm.at[layer, :, cols], wgu_s.at[slot, :, k * cut : (k + 1) * cut], load.at[3 + n + slot])
            yield pltpu.make_async_copy(wd_hbm.at[layer, pl.ds(pl.multiple_of(chunk * cut, cut), cut), :], wd_s.at[slot], load.at[5 + n + slot])

        load_qkv = lambda: pltpu.make_async_copy(qkv_ref.at[layer], qkv_s.at[:, : 3 * width], load.at[0])

        def at(number, more=True):
            return pl.when((phase == number) & more)

        @pl.when(step == 0)
        def _():
            for number in range(n):
                load_dy(number).start()
            for c in (*load_chunk(layer, 0, 0), *load_late()):
                c.start()
            greet(Place(side).others())

        at(last)(lambda: load_qkv().start())

        @pl.when(phase < n)
        def _():
            here = tile_at(phase)
            pl.when(top)(lambda: load_dy(phase).wait())
            h1 = h_ref[0] + dot(o_ref[0], wo_ref[layer]).astype(BF16)
            h1_s[here, :] = h1
            by_s[here, :] = jnp.zeros_like(h1, F32)
            wide = h1.astype(F32)
            b = (wide * scale_of(wide)).astype(BF16)
            b_s[here, :] = b
            bt_s[:, here] = b.T
            gt_s[:, here] = g_s[here, :].T

        chunk = lax.div(phase - n, 2)
        hidden_units = (phase >= n) & (phase < last)

        @pl.when(hidden_units & (lax.rem(phase - n, 2) == 0))
        def _():
            turn = lax.rem(chunk, 2)
            arrive(wgu_s.at[turn], load.at[3 + n + turn])
            arrive(wd_s.at[turn], load.at[5 + n + turn])

            @pl.when((chunk < side - 1) | (layer > 0))
            def _():
                end = chunk == side - 1
                for c in load_chunk(jnp.where(end, layer - 1, layer), jnp.where(end, 0, chunk + 1), 1 - turn):
                    c.start()

            wg, wu, wd = wgu_s.at[turn, :, :cut], wgu_s.at[turn, :, cut:], wd_s.at[turn]

            def tile(number, _):
                here = tile_at(number)
                b, g = b_s[here, :], g_s[here, :]
                sub = HEAD
                for c in range(0, cut, sub):
                    cols = slice(c, c + sub)
                    gate, up = dot(b, wg[:, cols]), dot(b, wu[:, cols])
                    dact = dot(g, wd[cols, :], 1, 1)
                    sig = jax.nn.sigmoid(gate)
                    silu = gate * sig
                    act_s[here, 2 * cut + c : 2 * cut + c + sub] = (silu * up).astype(BF16)
                    dgu_s[here, cols] = (dact * up * (sig + silu * (1 - sig))).astype(BF16)
                    dgu_s[here, cut + c : cut + c + sub] = (dact * silu).astype(BF16)
                by_s[here, :] += dot(dgu_s[here, :cut], wg[...], 1, 1) + dot(dgu_s[here, cut : 2 * cut], wu[...], 1, 1)

            lax.fori_loop(0, n, tile, None, unroll=2)

        @pl.when(hidden_units & (lax.rem(phase - n, 2) == 1))
        def _():
            slot = lax.rem(chunk, 2)
            for c in range(0, 2 * cut, cut):
                gu_o[slot, :, :, :, c : c + cut] = dot(bt_s[...], dgu_s[:, c : c + cut]).astype(BF16).reshape(*gu_shape[:3], cut)
            d_o[slot] = dot(gt_s[...], act_s[:, 2 * cut : 3 * cut]).T.astype(BF16).reshape(d_shape)

        do_s, dt_s, kt_s, dk_s, dq_s = h1_s, b_s, bt_s, by_s, sum_s

        @pl.when((phase >= last) & (phase < last + n))
        def _():
            number = phase - last
            here = tile_at(number)
            h1 = h1_s[here, :].astype(F32)
            r = scale_of(h1)
            dh1 = (g_s[here, :].astype(F32) + normed_bwd(h1 * r, r, by_s[here, :])).astype(BF16)
            g_s[here, :] = dh1
            dk_s[here, :] = jnp.zeros((ROWS, width), F32)
            dv_s[here, :] = jnp.zeros((ROWS, width), F32)
            dw_s[tile_at(number, d // n), :] = jnp.zeros((d // n, 3 * width), F32)
            do_s[here, :] = dot(dh1, wo_ref[layer], 1, 1).astype(BF16)
            by_wo = dot(o_ref[0].T, dh1)

            @pl.when(number == 0)
            def _():
                sum_s[...] = by_wo

            @pl.when(number > 0)
            def _():
                sum_s[...] += by_wo

            @pl.when(number == n - 1)
            def _():
                wo_o[...] = sum_s[...].astype(BF16).reshape(o_shape)

        heads = [slice(m * HEAD, (m + 1) * HEAD) for m in range(nh)]

        @at(last + n)
        def _():
            load_qkv().wait()

            @pl.when(top)
            def _():
                for c in load_late():
                    c.wait()

            for j in range(0, t, ROWS):
                for h in heads:
                    kt_s[h, j : j + ROWS] = qkv_s[j : j + ROWS, width + h.start : width + h.stop].T

        @pl.when(phase >= last + n)
        def _():
            i = per - 1 - phase
            here = tile_at(i)
            qs = [qkv_s[here, h] for h in heads]
            dos = [do_s[here, h] for h in heads]
            deltas = []
            for m, h in enumerate(heads):
                delta = (dos[m].astype(F32) * o_ref[0, :, h].astype(F32)).sum(-1, keepdims=True)
                deltas.append(jnp.broadcast_to(delta, (ROWS, 128)).T[:1, :])
            lses = [lse_ref[layer, m : m + 1, here] for m in range(nh)]

            def block(j, first):
                keys = tile_at(j)
                scores = [dot(qkv_s[keys, width + h.start : width + h.stop], q, 1, 1) for h, q in zip(heads, qs)]
                dps = [dot(qkv_s[keys, 2 * width + h.start : 2 * width + h.stop], g, 1, 1) for h, g in zip(heads, dos)]
                for m, h in enumerate(heads):
                    p = jnp.exp2(scores[m] * LOG2E - lses[m])
                    if first:
                        p = jnp.where(hidden(ROWS), 0.0, p)
                    ds = (p * (dps[m] - deltas[m])).astype(BF16)
                    dv_s[keys, h] += dot(p.astype(BF16), dos[m])
                    dk_s[keys, h] += dot(ds, qs[m])
                    dq = dot(kt_s[h, keys], ds)
                    dq_s[h, :] = dq if first else dq_s[h, :] + dq

            block(i, True)
            lax.fori_loop(0, i, lambda j, _: block(j, False), None)
            cos, sin = angles(tab_ref, i)
            for h in heads:
                dt_s[:ROWS, h] = rotated((dq_s[h, :] * HEAD**-0.5).T, cos, -sin).astype(BF16)
                dt_s[ROWS : 2 * ROWS, h] = rotated(dk_s[here, h], cos, -sin).astype(BF16)
                dt_s[2 * ROWS : 3 * ROWS, h] = dv_s[here, h].astype(BF16)
            wide = h_ref[0].astype(F32)
            r = scale_of(wide)
            y = wide * r
            yt = y.astype(BF16).T
            thirds = [(slice(k * ROWS, (k + 1) * ROWS), slice(k * width, (k + 1) * width)) for k in range(3)]
            for rows, cols in thirds:
                dw_s[:, cols] += dot(yt, dt_s[rows, :])

            @pl.when(top)
            def _():
                by = sum(dot(dt_s[rows, :], wqkv_s[:, cols], 1, 1) for rows, cols in thirds)
                g_s[here, :] = (g_s[here, :].astype(F32) + normed_bwd(y, r, by)).astype(BF16)

        @at(per - 1)
        def _():
            wqkv_o[...] = dw_s[...].astype(BF16).reshape(q_shape)


        def gu(chunk, *stages):
            for stage in stages:
                gu_task.run(stage, Place(side), gu_o.at[chunk % 2], ggu_ref.at[layer, chunk], gu_m[chunk % SLOTS])

        def down(chunk, *stages):
            for stage in stages:
                d_task.run(stage, Place(side), chunk, d_o.at[chunk % 2], gd_ref.at[layer], d_m[chunk % SLOTS])

        def out(stage):
            o_task.run(stage, Place(side), wo_o, go_ref.at[layer], o_m)

        def qkvs(stage, of):
            q_task.run(stage, Place(side), wqkv_o, gq_ref.at[of], q_m)

        @pl.when(step == n)
        def _():
            pl.semaphore_wait(pltpu.get_barrier_semaphore(), group - 1)

        def both(chunk, stage):
            down(chunk, stage)
            gu(chunk, stage)

        plan = {}

        def then(number, do, *args):
            plan.setdefault(number, []).append((do, args))

        for stage in (2, 3, 1, 0):
            for c in range(side):
                when = (n + 2 * c + 1, n + 2 * c + 2, n + 2 * c + 4, n + 2 * c + 6)[stage]
                left = c - side + 1
                if left == -2:
                    when = (when, when, when, last + 2)[stage]
                elif left == -1:
                    when = (when, when, last + 2, last + n)[stage]
                elif left == 0:
                    when = (when, last + n, last + n + 1, last + n + 2)[stage]
                then(when, both, c, stage)
            then(last + n - 1 + stage, out, stage)
        then(per - 1, qkvs, 0, layer)
        for number, todo in plan.items():

            @at(number)
            def _():
                for do, args in todo:
                    do(*args)

        for stage, number in ((1, n), (2, n + 2), (3, n + 4)):
            at(number, ~top)(lambda: qkvs(stage, layer + 1))

        @pl.when(step == layers * per - 1)
        def _():
            place = Place(side)
            mine = sum(square(gq_ref[k]) for k in range(1, layers))
            for k in range(layers):
                mine += square(go_ref[k]) + square(gd_ref[k])
                for c in range(side):
                    mine += square(ggu_ref[k, c])
            qkvs(1, 0)
            qkvs(2, 0)
            qkvs(3, 0)
            mine = jnp.broadcast_to(mine + square(gq_ref[0]), part.shape)
            part[...] = mine
            slots[place.me] = mine
            for device in place.others():
                remote(part, slots.at[place.me], send.at[0], recv.at[0], device).start()
            arrived(slots.at[: group - 1], send.at[0], recv.at[0], place.others()[0])
            total_ref[...] = slots[...].sum(0)

    layer_of = lambda s: layers - 1 - s // per

    def tile(s, phases):
        p = lax.rem(s, per)
        back = per - 1 - p
        late = jnp.where(p < n + 2 * side + n, n - 1, back)
        at_epilogue = jnp.clip(p - n - 2 * side, 0, n - 1)
        early = jnp.where(p < n, p, n - 1)
        if phases == "ends":
            return jnp.where(p < n, p, late)
        if phases == "all":
            return jnp.where(p < n, p, jnp.where(p < n + 2 * side + n, at_epilogue, back))
        return late

    outs = [sds((layers, q_shape[2], 3 * width), BF16), sds((layers, o_shape[2], d), BF16), sds((layers, side, *gu_shape[2:]), BF16),
            sds((layers, *d_shape[1:]), BF16), sds((8, 128), F32)]
    return pl.pallas_call(
        body,
        grid=(layers * per,),
        in_specs=[pl.BlockSpec((1, ROWS, d), lambda s: (layer_of(s), tile(s, "ends"), 0)),
                  pl.BlockSpec((1, ROWS, width), lambda s: (layer_of(s), tile(s, "all"), 0)),
                  whole(lse.shape), whole(wo.shape), ANY, ANY, ANY, ANY, ANY, ANY],
        out_specs=[whole(a.shape) for a in outs],
        out_shape=outs,
        scratch_shapes=[*own, *moves],
        compiler_params=pltpu.CompilerParams(dimension_semantics=("arbitrary",), vmem_limit_bytes=VMEM, has_side_effects=True, collective_id=cid),
        name="backward",
    )(h, o, lse, wo, wqkv, wgu, wd, dy, qkv, tab)


def adamw(total, count, weights, m, v, gq, go, ggu, gd):
    layers, side = ggu.shape[:2]

    def body(total_ref, gq_ref, go_ref, ggu_ref, gd_ref, *refs):
        w_refs, m_refs, v_refs, wn_refs, mn_refs, vn_refs = taken(refs, *[7] * 6)
        factor = jnp.minimum(1.0, 0.5 * lax.rsqrt(total_ref[0:1, 0:1] / count + 1e-30))

        def update(i, columns, g):
            g = g.astype(F32) * factor
            at = (0, slice(None), columns)
            mn = 0.9 * m_refs[i][at] + 0.1 * g
            vn = 0.95 * v_refs[i][at] + 0.05 * g * g
            mn_refs[i][at], vn_refs[i][at] = mn, vn
            w = w_refs[i][at].astype(F32)
            wn_refs[i][at] = (w - 0.02 * (mn * lax.rsqrt(vn + 1e-8) + 0.1 * w)).astype(BF16)

        every = slice(None)
        wide = gq_ref.shape[2] // 3
        for i in range(3):
            update(i, every, gq_ref[0, :, i * wide : (i + 1) * wide])
        update(3, every, go_ref[0])
        cut = ggu_ref.shape[3] // 2
        for c in range(side):
            for i in range(2):
                update(4 + i, slice(c * cut, (c + 1) * cut), ggu_ref[0, c, :, i * cut : (i + 1) * cut])
        update(6, every, gd_ref[0])

    one = lambda a: pl.BlockSpec((1, *a.shape[1:]), lambda l: (l,) + (0,) * (a.ndim - 1))
    own = [one(a) for a in weights]
    return pl.pallas_call(
        body,
        grid=(layers,),
        in_specs=[whole(total.shape), *(one(a) for a in (gq, go, ggu, gd)), *own * 3],
        out_specs=own * 3,
        out_shape=[*(sds(a.shape, BF16) for a in weights), *(sds(a.shape, F32) for a in (*m, *v))],
        compiler_params=pltpu.CompilerParams(dimension_semantics=("arbitrary",), vmem_limit_bytes=VMEM),
        name="adamw",
    )(total, gq, go, ggu, gd, *weights, *m, *v)


def solution(mesh):
    group = mesh.shape["dp"]
    side = side_of(group)

    def step(x, dy, *arrays):
        weights, m, v = (arrays[i : i + 7] for i in (0, 7, 14))
        x, dy = x[0], dy[0]
        qkv, o, lse, h, wqkv, wo, wgu, wd = forward(0, side, x, weights)
        *grads, total = backward(1, side, h, dy, qkv, o, lse, wqkv, wo, wgu, wd)
        return tuple(adamw(total, group * sum(w.size for w in weights), weights, m, v, *grads))

    states, cut = P(("rep", "dp"), None, None), P(None, "dp", None)
    return jax.shard_map(
        step,
        mesh=mesh,
        in_specs=(states, states) + (cut,) * 21,
        out_specs=(P("rep", "dp", None),) * 21,
        check_vma=False,
    )
```

```python
import functools

import jax
import jax.numpy as jnp
import numpy as np
from jax import lax
from jax.experimental import pallas as pl
from jax.experimental.pallas import tpu as pltpu
from jax.sharding import PartitionSpec as P

HEAD = 256
THETA = 10000
LOG2E = 1.4426950408889634
VMEM = 67_000_000
EPS = 1e-6
F32, BF16 = jnp.float32, jnp.bfloat16
MESH = pl.DeviceIdType.MESH
ANY = pl.BlockSpec(memory_space=pl.ANY)
ROWS = 512
STRIP = 256
SLOTS = 3
sds = jax.ShapeDtypeStruct


def dot(a, b, ca=1, cb=0):
    return lax.dot_general(a, b, (((ca,), (cb,)), ((), ())), preferred_element_type=F32)


def scale_of(h):
    return lax.rsqrt(jnp.mean(h * h, -1, keepdims=True) + EPS)


def normed_bwd(y, r, by):
    return r * (by - y * jnp.mean(by * y, -1, keepdims=True))


def table(tokens):
    half = HEAD // 2
    rate = np.float32(THETA) ** (-np.arange(half, dtype=np.float32) / np.float32(half))
    places = [np.arange(0, ROWS), np.arange(0, tokens, ROWS)]
    return jnp.asarray(np.concatenate([f(p[:, None] * rate.astype(np.float64)) for p in places for f in (np.cos, np.sin)]), F32)


def angles(ref, tile):
    n = ref.shape[0] // 2 - ROWS
    near_c, near_s = ref[:ROWS, :], ref[ROWS : 2 * ROWS, :]
    c, s = ref[pl.ds(2 * ROWS + tile, 1), :], ref[pl.ds(2 * ROWS + n + tile, 1), :]
    return c * near_c - s * near_s, s * near_c + c * near_s


def rotated(t, cos, sin):
    half = t.shape[-1] // 2
    a, b = t[:, :half], t[:, half:]
    return jnp.concatenate([a * cos - b * sin, b * cos + a * sin], -1)


def hidden(size):
    return lax.broadcasted_iota(jnp.int32, (size, size), 0) > lax.broadcasted_iota(jnp.int32, (size, size), 1)


def tile_at(n, size=ROWS):
    return pl.ds(pl.multiple_of(n * size, size), size)


def whole(shape):
    return pl.BlockSpec(shape, lambda *_: (0,) * len(shape), pipeline_mode=pl.Buffered(1))


def side_of(group):
    return int(round(group**0.5))


class Place:
    def __init__(self, side):
        rep, me = lax.axis_index("rep"), lax.axis_index("dp")
        self.side, self.me, self.x, self.y, self.core = side, me, lax.div(me, side), lax.rem(me, side), lax.rem(rep, 2)
        self.partner = {"rep": rep + 1 - 2 * self.core}

    def on(self, axis, k):
        at = lax.rem((self.x, self.y)[axis] + k, self.side)
        return at, {"dp": at * self.side + self.y if axis == 0 else self.x * self.side + at}

    def line(self):
        return [self.on(axis, k)[1] for axis in (0, 1) for k in range(1, self.side)]

    def others(self):
        n = self.side**2
        return [{"dp": lax.rem(self.me + k, n)} for k in range(1, n)]


def greet(devices):
    for device in devices:
        pl.semaphore_signal(pltpu.get_barrier_semaphore(), inc=1, device_id=device, device_id_type=MESH)


def remote(src, dst, send, recv, device):
    return pltpu.make_async_remote_copy(src_ref=src, dst_ref=dst, send_sem=send, recv_sem=recv, device_id=device, device_id_type=MESH)


def arrive(ref, sem):
    pltpu.make_async_copy(ref, ref, sem).wait()


def arrived(ref, send, recv, device):
    c = remote(ref, ref, recv if send is None else send, send if recv is None else recv, device)
    if recv is not None:
        c.wait_recv()
    if send is not None:
        c.wait_send()


class Gather:
    def __init__(self, side, rows, widths, by_rows, relayed):
        self.side, self.widths, self.by_rows, self.relayed = side, widths, by_rows, relayed
        n = side - 1
        self.shape = (side, side, rows, sum(widths))
        self.matrix = pltpu.VMEM(self.shape, BF16)
        self.sems = [pltpu.SemaphoreType.DMA((k,)) for k in (len(widths) + 2, 2, 2, 2 * n, 2, 2)]

    def run(self, stage, place, layer, shards, result, out, sems):
        local, send, come, across, near, far = sems
        n = self.side - 1
        copies, column = [], 0
        for k, (shard, width) in enumerate(zip(shards, self.widths, strict=True)):
            copies.append((shard.at[layer], out.at[place.x, place.y, :, column : column + width], local.at[k]))
            column += width
        size = out.shape[2] if self.by_rows else out.shape[3]
        every = slice(None)

        def copied(own):
            core = place.core if own else 1 - place.core
            piece = pl.ds(pl.multiple_of(core * (size // 2), size // 2), size // 2)
            at = (every, every, piece, every) if self.by_rows else (every, every, every, piece)
            return pltpu.make_async_copy(out.at[at], result.at[(layer, *at)], local.at[len(shards) + own])

        if stage == 0:
            for c in copies:
                pltpu.make_async_copy(*c).start()
        elif stage == 1:
            for c in copies:
                pltpu.make_async_copy(*c).wait()
        elif stage == 6:
            copied(0).wait()
            copied(1).wait()
            arrived(out.at[0, :n], send.at[0], None, place.partner)
            arrived(out.at[:n], send.at[1], None, place.partner)
        for q, waits in [(0, True), (1, True)] * (stage == 2) + [(0, False), (1, False)]:

            def view(at, core=place.core):
                piece = pl.ds(pl.multiple_of(core * (size // 2) + q * (size // 4), size // 4), size // 4)
                return out.at[at[0], at[1], piece, :] if self.by_rows else out.at[at[0], at[1], :, piece]

            along = lambda at: (at, place.y) if q == 0 else (place.x, at)
            over = lambda at: (every, at) if q == 0 else (at, every)
            here, line = view((place.x, place.y)), view(over(place.y if q == 0 else place.x))
            if stage == 1:
                for k in range(1, n + 1):
                    remote(here, here, send.at[0], come.at[q], place.on(q, k)[1]).start()
            elif waits:
                arrived(view((0, slice(0, n))), None, come.at[q], place.partner)
            elif stage == 2:
                for k in (1, n) if self.relayed else range(1, n + 1):
                    remote(line, line, send.at[1], across.at[q * n + k - 1], place.on(1 - q, k)[1]).start()
                for k in range(1, n + 1):
                    got = view(along(place.on(q, k)[0]))
                    remote(got, got, send.at[0], near.at[q], place.partner).start()
            elif stage in (3, 4):
                for k in ((1, n) if stage == 3 else (2,)) if self.relayed else range(1, n + 1) if stage == 3 else ():
                    at = place.on(1 - q, self.side - k)[0]
                    got = view(over(at))
                    arrived(got, None, across.at[q * n + k - 1], place.partner)
                    if self.relayed and stage == 3:
                        half = slice(0, self.side // 2) if k == 1 else slice(self.side // 2, self.side)
                        part = view((half, at) if q == 0 else (at, half))
                        remote(part, part, send.at[1], across.at[q * n + 1], place.on(1 - q, k)[1]).start()
                    remote(got, got, send.at[1], far.at[q], place.partner).start()
            elif stage == 5:
                arrived(view((0, slice(0, n))), None, near.at[q], place.partner)
                arrived(view((slice(0, n), every)), None, far.at[q], place.partner)
        if stage == (4 if self.relayed else 5):
            copied(1).start()
        if stage == 5:
            copied(0).start()


class Ring:
    def __init__(self, half):
        self.scratch = [pltpu.VMEM((2, *half), BF16), pltpu.VMEM((2, *half), BF16), pltpu.VMEM((2, 2, *half), BF16), pltpu.SemaphoreType.DMA((2,)),
                        pltpu.SemaphoreType.DMA((2,))]

    def start(self, place, axis, blocks, scratch, last=False):
        far, mid, near, send, recv = scratch
        opposite, _ = place.on(axis, 2)
        for relayed in (True, False):
            for d, k in enumerate((1, place.side - 1)):
                there, to = place.on(axis, k)
                if last:
                    if relayed:
                        remote(mid.at[d], near.at[d, d], send.at[1], recv.at[1], to).start()
                elif relayed:
                    remote(blocks(opposite, d), far.at[d], send.at[0], recv.at[0], to).start()
                else:
                    remote(blocks(there, 1 - d), near.at[d, 1 - d], send.at[1], recv.at[1], to).start()

    def middle(self, place, axis, blocks, scratch):
        far, mid, near, send, recv = scratch
        arrived(far, send.at[0], recv.at[0], place.on(axis, 1)[1])
        for d, k in enumerate((1, place.side - 1)):
            there, _ = place.on(axis, k)
            mid[d] = (blocks(there, d)[...].astype(F32) + far[d].astype(F32)).astype(BF16)
        self.start(place, axis, blocks, scratch, True)

    def end(self, place, axis, blocks, scratch):
        far, mid, near, send, recv = scratch
        arrived(near, send.at[1], recv.at[1], place.on(axis, 1)[1])

    def total(self, blocks, scratch, at, cut):
        near = scratch[2]
        return blocks(at, cut)[...].astype(F32) + near[0, cut].astype(F32) + near[1, cut].astype(F32)


class Crossed:
    def __init__(self, side, rows, width):
        self.side, self.width = side, width
        n, half = side - 1, width // 2
        self.ring = Ring((side // 2, rows, half))
        self.scratch = [*self.ring.scratch * 2, pltpu.VMEM((2, side, rows, half), BF16), pltpu.VMEM((2, n, rows, half), BF16),
                        pltpu.VMEM((2, rows, half), F32), pltpu.SemaphoreType.DMA((1,)), pltpu.SemaphoreType.DMA((1,))]

    def run(self, stage, place, src, out, scratch):
        *rings, (mid, two, own, send, recv) = taken(scratch, 5, 5, 5)
        n, half, cut = self.side - 1, self.width // 2, self.side // 2
        along = (lambda j, h: src.at[j, h * cut : (h + 1) * cut, :, :half]), (lambda j, h: src.at[h * cut : (h + 1) * cut, j, :, half:])
        for q in range(2):
            at = (place, q, along[q], rings[q])
            if stage == 0:
                self.ring.start(*at)
            elif stage == 1:
                self.ring.middle(*at)
            elif stage == 2:
                self.ring.end(*at)
                for h in range(2):
                    mid[q, h * cut : (h + 1) * cut] = self.ring.total(along[q], rings[q], (place.x, place.y)[q], h).astype(BF16)
                j = (place.y, place.x)[q]
                mine = (src[place.x, place.y, :, :half] if q == 0 else src[place.x, place.y, :, half:]).astype(F32)
                own[q] = mine + sum(rings[q][2][d, lax.div(j, cut), lax.rem(j, cut)].astype(F32) for d in range(2))
        if stage == 2:
            for q in range(2):
                for k in range(n):
                    there, to = place.on(1 - q, k + 1)
                    remote(mid.at[q, there], two.at[q, k], send.at[0], recv.at[0], to).start()
        elif stage == 3:
            arrived(two, send.at[0], recv.at[0], place.on(0, 1)[1])
            for q in range(2):
                t = own[q]
                for k in range(n):
                    t += two[q, k].astype(F32)
                out[:, q * half : (q + 1) * half] = t.astype(BF16)


class Lined:
    def __init__(self, side, rows, width):
        self.side, self.rows = side, rows
        n = side - 1
        self.ring = Ring((rows // 2, width))
        self.scratch = [*self.ring.scratch, pltpu.VMEM((rows, width), BF16), pltpu.VMEM((n, rows, width), BF16),
                        pltpu.VMEM((rows, width), F32), pltpu.SemaphoreType.DMA((1,)), pltpu.SemaphoreType.DMA((1,))]

    def run(self, stage, place, line, src, out, scratch):
        ring, (mid, two, own, send, recv) = taken(scratch, 5, 5)
        n, cut = self.side - 1, self.rows // 2
        ahead = lax.rem(line - place.x + self.side, self.side)
        at = (place, 1, lambda j, h: src.at[j, h * cut : (h + 1) * cut, :], ring)

        def second():
            return remote(mid, two.at[ahead - 1], send.at[0], recv.at[0], place.on(0, ahead)[1])

        if stage == 0:
            self.ring.start(*at)
        elif stage == 1:
            self.ring.middle(*at)
        elif stage == 2:
            self.ring.end(*at)
            for h in range(2):
                t = self.ring.total(at[2], ring, place.y, h)
                own[h * cut : (h + 1) * cut, :] = t
                mid[h * cut : (h + 1) * cut, :] = t.astype(BF16)
            pl.when(ahead != 0)(lambda: second().start())
        else:
            pl.when(ahead != 0)(lambda: second().wait_send())

            @pl.when(ahead == 0)
            def _():
                arrived(two, None, recv.at[0], place.on(0, 1)[1])
                t = own[...]
                for k in range(n):
                    t += two[k].astype(F32)
                out[...] = t.astype(BF16)


def taken(refs, *counts):
    out, at = [], 0
    for n in counts:
        out.append(refs[at : at + n])
        at += n
    return out


def forward(cid, side, x, weights):
    t, d = x.shape
    layers, width = weights[0].shape[0], weights[0].shape[2]
    f = weights[4].shape[2]
    nh, n = width // HEAD, t // ROWS
    shard = d // side**2
    tasks = [Gather(side, shard, [width] * 3, False, False), Gather(side, shard, [width], False, True), Gather(side, shard, [f, f], False, True),
             Gather(side, f // side**2, [d], True, True)]
    kinds = len(tasks)
    flat = [pltpu.VMEM((layers, *tasks[0].shape), BF16), *(task.matrix for _ in range(layers) for task in tasks[1:])]
    sems = [s for layer in range(layers) for task in (tasks[1:] if layer else tasks) for s in task.sems]
    own = [pltpu.VMEM((t, width), BF16), pltpu.VMEM((nh, HEAD + 8, t), BF16), pltpu.VMEM((nh, ROWS), F32), pltpu.VMEM((nh, HEAD + 8, ROWS), F32),
           pltpu.VMEM((t, width), BF16), pltpu.VMEM((t, d), BF16), pltpu.VMEM((ROWS, f), BF16), pltpu.VMEM((nh * ROWS // STRIP, ROWS, STRIP), F32),
           pltpu.VMEM((nh, ROWS), F32)]
    tab = table(t)

    def body(*refs):
        (x_ref, *rest) = refs
        (tab_ref,), shards, outs, scratch, moved = taken(rest, 1, 7, 4 + kinds, len(own), len(flat) + len(sems))
        qkv_ref, o_ref, lse_ref, h_ref, *wholes = outs
        k_s, vt_s, top_s, mix_s, o_s, h2_s, act_s, s_s, keep_s = scratch
        w_s = moved[0]
        matrices = [[w_s.at[layer], *m] for layer, m in enumerate(taken(moved[1:], *[kinds - 1] * layers))]
        flags = taken(moved[len(flat) :], *[6] * (layers * (kinds - 1) + 1))
        parts = [shards[:3], shards[3:4], shards[4:6], shards[6:]]
        step = pl.program_id(0)

        def go(layer, which, *stages):
            for stage in stages:
                for kind in which:
                    tasks[kind].run(stage, Place(side), layer, parts[kind], wholes[kind], matrices[layer][kind], flags[kind + (kinds - 1) * layer * (kind > 0)])

        def at(number):
            return pl.when(step == number)

        attention, ffn = (0,), (1, 2, 3)

        @at(0)
        def _():
            place = Place(side)
            peers = [*place.line(), place.partner]
            greet(peers)
            go(0, attention + ffn, 0)
            for m in range(nh):
                vt_s[m, HEAD:, :] = jnp.ones((8, t), BF16)
            pl.semaphore_wait(pltpu.get_barrier_semaphore(), len(peers))
            go(0, attention, 1)
            go(0, ffn, 1)
            go(0, attention, 2, 3, 5)
            go(0, ffn, 2)

        @at(n)
        def _():
            go(0, ffn, 4, 5)

        def matrix(layer, kind):
            return matrices[layer][kind]

        second = step >= 2 * n

        @pl.when((step < n) | second)
        def _():
            i = lax.rem(step, n)
            here = tile_at(i)
            layer = lax.div(step, 2 * n)

            h = jnp.where(second, h2_s[here, :], x_ref[...])

            @pl.when(~second)
            def _():
                h_ref[0] = x_ref[...]

            h = h.astype(F32)
            a = (h * scale_of(h)).astype(BF16)
            heads = [slice(m * HEAD, (m + 1) * HEAD) for m in range(nh)]
            raw = [[dot(a, w_s[layer, :, :, :, k * width + at.start : k * width + at.stop].reshape(d, HEAD)).astype(BF16) for k in range(3)] for at in heads]
            cos, sin = angles(tab_ref, i)
            pieces = [(m, slice(c, c + STRIP)) for m in range(nh) for c in range(0, ROWS, STRIP)]
            qs = []
            for m, at in enumerate(heads):
                q = rotated(raw[m][0].astype(F32), cos, sin).astype(BF16) * jnp.asarray(HEAD**-0.5, BF16)
                k = rotated(raw[m][1].astype(F32), cos, sin).astype(BF16)
                qkv_ref[0, :, at], qkv_ref[0, :, width + at.start : width + at.stop] = q, k
                qkv_ref[0, :, 2 * width + at.start : 2 * width + at.stop] = raw[m][2]
                vt_s[m, :HEAD, here] = raw[m][2].T
                k_s[here, at] = k
                qs.append(q)
                for p, (head, cols) in enumerate(pieces):
                    if head == m:
                        s = jnp.where(hidden(ROWS)[:, cols], -1e30, dot(k, q[cols, :], 1, 1))
                        s_s[p] = s
                        top_s[m : m + 1, cols] = s.max(0, keepdims=True)

            def scores(k, j):
                m, cols = pieces[k]
                return dot(k_s[tile_at(j), m * HEAD : (m + 1) * HEAD], qs[m][cols, :], 1, 1)

            def weights(k, top):
                return jnp.exp2((s_s[k] - top) * LOG2E).astype(BF16)

            def add(k, j, p, diagonal):
                m, cols = pieces[k]
                old = jnp.where(diagonal, 0.0, mix_s[m, :, cols] * keep_s[m : m + 1, cols])
                mix_s[m, :, cols] = old + dot(vt_s[m, :, tile_at(j)], p)

            def turn(j, _):
                before = jnp.where(j == 0, i, j - 1)
                late = None
                for k, (m, cols) in enumerate(pieces):
                    s = scores(k, j)
                    top = top_s[m : m + 1, cols]
                    p = weights(k, top)
                    s_s[k] = s
                    new = jnp.maximum(top, s.max(0, keepdims=True))
                    if late:
                        add(*late)
                        keep_s[pieces[k - 1][0] : pieces[k - 1][0] + 1, pieces[k - 1][1]] = keep
                    top_s[m : m + 1, cols] = new
                    keep = jnp.exp2((top - new) * LOG2E)
                    late = k, before, p, j == 0
                add(*late)
                keep_s[m : m + 1, cols] = keep

            lax.fori_loop(0, i, turn, None)
            end = jnp.where(i == 0, i, i - 1)

            def out(m):
                at = heads[m]
                total = mix_s[m, HEAD : HEAD + 1, :]
                o = (mix_s[m, :HEAD, :] * (1 / total)).T.astype(BF16)
                o_ref[0, :, at] = o
                o_s[here, at] = o
                lse_ref[0, m : m + 1, :] = top_s[m : m + 1, :] * LOG2E + jnp.log2(total)

            late = None
            for k, (m, cols) in enumerate(pieces):
                p = weights(k, top_s[m : m + 1, cols])
                if late:
                    add(*late)
                    if pieces[k - 1][0] != m:
                        out(m - 1)
                late = k, end, p, i == 0
            add(*late)
            out(nh - 1)

        @pl.when((step >= n) & ~second)
        def _():
            here = tile_at(step - n)
            wo, wgu, wd = (matrix(0, kind) for kind in ffn)
            h1 = x_ref[...] + dot(o_s[here, :], wo[...].reshape(width, d)).astype(BF16)
            wide = h1.astype(F32)
            b = (wide * scale_of(wide)).astype(BF16)
            cut = f // side
            for c in range(0, f, cut):
                gate = dot(b, wgu[:, :, :, c : c + cut].reshape(d, cut))
                up = dot(b, wgu[:, :, :, f + c : f + c + cut].reshape(d, cut))
                act_s[:, c : c + cut] = (gate * jax.nn.sigmoid(gate) * up).astype(BF16)
            h2 = h1 + dot(act_s[...], wd[...].reshape(f, d)).astype(BF16)
            h_ref[0] = h2
            h2_s[here, :] = h2

        plan = {0: [(0, attention, 6), (1, attention + ffn, 0)], n - 2: [(0, ffn, 3), (1, attention + ffn, 1)],
                n: [(1, attention + ffn, 2)], n + 2: [(1, attention, 3)], 2 * n - 1: [(1, attention, 5)], 2 * n: [(1, ffn, 3)],
                3 * n - 2: [(1, ffn, 4)], 3 * n - 1: [(1, ffn, 5), (0, ffn, 6), (1, attention + ffn, 6)]}
        for number, todo in plan.items():

            @at(number)
            def _():
                for what in todo:
                    go(*what)

    tile = lambda s: jnp.where(s < 2 * n, jnp.minimum(s, n - 1), s - 2 * n)
    by_layer = lambda w: pl.BlockSpec((1, ROWS, w), lambda s: (s // (2 * n), tile(s), 0))
    got = pl.pallas_call(
        body,
        grid=(3 * n,),
        in_specs=[pl.BlockSpec((ROWS, d), lambda s: (jnp.where(s < 2 * n, lax.rem(s, n), n - 1), 0)), whole(tab.shape), *[ANY] * 7],
        out_specs=[by_layer(3 * width), by_layer(width), pl.BlockSpec((1, nh, ROWS), lambda s: (s // (2 * n), 0, tile(s))),
                   pl.BlockSpec((1, ROWS, d), lambda s: (jnp.where(s < n, 0, 1), jnp.where(s < 2 * n, lax.rem(s, n), n - 1), 0)), *[ANY] * kinds],
        out_shape=[sds((layers, t, 3 * width), BF16), sds((layers, t, width), BF16), sds((layers, nh, t), F32), sds((layers, t, d), BF16),
                   *(sds((layers, *task.shape), BF16) for task in tasks)],
        scratch_shapes=[*own, *flat, *sems],
        compiler_params=pltpu.CompilerParams(dimension_semantics=("arbitrary",), vmem_limit_bytes=VMEM, has_side_effects=True, collective_id=cid),
        name="forward",
    )(x, tab, *weights)
    return [*got[:4], *(w.reshape(layers, -1, w.shape[-1]) for w in got[4:])]


def square(g):
    wide = g.astype(F32)
    return jnp.sum(jnp.sum(wide * wide, 0, keepdims=True), 1, keepdims=True)


def backward(cid, side, h, dy, qkv, o, lse, wqkv, wo, wgu, wd):
    layers, t, d = h.shape
    width = o.shape[2]
    f = wd.shape[1]
    n, nh, cut, group = t // ROWS, width // HEAD, f // side, side * side
    per = 3 * n + 2 * side + 1
    gu_shape, d_shape = (side, side, d // group, 2 * cut), (side, f // group, d)
    o_shape, q_shape = (side, side, width // group, d), (side, side, d // group, width)
    gu_task, d_task = Crossed(side, gu_shape[2], gu_shape[3]), Lined(side, d_shape[1], d)
    o_task, q_task = Crossed(side, o_shape[2], d), Crossed(side, q_shape[2], width)
    several = lambda task, n: [pltpu.VMEM((n, *s.shape), s.dtype) if s.memory_space == pltpu.VMEM else pltpu.SemaphoreType.DMA((n, *s.shape)) for s in task.scratch]
    moves = [*several(gu_task, SLOTS), *several(d_task, SLOTS), *o_task.scratch, *several(q_task, 3)]
    own = [pltpu.VMEM((t, d), BF16), pltpu.VMEM((d, t), BF16), pltpu.VMEM((t, d), BF16), pltpu.VMEM((d, t), BF16), pltpu.VMEM((t, d), F32),
           pltpu.VMEM((t, d), BF16), pltpu.VMEM((t, max(3 * cut, 3 * width)), BF16), pltpu.VMEM((2, *gu_shape), BF16),
           pltpu.VMEM((2, *d_shape), BF16), pltpu.VMEM((width, d), F32), pltpu.VMEM(o_shape, BF16), pltpu.VMEM((3, *q_shape), BF16),
           pltpu.VMEM((t, width), F32), pltpu.SemaphoreType.DMA((n + 7,)),
           pltpu.VMEM((group, 8, 128), F32), pltpu.VMEM((8, 128), F32), pltpu.SemaphoreType.DMA((1,)), pltpu.SemaphoreType.DMA((1,)),
           pltpu.VMEM((d, 3 * width), BF16), pltpu.VMEM((2 * (ROWS + n), HEAD // 2), F32), pltpu.VMEM((2, d, 2 * cut), BF16), pltpu.VMEM((2, cut, d), BF16)]
    tab = table(t)

    def body(*refs):
        ins, outs, scratch, moved = taken(refs, 10, 5, len(own), len(moves))
        h_ref, o_ref, lse_ref, wo_ref, wqkv_hbm, wgu_hbm, wd_hbm, dy_ref, qkv_ref, tab_hbm = ins
        gq_ref, go_ref, ggu_ref, gd_ref, total_ref = outs
        (b_s, bt_s, g_s, gt_s, by_s, h1_s, wide_s, gu_o, d_o, sum_s, wo_o, wqkv_o, dv_s, load, slots, part, send, recv, wqkv_s, tab_ref, wgu_s, wd_s) = scratch
        dgu_s, act_s, qkv_s = wide_s, wide_s, wide_s
        gu_m, d_m, o_m, q_m = taken(moved, *(len(task.scratch) for task in (gu_task, d_task, o_task, q_task)))
        step = pl.program_id(0)
        layer = layers - 1 - lax.div(step, per)
        phase = lax.rem(step, per)
        top = layer == layers - 1
        last = n + 2 * side
        load_dy = lambda number: pltpu.make_async_copy(dy_ref.at[tile_at(number)], g_s.at[tile_at(number)], load.at[1 + number])

        def load_late():
            return pltpu.make_async_copy(wqkv_hbm.at[layers - 1], wqkv_s, load.at[1 + n]), pltpu.make_async_copy(tab_hbm, tab_ref, load.at[2 + n])

        def load_chunk(layer, chunk, slot):
            for k in range(2):
                cols = pl.ds(pl.multiple_of(k * f + chunk * cut, cut), cut)
                yield pltpu.make_async_copy(wgu_hbm.at[layer, :, cols], wgu_s.at[slot, :, k * cut : (k + 1) * cut], load.at[3 + n + slot])
            yield pltpu.make_async_copy(wd_hbm.at[layer, pl.ds(pl.multiple_of(chunk * cut, cut), cut), :], wd_s.at[slot], load.at[5 + n + slot])

        load_qkv = lambda: pltpu.make_async_copy(qkv_ref.at[layer], qkv_s.at[:, : 3 * width], load.at[0])

        def at(number, more=True):
            return pl.when((phase == number) & more)

        @pl.when(step == 0)
        def _():
            for number in range(n):
                load_dy(number).start()
            for c in (*load_chunk(layer, 0, 0), *load_late()):
                c.start()
            greet(Place(side).others())

        @pl.when(step == n)
        def _():
            pl.semaphore_wait(pltpu.get_barrier_semaphore(), group - 1)

        at(last)(lambda: load_qkv().start())

        @pl.when(phase < n)
        def _():
            here = tile_at(phase)
            pl.when(top)(lambda: load_dy(phase).wait())
            h1 = h_ref[0] + dot(o_ref[0], wo_ref[layer]).astype(BF16)
            h1_s[here, :] = h1
            by_s[here, :] = jnp.zeros_like(h1, F32)
            wide = h1.astype(F32)
            b = (wide * scale_of(wide)).astype(BF16)
            b_s[here, :] = b
            bt_s[:, here] = b.T
            gt_s[:, here] = g_s[here, :].T

        chunk = lax.div(phase - n, 2)
        hidden_units = (phase >= n) & (phase < last)

        @pl.when(hidden_units & (lax.rem(phase - n, 2) == 0))
        def _():
            turn = lax.rem(chunk, 2)
            arrive(wgu_s.at[turn], load.at[3 + n + turn])
            arrive(wd_s.at[turn], load.at[5 + n + turn])

            @pl.when((chunk < side - 1) | (layer > 0))
            def _():
                end = chunk == side - 1
                for c in load_chunk(jnp.where(end, layer - 1, layer), jnp.where(end, 0, chunk + 1), 1 - turn):
                    c.start()

            wg, wu, wd = wgu_s.at[turn, :, :cut], wgu_s.at[turn, :, cut:], wd_s.at[turn]

            def tile(number, _):
                here = tile_at(number)
                b, g = b_s[here, :], g_s[here, :]
                sub = HEAD
                for c in range(0, cut, sub):
                    cols = slice(c, c + sub)
                    gate, up = dot(b, wg[:, cols]), dot(b, wu[:, cols])
                    dact = dot(g, wd[cols, :], 1, 1)
                    sig = jax.nn.sigmoid(gate)
                    silu = gate * sig
                    act_s[here, 2 * cut + c : 2 * cut + c + sub] = (silu * up).astype(BF16)
                    dgu_s[here, cols] = (dact * up * (sig + silu * (1 - sig))).astype(BF16)
                    dgu_s[here, cut + c : cut + c + sub] = (dact * silu).astype(BF16)
                by_s[here, :] += dot(dgu_s[here, :cut], wg[...], 1, 1) + dot(dgu_s[here, cut : 2 * cut], wu[...], 1, 1)

            lax.fori_loop(0, n, tile, None, unroll=2)

        @pl.when(hidden_units & (lax.rem(phase - n, 2) == 1))
        def _():
            slot = lax.rem(chunk, 2)
            for c in range(0, 2 * cut, cut):
                gu_o[slot, :, :, :, c : c + cut] = dot(bt_s[...], dgu_s[:, c : c + cut]).astype(BF16).reshape(*gu_shape[:3], cut)
            d_o[slot] = dot(gt_s[...], act_s[:, 2 * cut : 3 * cut]).T.astype(BF16).reshape(d_shape)

        do_s, kt_s, yt_s, dk_s, dq_s = h1_s, bt_s, gt_s, by_s, sum_s

        @pl.when((phase >= last) & (phase < last + n))
        def _():
            number = phase - last
            here = tile_at(number)
            h1 = h1_s[here, :].astype(F32)
            r = scale_of(h1)
            dh1 = (g_s[here, :].astype(F32) + normed_bwd(h1 * r, r, by_s[here, :])).astype(BF16)
            g_s[here, :] = dh1
            dk_s[here, :] = jnp.zeros((ROWS, width), F32)
            dv_s[here, :] = jnp.zeros((ROWS, width), F32)
            do_s[here, :] = dot(dh1, wo_ref[layer], 1, 1).astype(BF16)
            by_wo = dot(o_ref[0].T, dh1)

            @pl.when(number == 0)
            def _():
                sum_s[...] = by_wo

            @pl.when(number > 0)
            def _():
                sum_s[...] += by_wo

            @pl.when(number == n - 1)
            def _():
                wo_o[...] = sum_s[...].astype(BF16).reshape(o_shape)

        heads = [slice(m * HEAD, (m + 1) * HEAD) for m in range(nh)]

        @at(last + n)
        def _():
            load_qkv().wait()

            @pl.when(top)
            def _():
                for c in load_late():
                    c.wait()

            for j in range(0, t, ROWS):
                for h in heads:
                    kt_s[h, j : j + ROWS] = qkv_s[j : j + ROWS, width + h.start : width + h.stop].T

        @pl.when((phase >= last + n) & (phase < per - 1))
        def _():
            i = per - 2 - phase
            here = tile_at(i)
            qs = [qkv_s[here, h] for h in heads]
            dos = [do_s[here, h] for h in heads]
            deltas = []
            for m, h in enumerate(heads):
                delta = (dos[m].astype(F32) * o_ref[0, :, h].astype(F32)).sum(-1, keepdims=True)
                deltas.append(jnp.broadcast_to(delta, (ROWS, 128)).T[:1, :])
            lses = [lse_ref[layer, m : m + 1, here] for m in range(nh)]

            def block(keys, start, hide, first):
                span = slice(start, ROWS)
                scores = [dot(qkv_s[keys, width + h.start : width + h.stop], q[span, :], 1, 1) for h, q in zip(heads, qs)]
                dps = [dot(qkv_s[keys, 2 * width + h.start : 2 * width + h.stop], g[span, :], 1, 1) for h, g in zip(heads, dos)]
                for m, h in enumerate(heads):
                    p = jnp.exp2(scores[m] * LOG2E - lses[m][:, span])
                    if hide is not None:
                        p = jnp.where(hide, 0.0, p)
                    ds = (p * (dps[m] - deltas[m][:, span])).astype(BF16)
                    dv_s[keys, h] += dot(p.astype(BF16), dos[m][span, :])
                    dk_s[keys, h] += dot(ds, qs[m][span, :])
                    dq = dot(kt_s[h, keys], ds)
                    dq_s[h, span] = dq if first else dq_s[h, span] + dq

            wide = h_ref[0].astype(F32)
            yt_s[:, here] = (wide * scale_of(wide)).astype(BF16).T
            half = ROWS // 2
            hide = hidden(ROWS)
            block(pl.ds(pl.multiple_of(i * ROWS, ROWS), half), 0, hide[:half, :], True)
            block(pl.ds(pl.multiple_of(i * ROWS + half, half), half), half, hide[:half, :half], False)
            lax.fori_loop(0, i, lambda j, _: block(tile_at(j), 0, None, False), None)
            cos, sin = angles(tab_ref, i)
            for h in heads:
                qkv_s[here, h] = rotated((dq_s[h, :] * HEAD**-0.5).T, cos, -sin).astype(BF16)
                qkv_s[here, width + h.start : width + h.stop] = rotated(dk_s[here, h], cos, -sin).astype(BF16)
                qkv_s[here, 2 * width + h.start : 2 * width + h.stop] = dv_s[here, h].astype(BF16)

            @pl.when(top)
            def _():
                by = dot(qkv_s[here, : 3 * width], wqkv_s[...], 1, 1)
                wide = h_ref[0].astype(F32)
                r = scale_of(wide)
                y = wide * r
                g_s[here, :] = (g_s[here, :].astype(F32) + normed_bwd(y, r, by)).astype(BF16)

        def qkvs(stage, of, which=(0, 1, 2)):
            for k in which:
                q_task.run(stage, Place(side), wqkv_o.at[k], gq_ref.at[of, :, k * width : (k + 1) * width], [r.at[k] for r in q_m])

        @at(per - 1)
        def _():
            for k in range(3):
                wqkv_o[k] = dot(yt_s[...], qkv_s[:, k * width : (k + 1) * width]).astype(BF16).reshape(q_shape)
                qkvs(0, layer, (k,))


        def both(chunk, stage):
            slot, source = lax.rem(chunk, SLOTS), lax.rem(chunk, 2)
            d_task.run(stage, Place(side), chunk, d_o.at[source], gd_ref.at[layer], [r.at[slot] for r in d_m])
            gu_task.run(stage, Place(side), gu_o.at[source], ggu_ref.at[layer, chunk], [r.at[slot] for r in gu_m])

        def out(stage):
            o_task.run(stage, Place(side), wo_o, go_ref.at[layer], o_m)

        when = [[n + 2 * c + later for c in range(side)] for later in (1, 2, 4, 6)]
        when[1][-1] = last + n
        when[2][-2:] = last + 2, last + n + 1
        when[3][-3:] = last + 2, last + n, per - 1

        for stage in (2, 3, 1, 0):

            @pl.when(functools.reduce(jnp.logical_or, [phase == p for p in when[stage]]))
            def _():
                both(sum(jnp.where(phase == p, c, 0) for c, p in enumerate(when[stage])), stage)

            at(per - 1 if stage == 3 else last + n - 1 + stage)(lambda: out(stage))

        for stage, number in ((1, n), (2, n + 2), (3, n + 4)):
            at(number, ~top)(lambda: qkvs(stage, layer + 1))

        @pl.when(step == layers * per - 1)
        def _():
            place = Place(side)
            mine = sum(square(gq_ref[k]) for k in range(1, layers))
            for k in range(layers):
                mine += square(go_ref[k]) + square(gd_ref[k])
                for c in range(side):
                    mine += square(ggu_ref[k, c])
            qkvs(1, 0)
            qkvs(2, 0)
            qkvs(3, 0)
            mine = jnp.broadcast_to(mine + square(gq_ref[0]), part.shape)
            part[...] = mine
            slots[place.me] = mine
            for device in place.others():
                remote(part, slots.at[place.me], send.at[0], recv.at[0], device).start()
            arrived(slots.at[: group - 1], send.at[0], recv.at[0], place.others()[0])
            total_ref[...] = slots[...].sum(0)

    layer_of = lambda s: layers - 1 - s // per

    def tile(s, phases):
        p = lax.rem(s, per)
        back = jnp.maximum(per - 2 - p, 0)
        late = jnp.where(p < n + 2 * side + n, n - 1, back)
        at_epilogue = jnp.clip(p - n - 2 * side, 0, n - 1)
        early = jnp.where(p < n, p, n - 1)
        if phases == "ends":
            return jnp.where(p < n, p, late)
        if phases == "all":
            return jnp.where(p < n, p, jnp.where(p < n + 2 * side + n, at_epilogue, back))
        return late

    outs = [sds((layers, q_shape[2], 3 * width), BF16), sds((layers, o_shape[2], d), BF16), sds((layers, side, *gu_shape[2:]), BF16),
            sds((layers, *d_shape[1:]), BF16), sds((8, 128), F32)]
    return pl.pallas_call(
        body,
        grid=(layers * per,),
        in_specs=[pl.BlockSpec((1, ROWS, d), lambda s: (layer_of(s), tile(s, "ends"), 0)),
                  pl.BlockSpec((1, ROWS, width), lambda s: (layer_of(s), tile(s, "all"), 0)),
                  whole(lse.shape), whole(wo.shape), ANY, ANY, ANY, ANY, ANY, ANY],
        out_specs=[whole(a.shape) for a in outs],
        out_shape=outs,
        scratch_shapes=[*own, *moves],
        compiler_params=pltpu.CompilerParams(dimension_semantics=("arbitrary",), vmem_limit_bytes=VMEM, has_side_effects=True, collective_id=cid),
        name="backward",
    )(h, o, lse, wo, wqkv, wgu, wd, dy, qkv, tab)


def adamw(total, count, weights, m, v, gq, go, ggu, gd):
    layers, side = ggu.shape[:2]

    def body(total_ref, gq_ref, go_ref, ggu_ref, gd_ref, *refs):
        w_refs, m_refs, v_refs, wn_refs, mn_refs, vn_refs = taken(refs, *[7] * 6)
        factor = jnp.minimum(1.0, 0.5 * lax.rsqrt(total_ref[0:1, 0:1] / count + 1e-30))

        def update(i, columns, g):
            g = g.astype(F32) * factor
            at = (0, slice(None), columns)
            mn = 0.9 * m_refs[i][at] + 0.1 * g
            vn = 0.95 * v_refs[i][at] + 0.05 * g * g
            mn_refs[i][at], vn_refs[i][at] = mn, vn
            w = w_refs[i][at].astype(F32)
            wn_refs[i][at] = (w - 0.02 * (mn * lax.rsqrt(vn + 1e-8) + 0.1 * w)).astype(BF16)

        every = slice(None)
        wide = gq_ref.shape[2] // 3
        for i in range(3):
            update(i, every, gq_ref[0, :, i * wide : (i + 1) * wide])
        update(3, every, go_ref[0])
        cut = ggu_ref.shape[3] // 2
        for c in range(side):
            for i in range(2):
                update(4 + i, slice(c * cut, (c + 1) * cut), ggu_ref[0, c, :, i * cut : (i + 1) * cut])
        update(6, every, gd_ref[0])

    one = lambda a: pl.BlockSpec((1, *a.shape[1:]), lambda l: (l,) + (0,) * (a.ndim - 1))
    own = [one(a) for a in weights]
    return pl.pallas_call(
        body,
        grid=(layers,),
        in_specs=[whole(total.shape), *(one(a) for a in (gq, go, ggu, gd)), *own * 3],
        out_specs=own * 3,
        out_shape=[*(sds(a.shape, BF16) for a in weights), *(sds(a.shape, F32) for a in (*m, *v))],
        compiler_params=pltpu.CompilerParams(dimension_semantics=("arbitrary",), vmem_limit_bytes=VMEM),
        name="adamw",
    )(total, gq, go, ggu, gd, *weights, *m, *v)


def solution(mesh):
    group = mesh.shape["dp"]
    side = side_of(group)

    def step(x, dy, *arrays):
        weights, m, v = (arrays[i : i + 7] for i in (0, 7, 14))
        x, dy = x[0], dy[0]
        qkv, o, lse, h, wqkv, wo, wgu, wd = forward(0, side, x, weights)
        *grads, total = backward(1, side, h, dy, qkv, o, lse, wqkv, wo, wgu, wd)
        return tuple(adamw(total, group * sum(w.size for w in weights), weights, m, v, *grads))

    states, cut = P(("rep", "dp"), None, None), P(None, "dp", None)
    return jax.shard_map(
        step,
        mesh=mesh,
        in_specs=(states, states) + (cut,) * 21,
        out_specs=(P("rep", "dp", None),) * 21,
        check_vma=False,
    )
```

```python
import functools

import jax
import jax.numpy as jnp
import numpy as np
from jax import lax
from jax.experimental import pallas as pl
from jax.experimental.pallas import tpu as pltpu
from jax.sharding import PartitionSpec as P

HEAD = 256
THETA = 10000
LOG2E = 1.4426950408889634
VMEM = 67_000_000
EPS = 1e-6
F32, BF16 = jnp.float32, jnp.bfloat16
MESH = pl.DeviceIdType.MESH
ANY = pl.BlockSpec(memory_space=pl.ANY)
ROWS = 512
STRIP = 256
SLOTS = 3
sds = jax.ShapeDtypeStruct


def dot(a, b, ca=1, cb=0):
    return lax.dot_general(a, b, (((ca,), (cb,)), ((), ())), preferred_element_type=F32)


def scale_of(h):
    return lax.rsqrt(jnp.mean(h * h, -1, keepdims=True) + EPS)


def normed_bwd(y, r, by):
    return r * (by - y * jnp.mean(by * y, -1, keepdims=True))


def table(tokens):
    half = HEAD // 2
    rate = np.float32(THETA) ** (-np.arange(half, dtype=np.float32) / np.float32(half))
    places = [np.arange(0, ROWS), np.arange(0, tokens, ROWS)]
    return jnp.asarray(np.concatenate([f(p[:, None] * rate.astype(np.float64)) for p in places for f in (np.cos, np.sin)]), F32)


def angles(ref, tile):
    n = ref.shape[0] // 2 - ROWS
    near_c, near_s = ref[:ROWS, :], ref[ROWS : 2 * ROWS, :]
    c, s = ref[pl.ds(2 * ROWS + tile, 1), :], ref[pl.ds(2 * ROWS + n + tile, 1), :]
    return c * near_c - s * near_s, s * near_c + c * near_s


def rotated(t, cos, sin):
    half = t.shape[-1] // 2
    a, b = t[:, :half], t[:, half:]
    return jnp.concatenate([a * cos - b * sin, b * cos + a * sin], -1)


def hidden(size):
    return lax.broadcasted_iota(jnp.int32, (size, size), 0) > lax.broadcasted_iota(jnp.int32, (size, size), 1)


def tile_at(n, size=ROWS):
    return pl.ds(pl.multiple_of(n * size, size), size)


def whole(shape):
    return pl.BlockSpec(shape, lambda *_: (0,) * len(shape), pipeline_mode=pl.Buffered(1))


def side_of(group):
    return int(round(group**0.5))


class Place:
    def __init__(self, side):
        rep, me = lax.axis_index("rep"), lax.axis_index("dp")
        self.side, self.me, self.x, self.y, self.core = side, me, lax.div(me, side), lax.rem(me, side), lax.rem(rep, 2)
        self.partner = {"rep": rep + 1 - 2 * self.core}

    def on(self, axis, k):
        at = lax.rem((self.x, self.y)[axis] + k, self.side)
        return at, {"dp": at * self.side + self.y if axis == 0 else self.x * self.side + at}

    def line(self):
        return [self.on(axis, k)[1] for axis in (0, 1) for k in range(1, self.side)]

    def others(self):
        n = self.side**2
        return [{"dp": lax.rem(self.me + k, n)} for k in range(1, n)]


def greet(devices):
    for device in devices:
        pl.semaphore_signal(pltpu.get_barrier_semaphore(), inc=1, device_id=device, device_id_type=MESH)


def remote(src, dst, send, recv, device):
    return pltpu.make_async_remote_copy(src_ref=src, dst_ref=dst, send_sem=send, recv_sem=recv, device_id=device, device_id_type=MESH)


def arrive(ref, sem):
    pltpu.make_async_copy(ref, ref, sem).wait()


def arrived(ref, send, recv, device):
    c = remote(ref, ref, recv if send is None else send, send if recv is None else recv, device)
    if recv is not None:
        c.wait_recv()
    if send is not None:
        c.wait_send()


class Gather:
    def __init__(self, side, rows, widths, by_rows, relayed):
        self.side, self.widths, self.by_rows, self.relayed = side, widths, by_rows, relayed
        n = side - 1
        self.shape = (side, side, rows, sum(widths))
        self.matrix = pltpu.VMEM(self.shape, BF16)
        self.sems = [pltpu.SemaphoreType.DMA((k,)) for k in (len(widths) + 2, 2, 2, 2 * n, 2, 2)]

    def run(self, stage, place, layer, shards, result, out, sems):
        local, send, come, across, near, far = sems
        n = self.side - 1
        copies, column = [], 0
        for k, (shard, width) in enumerate(zip(shards, self.widths, strict=True)):
            copies.append((shard.at[layer], out.at[place.x, place.y, :, column : column + width], local.at[k]))
            column += width
        size = out.shape[2] if self.by_rows else out.shape[3]
        every = slice(None)

        def copied(own):
            core = place.core if own else 1 - place.core
            piece = pl.ds(pl.multiple_of(core * (size // 2), size // 2), size // 2)
            at = (every, every, piece, every) if self.by_rows else (every, every, every, piece)
            return pltpu.make_async_copy(out.at[at], result.at[(layer, *at)], local.at[len(shards) + own])

        if stage == 0:
            for c in copies:
                pltpu.make_async_copy(*c).start()
        elif stage == 1:
            for c in copies:
                pltpu.make_async_copy(*c).wait()
        elif stage == 6:
            copied(0).wait()
            copied(1).wait()
            arrived(out.at[0, :n], send.at[0], None, place.partner)
            arrived(out.at[:n], send.at[1], None, place.partner)
        for q, waits in [(0, True), (1, True)] * (stage == 2) + [(0, False), (1, False)]:

            def view(at, core=place.core):
                piece = pl.ds(pl.multiple_of(core * (size // 2) + q * (size // 4), size // 4), size // 4)
                return out.at[at[0], at[1], piece, :] if self.by_rows else out.at[at[0], at[1], :, piece]

            along = lambda at: (at, place.y) if q == 0 else (place.x, at)
            over = lambda at: (every, at) if q == 0 else (at, every)
            here, line = view((place.x, place.y)), view(over(place.y if q == 0 else place.x))
            if stage == 1:
                for k in range(1, n + 1):
                    remote(here, here, send.at[0], come.at[q], place.on(q, k)[1]).start()
            elif waits:
                arrived(view((0, slice(0, n))), None, come.at[q], place.partner)
            elif stage == 2:
                for k in (1, n) if self.relayed else range(1, n + 1):
                    remote(line, line, send.at[1], across.at[q * n + k - 1], place.on(1 - q, k)[1]).start()
                for k in range(1, n + 1):
                    got = view(along(place.on(q, k)[0]))
                    remote(got, got, send.at[0], near.at[q], place.partner).start()
            elif stage in (3, 4):
                for k in ((1, n) if stage == 3 else (2,)) if self.relayed else range(1, n + 1) if stage == 3 else ():
                    at = place.on(1 - q, self.side - k)[0]
                    got = view(over(at))
                    arrived(got, None, across.at[q * n + k - 1], place.partner)
                    if self.relayed and stage == 3:
                        half = slice(0, self.side // 2) if k == 1 else slice(self.side // 2, self.side)
                        part = view((half, at) if q == 0 else (at, half))
                        remote(part, part, send.at[1], across.at[q * n + 1], place.on(1 - q, k)[1]).start()
                    remote(got, got, send.at[1], far.at[q], place.partner).start()
            elif stage == 5:
                arrived(view((0, slice(0, n))), None, near.at[q], place.partner)
                arrived(view((slice(0, n), every)), None, far.at[q], place.partner)
        if stage == (4 if self.relayed else 5):
            copied(1).start()
        if stage == 5:
            copied(0).start()


class Ring:
    def __init__(self, half):
        self.scratch = [pltpu.VMEM((2, *half), BF16), pltpu.VMEM((2, *half), BF16), pltpu.VMEM((2, 2, *half), BF16), pltpu.SemaphoreType.DMA((2,)),
                        pltpu.SemaphoreType.DMA((2,))]

    def start(self, place, axis, blocks, scratch, last=False):
        far, mid, near, send, recv = scratch
        opposite, _ = place.on(axis, 2)
        for relayed in (True, False):
            for d, k in enumerate((1, place.side - 1)):
                there, to = place.on(axis, k)
                if last:
                    if relayed:
                        remote(mid.at[d], near.at[d, d], send.at[1], recv.at[1], to).start()
                elif relayed:
                    remote(blocks(opposite, d), far.at[d], send.at[0], recv.at[0], to).start()
                else:
                    remote(blocks(there, 1 - d), near.at[d, 1 - d], send.at[1], recv.at[1], to).start()

    def middle(self, place, axis, blocks, scratch):
        far, mid, near, send, recv = scratch
        arrived(far, send.at[0], recv.at[0], place.on(axis, 1)[1])
        for d, k in enumerate((1, place.side - 1)):
            there, _ = place.on(axis, k)
            mid[d] = (blocks(there, d)[...].astype(F32) + far[d].astype(F32)).astype(BF16)
        self.start(place, axis, blocks, scratch, True)

    def end(self, place, axis, blocks, scratch):
        far, mid, near, send, recv = scratch
        arrived(near, send.at[1], recv.at[1], place.on(axis, 1)[1])

    def total(self, blocks, scratch, at, cut):
        near = scratch[2]
        return blocks(at, cut)[...].astype(F32) + near[0, cut].astype(F32) + near[1, cut].astype(F32)


class Crossed:
    def __init__(self, side, rows, width):
        self.side, self.width = side, width
        n, half = side - 1, width // 2
        self.ring = Ring((side // 2, rows, half))
        self.scratch = [*self.ring.scratch * 2, pltpu.VMEM((2, side, rows, half), BF16), pltpu.VMEM((2, n, rows, half), BF16),
                        pltpu.VMEM((2, rows, half), F32), pltpu.SemaphoreType.DMA((1,)), pltpu.SemaphoreType.DMA((1,))]

    def run(self, stage, place, src, out, scratch):
        *rings, (mid, two, own, send, recv) = taken(scratch, 5, 5, 5)
        n, half, cut = self.side - 1, self.width // 2, self.side // 2
        along = (lambda j, h: src.at[j, h * cut : (h + 1) * cut, :, :half]), (lambda j, h: src.at[h * cut : (h + 1) * cut, j, :, half:])
        for q in range(2):
            at = (place, q, along[q], rings[q])
            if stage == 0:
                self.ring.start(*at)
            elif stage == 1:
                self.ring.middle(*at)
            elif stage == 2:
                self.ring.end(*at)
                for h in range(2):
                    mid[q, h * cut : (h + 1) * cut] = self.ring.total(along[q], rings[q], (place.x, place.y)[q], h).astype(BF16)
                j = (place.y, place.x)[q]
                mine = (src[place.x, place.y, :, :half] if q == 0 else src[place.x, place.y, :, half:]).astype(F32)
                own[q] = mine + sum(rings[q][2][d, lax.div(j, cut), lax.rem(j, cut)].astype(F32) for d in range(2))
        if stage == 2:
            for q in range(2):
                for k in range(n):
                    there, to = place.on(1 - q, k + 1)
                    remote(mid.at[q, there], two.at[q, k], send.at[0], recv.at[0], to).start()
        elif stage == 3:
            arrived(two, send.at[0], recv.at[0], place.on(0, 1)[1])
            for q in range(2):
                t = own[q]
                for k in range(n):
                    t += two[q, k].astype(F32)
                out[:, q * half : (q + 1) * half] = t.astype(BF16)


class Lined:
    def __init__(self, side, rows, width):
        self.side, self.rows = side, rows
        n = side - 1
        self.ring = Ring((rows // 2, width))
        self.scratch = [*self.ring.scratch, pltpu.VMEM((rows, width), BF16), pltpu.VMEM((n, rows, width), BF16),
                        pltpu.VMEM((rows, width), F32), pltpu.SemaphoreType.DMA((1,)), pltpu.SemaphoreType.DMA((1,))]

    def run(self, stage, place, line, src, out, scratch):
        ring, (mid, two, own, send, recv) = taken(scratch, 5, 5)
        n, cut = self.side - 1, self.rows // 2
        ahead = lax.rem(line - place.x + self.side, self.side)
        at = (place, 1, lambda j, h: src.at[j, h * cut : (h + 1) * cut, :], ring)

        def second():
            return remote(mid, two.at[ahead - 1], send.at[0], recv.at[0], place.on(0, ahead)[1])

        if stage == 0:
            self.ring.start(*at)
        elif stage == 1:
            self.ring.middle(*at)
        elif stage == 2:
            self.ring.end(*at)
            for h in range(2):
                t = self.ring.total(at[2], ring, place.y, h)
                own[h * cut : (h + 1) * cut, :] = t
                mid[h * cut : (h + 1) * cut, :] = t.astype(BF16)
            pl.when(ahead != 0)(lambda: second().start())
        else:
            pl.when(ahead != 0)(lambda: second().wait_send())

            @pl.when(ahead == 0)
            def _():
                arrived(two, None, recv.at[0], place.on(0, 1)[1])
                t = own[...]
                for k in range(n):
                    t += two[k].astype(F32)
                out[...] = t.astype(BF16)


def taken(refs, *counts):
    out, at = [], 0
    for n in counts:
        out.append(refs[at : at + n])
        at += n
    return out


def forward(cid, side, x, weights):
    t, d = x.shape
    layers, width = weights[0].shape[0], weights[0].shape[2]
    f = weights[4].shape[2]
    nh, n = width // HEAD, t // ROWS
    shard = d // side**2
    tasks = [Gather(side, shard, [width] * 3, False, False), Gather(side, shard, [width], False, True), Gather(side, shard, [f, f], False, True),
             Gather(side, f // side**2, [d], True, True)]
    kinds = len(tasks)
    flat = [pltpu.VMEM((layers, *tasks[0].shape), BF16), *(task.matrix for _ in range(layers) for task in tasks[1:])]
    sems = [s for layer in range(layers) for task in (tasks[1:] if layer else tasks) for s in task.sems]
    own = [pltpu.VMEM((t, width), BF16), pltpu.VMEM((nh, HEAD + 8, t), BF16), pltpu.VMEM((nh, ROWS), F32), pltpu.VMEM((nh, HEAD + 8, ROWS), F32),
           pltpu.VMEM((t, width), BF16), pltpu.VMEM((t, d), BF16), pltpu.VMEM((ROWS, f), BF16), pltpu.VMEM((nh * ROWS // STRIP, ROWS, STRIP), F32),
           pltpu.VMEM((nh, ROWS), F32)]
    tab = table(t)

    def body(*refs):
        (x_ref, *rest) = refs
        (tab_ref,), shards, outs, scratch, moved = taken(rest, 1, 7, 4 + kinds, len(own), len(flat) + len(sems))
        qkv_ref, o_ref, lse_ref, h_ref, *wholes = outs
        k_s, vt_s, top_s, mix_s, o_s, h2_s, act_s, s_s, keep_s = scratch
        w_s = moved[0]
        matrices = [[w_s.at[layer], *m] for layer, m in enumerate(taken(moved[1:], *[kinds - 1] * layers))]
        flags = taken(moved[len(flat) :], *[6] * (layers * (kinds - 1) + 1))
        parts = [shards[:3], shards[3:4], shards[4:6], shards[6:]]
        step = pl.program_id(0)

        def go(layer, which, *stages):
            for stage in stages:
                for kind in which:
                    tasks[kind].run(stage, Place(side), layer, parts[kind], wholes[kind], matrices[layer][kind], flags[kind + (kinds - 1) * layer * (kind > 0)])

        def at(number):
            return pl.when(step == number)

        attention, ffn = (0,), (1, 2, 3)

        @at(0)
        def _():
            place = Place(side)
            peers = [*place.line(), place.partner]
            greet(peers)
            go(0, attention + ffn, 0)
            for m in range(nh):
                vt_s[m, HEAD:, :] = jnp.ones((8, t), BF16)
            pl.semaphore_wait(pltpu.get_barrier_semaphore(), len(peers))
            go(0, attention, 1)
            go(0, ffn, 1)
            go(0, attention, 2, 3, 5)
            go(0, ffn, 2)

        @at(n)
        def _():
            go(0, ffn, 4, 5)

        def matrix(layer, kind):
            return matrices[layer][kind]

        second = step >= 2 * n

        @pl.when((step < n) | second)
        def _():
            i = lax.rem(step, n)
            here = tile_at(i)
            layer = lax.div(step, 2 * n)

            h = jnp.where(second, h2_s[here, :], x_ref[...])

            @pl.when(~second)
            def _():
                h_ref[0] = x_ref[...]

            h = h.astype(F32)
            a = (h * scale_of(h)).astype(BF16)
            heads = [slice(m * HEAD, (m + 1) * HEAD) for m in range(nh)]
            raw = [[dot(a, w_s[layer, :, :, :, k * width + at.start : k * width + at.stop].reshape(d, HEAD)).astype(BF16) for k in range(3)] for at in heads]
            cos, sin = angles(tab_ref, i)
            pieces = [(m, slice(c, c + STRIP)) for m in range(nh) for c in range(0, ROWS, STRIP)]
            qs = []
            for m, at in enumerate(heads):
                q = rotated(raw[m][0].astype(F32), cos, sin).astype(BF16) * jnp.asarray(HEAD**-0.5, BF16)
                k = rotated(raw[m][1].astype(F32), cos, sin).astype(BF16)
                qkv_ref[0, :, at], qkv_ref[0, :, width + at.start : width + at.stop] = q, k
                qkv_ref[0, :, 2 * width + at.start : 2 * width + at.stop] = raw[m][2]
                vt_s[m, :HEAD, here] = raw[m][2].T
                k_s[here, at] = k
                qs.append(q)
                for p, (head, cols) in enumerate(pieces):
                    if head == m:
                        s = jnp.where(hidden(ROWS)[:, cols], -1e30, dot(k, q[cols, :], 1, 1))
                        s_s[p] = s
                        top_s[m : m + 1, cols] = s.max(0, keepdims=True)

            def scores(k, j):
                m, cols = pieces[k]
                return dot(k_s[tile_at(j), m * HEAD : (m + 1) * HEAD], qs[m][cols, :], 1, 1)

            def weights(k, top):
                return jnp.exp2((s_s[k] - top) * LOG2E).astype(BF16)

            def add(k, j, p, diagonal):
                m, cols = pieces[k]
                old = jnp.where(diagonal, 0.0, mix_s[m, :, cols] * keep_s[m : m + 1, cols])
                mix_s[m, :, cols] = old + dot(vt_s[m, :, tile_at(j)], p)

            def turn(j, _):
                before = jnp.where(j == 0, i, j - 1)
                late = None
                for k, (m, cols) in enumerate(pieces):
                    s = scores(k, j)
                    top = top_s[m : m + 1, cols]
                    p = weights(k, top)
                    s_s[k] = s
                    new = jnp.maximum(top, s.max(0, keepdims=True))
                    if late:
                        add(*late)
                        keep_s[pieces[k - 1][0] : pieces[k - 1][0] + 1, pieces[k - 1][1]] = keep
                    top_s[m : m + 1, cols] = new
                    keep = jnp.exp2((top - new) * LOG2E)
                    late = k, before, p, j == 0
                add(*late)
                keep_s[m : m + 1, cols] = keep

            lax.fori_loop(0, i, turn, None)
            end = jnp.where(i == 0, i, i - 1)

            def out(m):
                at = heads[m]
                total = mix_s[m, HEAD : HEAD + 1, :]
                o = (mix_s[m, :HEAD, :] * (1 / total)).astype(BF16).T
                o_ref[0, :, at] = o
                o_s[here, at] = o
                lse_ref[0, m : m + 1, :] = top_s[m : m + 1, :] * LOG2E + jnp.log2(total)

            late = None
            for k, (m, cols) in enumerate(pieces):
                p = weights(k, top_s[m : m + 1, cols])
                if late:
                    add(*late)
                    if pieces[k - 1][0] != m:
                        out(m - 1)
                late = k, end, p, i == 0
            add(*late)
            out(nh - 1)

        @pl.when((step >= n) & ~second)
        def _():
            here = tile_at(step - n)
            wo, wgu, wd = (matrix(0, kind) for kind in ffn)
            h1 = x_ref[...] + dot(o_s[here, :], wo[...].reshape(width, d)).astype(BF16)
            wide = h1.astype(F32)
            b = (wide * scale_of(wide)).astype(BF16)
            cut = f // side
            for c in range(0, f, cut):
                gate = dot(b, wgu[:, :, :, c : c + cut].reshape(d, cut))
                up = dot(b, wgu[:, :, :, f + c : f + c + cut].reshape(d, cut))
                act_s[:, c : c + cut] = (gate * jax.nn.sigmoid(gate) * up).astype(BF16)
            h2 = h1 + dot(act_s[...], wd[...].reshape(f, d)).astype(BF16)
            h_ref[0] = h2
            h2_s[here, :] = h2

        plan = {0: [(0, attention, 6), (1, attention + ffn, 0)], n - 2: [(0, ffn, 3), (1, attention + ffn, 1)],
                n: [(1, attention + ffn, 2)], n + 2: [(1, attention, 3)], 2 * n - 1: [(1, attention, 5)], 2 * n: [(1, ffn, 3)],
                3 * n - 2: [(1, ffn, 4)], 3 * n - 1: [(1, ffn, 5), (0, ffn, 6), (1, attention + ffn, 6)]}
        for number, todo in plan.items():

            @at(number)
            def _():
                for what in todo:
                    go(*what)

    tile = lambda s: jnp.where(s < 2 * n, jnp.minimum(s, n - 1), s - 2 * n)
    by_layer = lambda w: pl.BlockSpec((1, ROWS, w), lambda s: (s // (2 * n), tile(s), 0))
    got = pl.pallas_call(
        body,
        grid=(3 * n,),
        in_specs=[pl.BlockSpec((ROWS, d), lambda s: (jnp.where(s < 2 * n, lax.rem(s, n), n - 1), 0)), whole(tab.shape), *[ANY] * 7],
        out_specs=[by_layer(3 * width), by_layer(width), pl.BlockSpec((1, nh, ROWS), lambda s: (s // (2 * n), 0, tile(s))),
                   pl.BlockSpec((1, ROWS, d), lambda s: (jnp.where(s < n, 0, 1), jnp.where(s < 2 * n, lax.rem(s, n), n - 1), 0)), *[ANY] * kinds],
        out_shape=[sds((layers, t, 3 * width), BF16), sds((layers, t, width), BF16), sds((layers, nh, t), F32), sds((layers, t, d), BF16),
                   *(sds((layers, *task.shape), BF16) for task in tasks)],
        scratch_shapes=[*own, *flat, *sems],
        compiler_params=pltpu.CompilerParams(dimension_semantics=("arbitrary",), vmem_limit_bytes=VMEM, has_side_effects=True, collective_id=cid),
        name="forward",
    )(x, tab, *weights)
    return [*got[:4], *(w.reshape(layers, -1, w.shape[-1]) for w in got[4:])]


def square(g):
    wide = g.astype(F32)
    return jnp.sum(jnp.sum(wide * wide, 0, keepdims=True), 1, keepdims=True)


def backward(cid, side, h, dy, qkv, o, lse, wqkv, wo, wgu, wd):
    layers, t, d = h.shape
    width = o.shape[2]
    f = wd.shape[1]
    n, nh, cut, group = t // ROWS, width // HEAD, f // side, side * side
    per = 2 + side + n
    gu_shape, d_shape = (side, side, d // group, 2 * cut), (side, f // group, d)
    o_shape, q_shape = (side, side, width // group, d), (side, side, d // group, width)
    gu_task, d_task = Crossed(side, gu_shape[2], gu_shape[3]), Lined(side, d_shape[1], d)
    o_task, q_task = Crossed(side, o_shape[2], d), Crossed(side, q_shape[2], width)
    several = lambda task, n: [pltpu.VMEM((n, *s.shape), s.dtype) if s.memory_space == pltpu.VMEM else pltpu.SemaphoreType.DMA((n, *s.shape)) for s in task.scratch]
    moves = [*several(gu_task, SLOTS), *several(d_task, SLOTS), *o_task.scratch, *several(q_task, 3)]
    own = [pltpu.VMEM((t, d), BF16), pltpu.VMEM((d, t), BF16), pltpu.VMEM((t, d), BF16), pltpu.VMEM((d, t), BF16), pltpu.VMEM((t, d), F32),
           pltpu.VMEM((t, d), BF16), pltpu.VMEM((t, max(3 * cut, 3 * width)), BF16), pltpu.VMEM((2, *gu_shape), BF16),
           pltpu.VMEM((2, *d_shape), BF16), pltpu.VMEM((width, d), F32), pltpu.VMEM(o_shape, BF16), pltpu.VMEM((3, *q_shape), BF16),
           pltpu.VMEM((t, width), F32), pltpu.SemaphoreType.DMA((n + 7,)),
           pltpu.VMEM((group, 8, 128), F32), pltpu.VMEM((8, 128), F32), pltpu.SemaphoreType.DMA((1,)), pltpu.SemaphoreType.DMA((1,)),
           pltpu.VMEM((d, 3 * width), BF16), pltpu.VMEM((2 * (ROWS + n), HEAD // 2), F32), pltpu.VMEM((2, d, 2 * cut), BF16), pltpu.VMEM((2, cut, d), BF16),
           pltpu.VMEM((t, d), BF16), pltpu.VMEM((t, width), BF16), pltpu.SemaphoreType.DMA((2, n))]
    tab = table(t)

    def body(*refs):
        ins, outs, scratch, moved = taken(refs, 10, 5, len(own), len(moves))
        h_hbm, o_hbm, lse_ref, wo_ref, wqkv_hbm, wgu_hbm, wd_hbm, dy_ref, qkv_ref, tab_hbm = ins
        gq_ref, go_ref, ggu_ref, gd_ref, total_ref = outs
        (b_s, bt_s, g_s, gt_s, by_s, h1_s, wide_s, gu_o, d_o, sum_s, wo_o, wqkv_o, dv_s, load, slots, part, send, recv, wqkv_s, tab_ref, wgu_s, wd_s, h_s, o_s, come) = scratch
        dgu_s, act_s, qkv_s = wide_s, wide_s, wide_s
        gu_m, d_m, o_m, q_m = taken(moved, *(len(task.scratch) for task in (gu_task, d_task, o_task, q_task)))
        step = pl.program_id(0)
        layer = layers - 1 - lax.div(step, per)
        phase = lax.rem(step, per)
        top = layer == layers - 1
        last = side + 1
        load_dy = lambda number: pltpu.make_async_copy(dy_ref.at[tile_at(number)], g_s.at[tile_at(number)], load.at[1 + number])

        def load_late():
            return pltpu.make_async_copy(wqkv_hbm.at[layers - 1], wqkv_s, load.at[1 + n]), pltpu.make_async_copy(tab_hbm, tab_ref, load.at[2 + n])

        def load_chunk(layer, chunk, slot):
            for k in range(2):
                cols = pl.ds(pl.multiple_of(k * f + chunk * cut, cut), cut)
                yield pltpu.make_async_copy(wgu_hbm.at[layer, :, cols], wgu_s.at[slot, :, k * cut : (k + 1) * cut], load.at[3 + n + slot])
            yield pltpu.make_async_copy(wd_hbm.at[layer, pl.ds(pl.multiple_of(chunk * cut, cut), cut), :], wd_s.at[slot], load.at[5 + n + slot])

        def load_tile(layer, number):
            for k, (src, dst) in enumerate(((h_hbm, h_s), (o_hbm, o_s))):
                yield pltpu.make_async_copy(src.at[layer, tile_at(number)], dst.at[tile_at(number)], come.at[k, number])

        load_qkv = lambda: pltpu.make_async_copy(qkv_ref.at[layer], qkv_s.at[:, : 3 * width], load.at[0])

        def at(number, more=True):
            return pl.when((phase == number) & more)

        @pl.when(step == 0)
        def _():
            for number in reversed(range(n)):
                for c in (*load_tile(layer, number), load_dy(number)):
                    c.start()
            for c in (*load_chunk(layer, 0, 0), *load_late()):
                c.start()
            greet(Place(side).others())

        @pl.when(step == 1)
        def _():
            pl.semaphore_wait(pltpu.get_barrier_semaphore(), group - 1)

        at(last)(lambda: load_qkv().start())

        @at(0)
        def _():
            def tile(k, _):
                number = n - 1 - k
                here = tile_at(number)
                for c in load_tile(layer, number):
                    c.wait()
                pl.when(top)(lambda: load_dy(number).wait())
                h1 = h_s[here, :] + dot(o_s[here, :], wo_ref[layer]).astype(BF16)
                h1_s[here, :] = h1
                by_s[here, :] = jnp.zeros_like(h1, F32)
                wide = h1.astype(F32)
                b = (wide * scale_of(wide)).astype(BF16)
                b_s[here, :] = b
                bt_s[:, here] = b.T
                gt_s[:, here] = g_s[here, :].T

            lax.fori_loop(0, n, tile, None)

        chunk = phase - 1
        hidden_units = (phase > 0) & (phase < last)

        @pl.when(hidden_units)
        def _():
            turn = lax.rem(chunk, 2)
            arrive(wgu_s.at[turn], load.at[3 + n + turn])
            arrive(wd_s.at[turn], load.at[5 + n + turn])

            @pl.when((chunk < side - 1) | (layer > 0))
            def _():
                end = chunk == side - 1
                for c in load_chunk(jnp.where(end, layer - 1, layer), jnp.where(end, 0, chunk + 1), 1 - turn):
                    c.start()

            wg, wu, wd = wgu_s.at[turn, :, :cut], wgu_s.at[turn, :, cut:], wd_s.at[turn]

            def tile(number, _):
                here = tile_at(number)
                b, g = b_s[here, :], g_s[here, :]
                sub = HEAD
                for c in range(0, cut, sub):
                    cols = slice(c, c + sub)
                    gate, up = dot(b, wg[:, cols]), dot(b, wu[:, cols])
                    dact = dot(g, wd[cols, :], 1, 1)
                    sig = jax.nn.sigmoid(gate)
                    silu = gate * sig
                    act_s[here, 2 * cut + c : 2 * cut + c + sub] = (silu * up).astype(BF16)
                    dgu_s[here, cols] = (dact * up * (sig + silu * (1 - sig))).astype(BF16)
                    dgu_s[here, cut + c : cut + c + sub] = (dact * silu).astype(BF16)
                by_s[here, :] += dot(dgu_s[here, :cut], wg[...], 1, 1) + dot(dgu_s[here, cut : 2 * cut], wu[...], 1, 1)

            lax.fori_loop(0, n, tile, None, unroll=2)

        do_s, kt_s, yt_s, dk_s, dq_s = h1_s, bt_s, gt_s, by_s, sum_s

        @at(last)
        def _():
            def tile(number, _):
                here = tile_at(number)
                h1 = h1_s[here, :].astype(F32)
                r = scale_of(h1)
                dh1 = (g_s[here, :].astype(F32) + normed_bwd(h1 * r, r, by_s[here, :])).astype(BF16)
                g_s[here, :] = dh1
                dk_s[here, :] = jnp.zeros((ROWS, width), F32)
                dv_s[here, :] = jnp.zeros((ROWS, width), F32)
                do_s[here, :] = dot(dh1, wo_ref[layer], 1, 1).astype(BF16)
                sum_s[...] = jnp.where(number == 0, 0.0, sum_s[...]) + dot(o_s[here, :].T, dh1)

            lax.fori_loop(0, n, tile, None)
            wo_o[...] = sum_s[...].astype(BF16).reshape(o_shape)

        heads = [slice(m * HEAD, (m + 1) * HEAD) for m in range(nh)]

        @at(last + 1)
        def _():
            load_qkv().wait()

            @pl.when(top)
            def _():
                for c in load_late():
                    c.wait()

            for j in range(0, t, ROWS):
                for h in heads:
                    kt_s[h, j : j + ROWS] = qkv_s[j : j + ROWS, width + h.start : width + h.stop].T

        @pl.when(phase > last)
        def _():
            i = per - 1 - phase
            here = tile_at(i)
            qs = [qkv_s[here, h] for h in heads]
            dos = [do_s[here, h] for h in heads]
            deltas = []
            for m, h in enumerate(heads):
                delta = (dos[m].astype(F32) * o_s[here, h].astype(F32)).sum(-1, keepdims=True)
                deltas.append(jnp.broadcast_to(delta, (ROWS, 128)).T[:1, :])
            lses = [lse_ref[layer, m : m + 1, here] for m in range(nh)]

            def block(keys, start, hide, first):
                span = slice(start, ROWS)
                scores = [dot(qkv_s[keys, width + h.start : width + h.stop], q[span, :], 1, 1) for h, q in zip(heads, qs)]
                dps = [dot(qkv_s[keys, 2 * width + h.start : 2 * width + h.stop], g[span, :], 1, 1) for h, g in zip(heads, dos)]
                for m, h in enumerate(heads):
                    p = jnp.exp2(scores[m] * LOG2E - lses[m][:, span])
                    if hide is not None:
                        p = jnp.where(hide, 0.0, p)
                    ds = (p * (dps[m] - deltas[m][:, span])).astype(BF16)
                    dv_s[keys, h] += dot(p.astype(BF16), dos[m][span, :])
                    dk_s[keys, h] += dot(ds, qs[m][span, :])
                    dq = dot(kt_s[h, keys], ds)
                    dq_s[h, span] = dq if first else dq_s[h, span] + dq

            wide = h_s[here, :].astype(F32)
            yt_s[:, here] = (wide * scale_of(wide)).astype(BF16).T
            half = ROWS // 2
            hide = hidden(ROWS)
            block(pl.ds(pl.multiple_of(i * ROWS, ROWS), half), 0, hide[:half, :], True)
            block(pl.ds(pl.multiple_of(i * ROWS + half, half), half), half, hide[:half, :half], False)
            lax.fori_loop(0, i, lambda j, _: block(tile_at(j), 0, None, False), None)
            cos, sin = angles(tab_ref, i)
            for h in heads:
                qkv_s[here, h] = rotated((dq_s[h, :] * HEAD**-0.5).astype(BF16).T.astype(F32), cos, -sin).astype(BF16)
                qkv_s[here, width + h.start : width + h.stop] = rotated(dk_s[here, h], cos, -sin).astype(BF16)
                qkv_s[here, 2 * width + h.start : 2 * width + h.stop] = dv_s[here, h].astype(BF16)

            @pl.when(top)
            def _():
                by = dot(qkv_s[here, : 3 * width], wqkv_s[...], 1, 1)
                wide = h_s[here, :].astype(F32)
                r = scale_of(wide)
                y = wide * r
                g_s[here, :] = (g_s[here, :].astype(F32) + normed_bwd(y, r, by)).astype(BF16)

            @pl.when(layer > 0)
            def _():
                for c in load_tile(layer - 1, i):
                    c.start()

        def qkvs(stage, of, which=(0, 1, 2)):
            for k in which:
                q_task.run(stage, Place(side), wqkv_o.at[k], gq_ref.at[of, :, k * width : (k + 1) * width], [r.at[k] for r in q_m])


        def both(chunk, stage):
            slot, source = lax.rem(chunk, SLOTS), lax.rem(chunk, 2)
            d_task.run(stage, Place(side), chunk, d_o.at[source], gd_ref.at[layer], [r.at[slot] for r in d_m])
            gu_task.run(stage, Place(side), gu_o.at[source], ggu_ref.at[layer, chunk], [r.at[slot] for r in gu_m])

        def out(stage):
            o_task.run(stage, Place(side), wo_o, go_ref.at[layer], o_m)

        when = [[], [c + 2 for c in range(side)], [c + 3 for c in range(side)], [c + 4 for c in range(side - 1)]]
        when[1][-1] = last + 1
        when[2][-2:] = last, last + 2
        when[3][-2:] = last, last + 1

        for stage in (2, 3, 1):

            @pl.when(functools.reduce(jnp.logical_or, [phase == p for p in when[stage]]))
            def _():
                both(sum(jnp.where(phase == p, c, 0) for c, p in enumerate(when[stage])), stage)

        for stage in range(3):
            at(last + stage)(lambda: out(stage))
        for stage in range(1, 4):
            at(stage, ~top)(lambda: qkvs(stage, layer + 1))

        @pl.when(hidden_units)
        def _():
            slot = lax.rem(chunk, 2)
            for c in range(0, 2 * cut, cut):
                gu_o[slot, :, :, :, c : c + cut] = dot(bt_s[...], dgu_s[:, c : c + cut]).astype(BF16).reshape(*gu_shape[:3], cut)
            d_o[slot] = dot(gt_s[...], act_s[:, 2 * cut : 3 * cut]).astype(BF16).T.reshape(d_shape)
            both(chunk, 0)

        @at(per - 1)
        def _():
            for k in range(3):
                wqkv_o[k] = dot(yt_s[...], qkv_s[:, k * width : (k + 1) * width]).astype(BF16).reshape(q_shape)
                qkvs(0, layer, (k,))
            both(side - 1, 3)
            out(3)

        @pl.when(step == layers * per - 1)
        def _():
            place = Place(side)
            mine = sum(square(gq_ref[k]) for k in range(1, layers))
            for k in range(layers):
                mine += square(go_ref[k]) + square(gd_ref[k])
                for c in range(side):
                    mine += square(ggu_ref[k, c])
            qkvs(1, 0)
            qkvs(2, 0)
            qkvs(3, 0)
            mine = jnp.broadcast_to(mine + square(gq_ref[0]), part.shape)
            part[...] = mine
            slots[place.me] = mine
            for device in place.others():
                remote(part, slots.at[place.me], send.at[0], recv.at[0], device).start()
            arrived(slots.at[: group - 1], send.at[0], recv.at[0], place.others()[0])
            total_ref[...] = slots[...].sum(0)

    outs = [sds((layers, q_shape[2], 3 * width), BF16), sds((layers, o_shape[2], d), BF16), sds((layers, side, *gu_shape[2:]), BF16),
            sds((layers, *d_shape[1:]), BF16), sds((8, 128), F32)]
    return pl.pallas_call(
        body,
        grid=(layers * per,),
        in_specs=[ANY, ANY, whole(lse.shape), whole(wo.shape), *[ANY] * 6],
        out_specs=[whole(a.shape) for a in outs],
        out_shape=outs,
        scratch_shapes=[*own, *moves],
        compiler_params=pltpu.CompilerParams(dimension_semantics=("arbitrary",), vmem_limit_bytes=VMEM, has_side_effects=True, collective_id=cid),
        name="backward",
    )(h, o, lse, wo, wqkv, wgu, wd, dy, qkv, tab)


def adamw(total, count, weights, m, v, gq, go, ggu, gd):
    layers, side = ggu.shape[:2]

    def body(total_ref, gq_ref, go_ref, ggu_ref, gd_ref, *refs):
        w_refs, m_refs, v_refs, wn_refs, mn_refs, vn_refs = taken(refs, *[7] * 6)
        factor = jnp.minimum(1.0, 0.5 * lax.rsqrt(total_ref[0:1, 0:1] / count + 1e-30))

        def update(i, columns, g):
            g = g.astype(F32) * factor
            at = (0, slice(None), columns)
            mn = 0.9 * m_refs[i][at] + 0.1 * g
            vn = 0.95 * v_refs[i][at] + 0.05 * g * g
            mn_refs[i][at], vn_refs[i][at] = mn, vn
            w = w_refs[i][at].astype(F32)
            wn_refs[i][at] = (w - 0.02 * (mn * lax.rsqrt(vn + 1e-8) + 0.1 * w)).astype(BF16)

        every = slice(None)
        wide = gq_ref.shape[2] // 3
        for i in range(3):
            update(i, every, gq_ref[0, :, i * wide : (i + 1) * wide])
        update(3, every, go_ref[0])
        cut = ggu_ref.shape[3] // 2
        for c in range(side):
            for i in range(2):
                update(4 + i, slice(c * cut, (c + 1) * cut), ggu_ref[0, c, :, i * cut : (i + 1) * cut])
        update(6, every, gd_ref[0])

    one = lambda a: pl.BlockSpec((1, *a.shape[1:]), lambda l: (l,) + (0,) * (a.ndim - 1))
    own = [one(a) for a in weights]
    return pl.pallas_call(
        body,
        grid=(layers,),
        in_specs=[whole(total.shape), *(one(a) for a in (gq, go, ggu, gd)), *own * 3],
        out_specs=own * 3,
        out_shape=[*(sds(a.shape, BF16) for a in weights), *(sds(a.shape, F32) for a in (*m, *v))],
        compiler_params=pltpu.CompilerParams(dimension_semantics=("arbitrary",), vmem_limit_bytes=VMEM),
        name="adamw",
    )(total, gq, go, ggu, gd, *weights, *m, *v)


def solution(mesh):
    group = mesh.shape["dp"]
    side = side_of(group)

    def step(x, dy, *arrays):
        weights, m, v = (arrays[i : i + 7] for i in (0, 7, 14))
        x, dy = x[0], dy[0]
        qkv, o, lse, h, wqkv, wo, wgu, wd = forward(0, side, x, weights)
        *grads, total = backward(1, side, h, dy, qkv, o, lse, wqkv, wo, wgu, wd)
        return tuple(adamw(total, group * sum(w.size for w in weights), weights, m, v, *grads))

    states, cut = P(("rep", "dp"), None, None), P(None, "dp", None)
    return jax.shard_map(
        step,
        mesh=mesh,
        in_specs=(states, states) + (cut,) * 21,
        out_specs=(P("rep", "dp", None),) * 21,
        check_vma=False,
    )
```

```python
import functools

import jax
import jax.numpy as jnp
import numpy as np
from jax import lax
from jax.experimental import pallas as pl
from jax.experimental.pallas import tpu as pltpu
from jax.sharding import PartitionSpec as P

HEAD = 256
THETA = 10000
LOG2E = 1.4426950408889634
VMEM = 67_000_000
EPS = 1e-6
F32, BF16 = jnp.float32, jnp.bfloat16
MESH = pl.DeviceIdType.MESH
ANY = pl.BlockSpec(memory_space=pl.ANY)
ROWS = 512
STRIP = 256
SLOTS = 3
sds = jax.ShapeDtypeStruct


def dot(a, b, ca=1, cb=0):
    return lax.dot_general(a, b, (((ca,), (cb,)), ((), ())), preferred_element_type=F32)


def scale_of(h):
    return lax.rsqrt(jnp.mean(h * h, -1, keepdims=True) + EPS)


def normed_bwd(y, r, by):
    return r * (by - y * jnp.mean(by * y, -1, keepdims=True))


def table(tokens):
    half = HEAD // 2
    rate = np.float32(THETA) ** (-np.arange(half, dtype=np.float32) / np.float32(half))
    places = [np.arange(0, ROWS), np.arange(0, tokens, ROWS)]
    return jnp.asarray(np.concatenate([f(p[:, None] * rate.astype(np.float64)) for p in places for f in (np.cos, np.sin)]), F32)


def angles(ref, tile):
    n = ref.shape[0] // 2 - ROWS
    near_c, near_s = ref[:ROWS, :], ref[ROWS : 2 * ROWS, :]
    c, s = ref[pl.ds(2 * ROWS + tile, 1), :], ref[pl.ds(2 * ROWS + n + tile, 1), :]
    return c * near_c - s * near_s, s * near_c + c * near_s


def rotated(t, cos, sin):
    half = t.shape[-1] // 2
    a, b = t[:, :half], t[:, half:]
    return jnp.concatenate([a * cos - b * sin, b * cos + a * sin], -1)


def hidden(size):
    return lax.broadcasted_iota(jnp.int32, (size, size), 0) > lax.broadcasted_iota(jnp.int32, (size, size), 1)


def tile_at(n, size=ROWS):
    return pl.ds(pl.multiple_of(n * size, size), size)


def whole(shape):
    return pl.BlockSpec(shape, lambda *_: (0,) * len(shape), pipeline_mode=pl.Buffered(1))


def side_of(group):
    return int(round(group**0.5))


class Place:
    def __init__(self, side):
        rep, me = lax.axis_index("rep"), lax.axis_index("dp")
        self.side, self.me, self.x, self.y, self.core = side, me, lax.div(me, side), lax.rem(me, side), lax.rem(rep, 2)
        self.partner = {"rep": rep + 1 - 2 * self.core}

    def on(self, axis, k):
        at = lax.rem((self.x, self.y)[axis] + k, self.side)
        return at, {"dp": at * self.side + self.y if axis == 0 else self.x * self.side + at}

    def line(self):
        return [self.on(axis, k)[1] for axis in (0, 1) for k in range(1, self.side)]

    def others(self):
        n = self.side**2
        return [{"dp": lax.rem(self.me + k, n)} for k in range(1, n)]


def greet(devices):
    for device in devices:
        pl.semaphore_signal(pltpu.get_barrier_semaphore(), inc=1, device_id=device, device_id_type=MESH)


def remote(src, dst, send, recv, device):
    return pltpu.make_async_remote_copy(src_ref=src, dst_ref=dst, send_sem=send, recv_sem=recv, device_id=device, device_id_type=MESH)


def arrive(ref, sem):
    pltpu.make_async_copy(ref, ref, sem).wait()


def arrived(ref, send, recv, device):
    c = remote(ref, ref, recv if send is None else send, send if recv is None else recv, device)
    if recv is not None:
        c.wait_recv()
    if send is not None:
        c.wait_send()


class Gather:
    def __init__(self, side, rows, widths, by_rows, relayed):
        self.side, self.widths, self.by_rows, self.relayed = side, widths, by_rows, relayed
        n = side - 1
        self.shape = (side, side, rows, sum(widths))
        self.matrix = pltpu.VMEM(self.shape, BF16)
        self.sems = [pltpu.SemaphoreType.DMA((k,)) for k in (len(widths) + 2, 2, 2, 2 * n, 2, 2)]

    def run(self, stage, place, layer, shards, result, out, sems):
        local, send, come, across, near, far = sems
        n = self.side - 1
        copies, column = [], 0
        for k, (shard, width) in enumerate(zip(shards, self.widths, strict=True)):
            copies.append((shard.at[layer], out.at[place.x, place.y, :, column : column + width], local.at[k]))
            column += width
        size = out.shape[2] if self.by_rows else out.shape[3]
        every = slice(None)

        def copied(own):
            core = place.core if own else 1 - place.core
            piece = pl.ds(pl.multiple_of(core * (size // 2), size // 2), size // 2)
            at = (every, every, piece, every) if self.by_rows else (every, every, every, piece)
            return pltpu.make_async_copy(out.at[at], result.at[(layer, *at)], local.at[len(shards) + own])

        if stage == 0:
            for c in copies:
                pltpu.make_async_copy(*c).start()
        elif stage == 1:
            for c in copies:
                pltpu.make_async_copy(*c).wait()
        elif stage == 6:
            copied(0).wait()
            copied(1).wait()
            arrived(out.at[0, :n], send.at[0], None, place.partner)
            arrived(out.at[:n], send.at[1], None, place.partner)
        for q, waits in [(0, True), (1, True)] * (stage == 2) + [(0, False), (1, False)]:

            def view(at, core=place.core):
                piece = pl.ds(pl.multiple_of(core * (size // 2) + q * (size // 4), size // 4), size // 4)
                return out.at[at[0], at[1], piece, :] if self.by_rows else out.at[at[0], at[1], :, piece]

            along = lambda at: (at, place.y) if q == 0 else (place.x, at)
            over = lambda at: (every, at) if q == 0 else (at, every)
            here, line = view((place.x, place.y)), view(over(place.y if q == 0 else place.x))
            if stage == 1:
                for k in range(1, n + 1):
                    remote(here, here, send.at[0], come.at[q], place.on(q, k)[1]).start()
            elif waits:
                arrived(view((0, slice(0, n))), None, come.at[q], place.partner)
            elif stage == 2:
                for k in (1, n) if self.relayed else range(1, n + 1):
                    remote(line, line, send.at[1], across.at[q * n + k - 1], place.on(1 - q, k)[1]).start()
                for k in range(1, n + 1):
                    got = view(along(place.on(q, k)[0]))
                    remote(got, got, send.at[0], near.at[q], place.partner).start()
            elif stage in (3, 4):
                for k in ((1, n) if stage == 3 else (2,)) if self.relayed else range(1, n + 1) if stage == 3 else ():
                    at = place.on(1 - q, self.side - k)[0]
                    got = view(over(at))
                    arrived(got, None, across.at[q * n + k - 1], place.partner)
                    if self.relayed and stage == 3:
                        half = slice(0, self.side // 2) if k == 1 else slice(self.side // 2, self.side)
                        part = view((half, at) if q == 0 else (at, half))
                        remote(part, part, send.at[1], across.at[q * n + 1], place.on(1 - q, k)[1]).start()
                    remote(got, got, send.at[1], far.at[q], place.partner).start()
            elif stage == 5:
                arrived(view((0, slice(0, n))), None, near.at[q], place.partner)
                arrived(view((slice(0, n), every)), None, far.at[q], place.partner)
        if stage == (4 if self.relayed else 5):
            copied(1).start()
        if stage == 5:
            copied(0).start()


class Ring:
    def __init__(self, half):
        self.scratch = [pltpu.VMEM((2, *half), BF16), pltpu.VMEM((2, *half), BF16), pltpu.VMEM((2, 2, *half), BF16), pltpu.SemaphoreType.DMA((2,)),
                        pltpu.SemaphoreType.DMA((2,))]

    def start(self, place, axis, blocks, scratch, last=False):
        far, mid, near, send, recv = scratch
        opposite, _ = place.on(axis, 2)
        for relayed in (True, False):
            for d, k in enumerate((1, place.side - 1)):
                there, to = place.on(axis, k)
                if last:
                    if relayed:
                        remote(mid.at[d], near.at[d, d], send.at[1], recv.at[1], to).start()
                elif relayed:
                    remote(blocks(opposite, d), far.at[d], send.at[0], recv.at[0], to).start()
                else:
                    remote(blocks(there, 1 - d), near.at[d, 1 - d], send.at[1], recv.at[1], to).start()

    def middle(self, place, axis, blocks, scratch):
        far, mid, near, send, recv = scratch
        arrived(far, send.at[0], recv.at[0], place.on(axis, 1)[1])
        for d, k in enumerate((1, place.side - 1)):
            there, _ = place.on(axis, k)
            mid[d] = (blocks(there, d)[...].astype(F32) + far[d].astype(F32)).astype(BF16)
        self.start(place, axis, blocks, scratch, True)

    def end(self, place, axis, blocks, scratch):
        far, mid, near, send, recv = scratch
        arrived(near, send.at[1], recv.at[1], place.on(axis, 1)[1])

    def total(self, blocks, scratch, at, cut):
        near = scratch[2]
        return blocks(at, cut)[...].astype(F32) + near[0, cut].astype(F32) + near[1, cut].astype(F32)


class Crossed:
    def __init__(self, side, rows, width):
        self.side, self.width = side, width
        n, half = side - 1, width // 2
        self.ring = Ring((side // 2, rows, half))
        self.scratch = [*self.ring.scratch * 2, pltpu.VMEM((2, side, rows, half), BF16), pltpu.VMEM((2, n, rows, half), BF16),
                        pltpu.VMEM((2, rows, half), F32), pltpu.SemaphoreType.DMA((1,)), pltpu.SemaphoreType.DMA((1,))]

    def run(self, stage, place, src, out, scratch):
        *rings, (mid, two, own, send, recv) = taken(scratch, 5, 5, 5)
        n, half, cut = self.side - 1, self.width // 2, self.side // 2
        along = (lambda j, h: src.at[j, h * cut : (h + 1) * cut, :, :half]), (lambda j, h: src.at[h * cut : (h + 1) * cut, j, :, half:])
        for q in range(2):
            at = (place, q, along[q], rings[q])
            if stage == 0:
                self.ring.start(*at)
            elif stage == 1:
                self.ring.middle(*at)
            elif stage == 2:
                self.ring.end(*at)
                for h in range(2):
                    mid[q, h * cut : (h + 1) * cut] = self.ring.total(along[q], rings[q], (place.x, place.y)[q], h).astype(BF16)
                j = (place.y, place.x)[q]
                mine = (src[place.x, place.y, :, :half] if q == 0 else src[place.x, place.y, :, half:]).astype(F32)
                own[q] = mine + sum(rings[q][2][d, lax.div(j, cut), lax.rem(j, cut)].astype(F32) for d in range(2))
        if stage == 2:
            for q in range(2):
                for k in range(n):
                    there, to = place.on(1 - q, k + 1)
                    remote(mid.at[q, there], two.at[q, k], send.at[0], recv.at[0], to).start()
        elif stage == 3:
            arrived(two, send.at[0], recv.at[0], place.on(0, 1)[1])
            for q in range(2):
                t = own[q]
                for k in range(n):
                    t += two[q, k].astype(F32)
                out[:, q * half : (q + 1) * half] = t.astype(BF16)


class Lined:
    def __init__(self, side, rows, width):
        self.side, self.rows = side, rows
        n = side - 1
        self.ring = Ring((rows // 2, width))
        self.scratch = [*self.ring.scratch, pltpu.VMEM((rows, width), BF16), pltpu.VMEM((n, rows, width), BF16),
                        pltpu.VMEM((rows, width), F32), pltpu.SemaphoreType.DMA((1,)), pltpu.SemaphoreType.DMA((1,))]

    def run(self, stage, place, line, src, out, scratch):
        ring, (mid, two, own, send, recv) = taken(scratch, 5, 5)
        n, cut = self.side - 1, self.rows // 2
        ahead = lax.rem(line - place.x + self.side, self.side)
        at = (place, 1, lambda j, h: src.at[j, h * cut : (h + 1) * cut, :], ring)

        def second():
            return remote(mid, two.at[ahead - 1], send.at[0], recv.at[0], place.on(0, ahead)[1])

        if stage == 0:
            self.ring.start(*at)
        elif stage == 1:
            self.ring.middle(*at)
        elif stage == 2:
            self.ring.end(*at)
            for h in range(2):
                t = self.ring.total(at[2], ring, place.y, h)
                own[h * cut : (h + 1) * cut, :] = t
                mid[h * cut : (h + 1) * cut, :] = t.astype(BF16)
            pl.when(ahead != 0)(lambda: second().start())
        else:
            pl.when(ahead != 0)(lambda: second().wait_send())

            @pl.when(ahead == 0)
            def _():
                arrived(two, None, recv.at[0], place.on(0, 1)[1])
                t = own[...]
                for k in range(n):
                    t += two[k].astype(F32)
                out[...] = t.astype(BF16)


def taken(refs, *counts):
    out, at = [], 0
    for n in counts:
        out.append(refs[at : at + n])
        at += n
    return out


def forward(cid, side, x, weights):
    t, d = x.shape
    layers, width = weights[0].shape[0], weights[0].shape[2]
    f = weights[4].shape[2]
    nh, n = width // HEAD, t // ROWS
    shard = d // side**2
    tasks = [Gather(side, shard, [width] * 3, False, False), Gather(side, shard, [width], False, True), Gather(side, shard, [f, f], False, True),
             Gather(side, f // side**2, [d], True, True)]
    kinds = len(tasks)
    flat = [pltpu.VMEM((layers, *tasks[0].shape), BF16), *(task.matrix for _ in range(layers) for task in tasks[1:])]
    sems = [s for layer in range(layers) for task in (tasks[1:] if layer else tasks) for s in task.sems]
    own = [pltpu.VMEM((t, width), BF16), pltpu.VMEM((nh, HEAD + 8, t), BF16), pltpu.VMEM((nh, ROWS), F32), pltpu.VMEM((nh, HEAD + 8, ROWS), F32),
           pltpu.VMEM((t, width), BF16), pltpu.VMEM((t, d), BF16), pltpu.VMEM((ROWS, f), BF16), pltpu.VMEM((nh * ROWS // STRIP, ROWS, STRIP), F32),
           pltpu.VMEM((nh, ROWS), F32), pltpu.VMEM((t, d), BF16), pltpu.VMEM((2 * (ROWS + n), HEAD // 2), F32), pltpu.SemaphoreType.DMA((n + 1,))]
    tab = table(t)

    def body(*refs):
        (x_hbm, tab_hbm), shards, outs, scratch, moved = taken(refs, 2, 7, 4 + kinds, len(own), len(flat) + len(sems))
        qkv_ref, o_ref, lse_ref, h_ref, *wholes = outs
        k_s, vt_s, top_s, mix_s, o_s, h2_s, act_s, s_s, keep_s, x_s, tab_ref, load = scratch
        w_s = moved[0]
        matrices = [[w_s.at[layer], *m] for layer, m in enumerate(taken(moved[1:], *[kinds - 1] * layers))]
        flags = taken(moved[len(flat) :], *[6] * (layers * (kinds - 1) + 1))
        parts = [shards[:3], shards[3:4], shards[4:6], shards[6:]]
        step = pl.program_id(0)

        def go(layer, which, *stages):
            for stage in stages:
                for kind in which:
                    tasks[kind].run(stage, Place(side), layer, parts[kind], wholes[kind], matrices[layer][kind], flags[kind + (kinds - 1) * layer * (kind > 0)])

        def at(number):
            return pl.when(step == number)

        attention, ffn = (0,), (1, 2, 3)
        load_x = lambda number: pltpu.make_async_copy(x_hbm.at[tile_at(number)], x_s.at[tile_at(number)], load.at[number])
        load_tab = lambda: pltpu.make_async_copy(tab_hbm, tab_ref, load.at[n])

        @at(0)
        def _():
            place = Place(side)
            peers = [*place.line(), place.partner]
            greet(peers)
            go(0, attention + ffn, 0)
            for number in range(n):
                load_x(number).start()
            load_tab().start()
            for m in range(nh):
                vt_s[m, HEAD:, :] = jnp.ones((8, t), BF16)
            pl.semaphore_wait(pltpu.get_barrier_semaphore(), len(peers))
            go(0, attention, 1)
            go(0, ffn, 1)
            go(0, attention, 2, 3)
            go(0, ffn, 2)
            go(0, attention, 5)
            load_tab().wait()

        @pl.when(step < n)
        def _():
            load_x(step).wait()
            h_ref[0] = x_s[tile_at(step), :]

        @at(n)
        def _():
            go(0, ffn, 4, 5)

        def matrix(layer, kind):
            return matrices[layer][kind]

        second = step >= 2 * n

        @pl.when((step < n) | second)
        def _():
            i = lax.rem(step, n)
            here = tile_at(i)
            layer = lax.div(step, 2 * n)

            h = jnp.where(second, h2_s[here, :], x_s[here, :])
            h = h.astype(F32)
            a = (h * scale_of(h)).astype(BF16)
            heads = [slice(m * HEAD, (m + 1) * HEAD) for m in range(nh)]
            raw = [[dot(a, w_s[layer, :, :, :, k * width + at.start : k * width + at.stop].reshape(d, HEAD)).astype(BF16) for k in range(3)] for at in heads]
            cos, sin = angles(tab_ref, i)
            pieces = [(m, slice(c, c + STRIP)) for m in range(nh) for c in range(0, ROWS, STRIP)]
            qs = []
            for m, at in enumerate(heads):
                q = rotated(raw[m][0].astype(F32), cos, sin).astype(BF16) * jnp.asarray(HEAD**-0.5, BF16)
                k = rotated(raw[m][1].astype(F32), cos, sin).astype(BF16)
                qkv_ref[0, :, at], qkv_ref[0, :, width + at.start : width + at.stop] = q, k
                qkv_ref[0, :, 2 * width + at.start : 2 * width + at.stop] = raw[m][2]
                vt_s[m, :HEAD, here] = raw[m][2].T
                k_s[here, at] = k
                qs.append(q)
                for p, (head, cols) in enumerate(pieces):
                    if head == m:
                        s = jnp.where(hidden(ROWS)[:, cols], -1e30, dot(k, q[cols, :], 1, 1))
                        s_s[p] = s
                        top_s[m : m + 1, cols] = s.max(0, keepdims=True)

            def scores(k, j):
                m, cols = pieces[k]
                return dot(k_s[tile_at(j), m * HEAD : (m + 1) * HEAD], qs[m][cols, :], 1, 1)

            def weights(k, top):
                return jnp.exp2((s_s[k] - top) * LOG2E).astype(BF16)

            def add(k, j, p, diagonal):
                m, cols = pieces[k]
                old = jnp.where(diagonal, 0.0, mix_s[m, :, cols] * keep_s[m : m + 1, cols])
                mix_s[m, :, cols] = old + dot(vt_s[m, :, tile_at(j)], p)

            def turn(j, _):
                before = jnp.where(j == 0, i, j - 1)
                late = None
                for k, (m, cols) in enumerate(pieces):
                    s = scores(k, j)
                    top = top_s[m : m + 1, cols]
                    p = weights(k, top)
                    s_s[k] = s
                    new = jnp.maximum(top, s.max(0, keepdims=True))
                    if late:
                        add(*late)
                        keep_s[pieces[k - 1][0] : pieces[k - 1][0] + 1, pieces[k - 1][1]] = keep
                    top_s[m : m + 1, cols] = new
                    keep = jnp.exp2((top - new) * LOG2E)
                    late = k, before, p, j == 0
                add(*late)
                keep_s[m : m + 1, cols] = keep

            pl.when(step == 3 * n - 1)(lambda: go(1, ffn, 5))
            lax.fori_loop(0, i, turn, None)
            end = jnp.where(i == 0, i, i - 1)

            def out(m):
                at = heads[m]
                total = mix_s[m, HEAD : HEAD + 1, :]
                o = (mix_s[m, :HEAD, :] * (1 / total)).astype(BF16).T
                o_ref[0, :, at] = o
                o_s[here, at] = o
                lse_ref[0, m : m + 1, :] = top_s[m : m + 1, :] * LOG2E + jnp.log2(total)

            late = None
            for k, (m, cols) in enumerate(pieces):
                p = weights(k, top_s[m : m + 1, cols])
                if late:
                    add(*late)
                    if pieces[k - 1][0] != m:
                        out(m - 1)
                late = k, end, p, i == 0
            add(*late)
            out(nh - 1)

        @pl.when((step >= n) & ~second)
        def _():
            here = tile_at(step - n)
            wo, wgu, wd = (matrix(0, kind) for kind in ffn)
            h1 = x_s[here, :] + dot(o_s[here, :], wo[...].reshape(width, d)).astype(BF16)
            wide = h1.astype(F32)
            b = (wide * scale_of(wide)).astype(BF16)
            cut = f // side
            for c in range(0, f, cut):
                gate = dot(b, wgu[:, :, :, c : c + cut].reshape(d, cut))
                up = dot(b, wgu[:, :, :, f + c : f + c + cut].reshape(d, cut))
                act_s[:, c : c + cut] = (gate * jax.nn.sigmoid(gate) * up).astype(BF16)
            h2 = h1 + dot(act_s[...], wd[...].reshape(f, d)).astype(BF16)
            h_ref[0] = h2
            h2_s[here, :] = h2

        plan = {0: [(0, attention, 6), (1, attention + ffn, 0)], n - 2: [(0, ffn, 3), (1, attention + ffn, 1)],
                n: [(1, attention + ffn, 2)], n + 2: [(1, attention, 3)], 2 * n - 1: [(1, attention, 5)], 2 * n: [(1, ffn, 3)],
                3 * n - 2: [(1, ffn, 4)], 3 * n - 1: [(0, ffn, 6), (1, attention + ffn, 6)]}
        for number, todo in plan.items():

            @at(number)
            def _():
                for what in todo:
                    go(*what)

    tile = lambda s: jnp.where(s < 2 * n, jnp.minimum(s, n - 1), s - 2 * n)
    by_layer = lambda w: pl.BlockSpec((1, ROWS, w), lambda s: (s // (2 * n), tile(s), 0))
    got = pl.pallas_call(
        body,
        grid=(3 * n,),
        in_specs=[ANY] * 9,
        out_specs=[by_layer(3 * width), by_layer(width), pl.BlockSpec((1, nh, ROWS), lambda s: (s // (2 * n), 0, tile(s))),
                   pl.BlockSpec((1, ROWS, d), lambda s: (jnp.where(s < n, 0, 1), jnp.where(s < 2 * n, lax.rem(s, n), n - 1), 0)), *[ANY] * kinds],
        out_shape=[sds((layers, t, 3 * width), BF16), sds((layers, t, width), BF16), sds((layers, nh, t), F32), sds((layers, t, d), BF16),
                   *(sds((layers, *task.shape), BF16) for task in tasks)],
        scratch_shapes=[*own, *flat, *sems],
        compiler_params=pltpu.CompilerParams(dimension_semantics=("arbitrary",), vmem_limit_bytes=VMEM, has_side_effects=True, collective_id=cid),
        name="forward",
    )(x, tab, *weights)
    return [*got[:4], *(w.reshape(layers, -1, w.shape[-1]) for w in got[4:])]


def square(g):
    wide = g.astype(F32)
    return jnp.sum(jnp.sum(wide * wide, 0, keepdims=True), 1, keepdims=True)


def backward(cid, side, h, dy, qkv, o, lse, wqkv, wo, wgu, wd):
    layers, t, d = h.shape
    width = o.shape[2]
    f = wd.shape[1]
    n, nh, cut, group = t // ROWS, width // HEAD, f // side, side * side
    per = 2 + side + n
    gu_shape, d_shape = (side, side, d // group, 2 * cut), (side, f // group, d)
    o_shape, q_shape = (side, side, width // group, d), (side, side, d // group, width)
    gu_task, d_task = Crossed(side, gu_shape[2], gu_shape[3]), Lined(side, d_shape[1], d)
    o_task, q_task = Crossed(side, o_shape[2], d), Crossed(side, q_shape[2], width)
    several = lambda task, n: [pltpu.VMEM((n, *s.shape), s.dtype) if s.memory_space == pltpu.VMEM else pltpu.SemaphoreType.DMA((n, *s.shape)) for s in task.scratch]
    moves = [*several(gu_task, SLOTS), *several(d_task, SLOTS), *o_task.scratch, *several(q_task, 3)]
    own = [pltpu.VMEM((t, d), BF16), pltpu.VMEM((d, t), BF16), pltpu.VMEM((t, d), BF16), pltpu.VMEM((d, t), BF16), pltpu.VMEM((t, d), F32),
           pltpu.VMEM((t, d), BF16), pltpu.VMEM((t, max(3 * cut, 3 * width)), BF16), pltpu.VMEM((2, *gu_shape), BF16),
           pltpu.VMEM((2, *d_shape), BF16), pltpu.VMEM((width, d), F32), pltpu.VMEM(o_shape, BF16), pltpu.VMEM((3, *q_shape), BF16),
           pltpu.VMEM((t, width), F32), pltpu.SemaphoreType.DMA((n + 9,)),
           pltpu.VMEM((group, 8, 128), F32), pltpu.VMEM((8, 128), F32), pltpu.SemaphoreType.DMA((1,)), pltpu.SemaphoreType.DMA((1,)),
           pltpu.VMEM((d, 3 * width), BF16), pltpu.VMEM((2 * (ROWS + n), HEAD // 2), F32), pltpu.VMEM((2, d, 2 * cut), BF16), pltpu.VMEM((2, cut, d), BF16),
           pltpu.VMEM((t, d), BF16), pltpu.VMEM((t, width), BF16), pltpu.SemaphoreType.DMA((2, n)),
           pltpu.VMEM(lse.shape, F32), pltpu.VMEM(wo.shape, BF16)]
    tab = table(t)

    def body(*refs):
        ins, outs, scratch, moved = taken(refs, 10, 5, len(own), len(moves))
        h_hbm, o_hbm, lse_hbm, wo_hbm, wqkv_hbm, wgu_hbm, wd_hbm, dy_ref, qkv_ref, tab_hbm = ins
        gq_ref, go_ref, ggu_ref, gd_ref, total_ref = outs
        (b_s, bt_s, g_s, gt_s, by_s, h1_s, wide_s, gu_o, d_o, sum_s, wo_o, wqkv_o, dv_s, load, slots, part, send, recv, wqkv_s, tab_ref, wgu_s, wd_s, h_s, o_s, come, lse_ref, wo_ref) = scratch
        dgu_s, act_s, qkv_s = wide_s, wide_s, wide_s
        gu_m, d_m, o_m, q_m = taken(moved, *(len(task.scratch) for task in (gu_task, d_task, o_task, q_task)))
        step = pl.program_id(0)
        layer = layers - 1 - lax.div(step, per)
        phase = lax.rem(step, per)
        top = layer == layers - 1
        last = side + 1
        load_dy = lambda number: pltpu.make_async_copy(dy_ref.at[tile_at(number)], g_s.at[tile_at(number)], load.at[1 + number])

        def load_late():
            return [pltpu.make_async_copy(*c, load.at[k])
                    for k, c in ((1 + n, (wqkv_hbm.at[layers - 1], wqkv_s)), (2 + n, (tab_hbm, tab_ref)), (7 + n, (lse_hbm, lse_ref)))]

        load_wo = lambda: pltpu.make_async_copy(wo_hbm, wo_ref, load.at[8 + n])

        def load_chunk(layer, chunk, slot):
            for k in range(2):
                cols = pl.ds(pl.multiple_of(k * f + chunk * cut, cut), cut)
                yield pltpu.make_async_copy(wgu_hbm.at[layer, :, cols], wgu_s.at[slot, :, k * cut : (k + 1) * cut], load.at[3 + n + slot])
            yield pltpu.make_async_copy(wd_hbm.at[layer, pl.ds(pl.multiple_of(chunk * cut, cut), cut), :], wd_s.at[slot], load.at[5 + n + slot])

        def load_tile(layer, number):
            for k, (src, dst) in enumerate(((h_hbm, h_s), (o_hbm, o_s))):
                yield pltpu.make_async_copy(src.at[layer, tile_at(number)], dst.at[tile_at(number)], come.at[k, number])

        load_qkv = lambda: pltpu.make_async_copy(qkv_ref.at[layer], qkv_s.at[:, : 3 * width], load.at[0])

        def at(number, more=True):
            return pl.when((phase == number) & more)

        @pl.when(step == 0)
        def _():
            load_wo().start()
            for number in reversed(range(n)):
                for c in (*load_tile(layer, number), load_dy(number)):
                    c.start()
            for c in (*load_chunk(layer, 0, 0), *load_late()):
                c.start()
            greet(Place(side).others())
            by_s[...] = jnp.zeros((t, d), F32)
            load_wo().wait()

        @pl.when(step == 1)
        def _():
            pl.semaphore_wait(pltpu.get_barrier_semaphore(), group - 1)

        at(last)(lambda: load_qkv().start())

        @at(0)
        def _():
            def tile(k, _):
                number = n - 1 - k
                here = tile_at(number)
                for c in load_tile(layer, number):
                    c.wait()
                pl.when(top)(lambda: load_dy(number).wait())
                h1 = h_s[here, :] + dot(o_s[here, :], wo_ref[layer]).astype(BF16)
                h1_s[here, :] = h1
                wide = h1.astype(F32)
                b = (wide * scale_of(wide)).astype(BF16)
                b_s[here, :] = b
                bt_s[:, here] = b.T
                gt_s[:, here] = g_s[here, :].T

            lax.fori_loop(0, n, tile, None)

        chunk = phase - 1
        hidden_units = (phase > 0) & (phase < last)

        @pl.when(hidden_units)
        def _():
            turn = lax.rem(chunk, 2)
            arrive(wgu_s.at[turn], load.at[3 + n + turn])
            arrive(wd_s.at[turn], load.at[5 + n + turn])

            @pl.when((chunk < side - 1) | (layer > 0))
            def _():
                end = chunk == side - 1
                for c in load_chunk(jnp.where(end, layer - 1, layer), jnp.where(end, 0, chunk + 1), 1 - turn):
                    c.start()

            wg, wu, wd = wgu_s.at[turn, :, :cut], wgu_s.at[turn, :, cut:], wd_s.at[turn]

            def tile(number, _):
                here = tile_at(number)
                b, g = b_s[here, :], g_s[here, :]
                sub = HEAD
                for c in range(0, cut, sub):
                    cols = slice(c, c + sub)
                    gate, up = dot(b, wg[:, cols]), dot(b, wu[:, cols])
                    dact = dot(g, wd[cols, :], 1, 1)
                    sig = jax.nn.sigmoid(gate)
                    silu = gate * sig
                    act_s[here, 2 * cut + c : 2 * cut + c + sub] = (silu * up).astype(BF16)
                    dgu_s[here, cols] = (dact * up * (sig + silu * (1 - sig))).astype(BF16)
                    dgu_s[here, cut + c : cut + c + sub] = (dact * silu).astype(BF16)
                by_s[here, :] += dot(dgu_s[here, :cut], wg[...], 1, 1) + dot(dgu_s[here, cut : 2 * cut], wu[...], 1, 1)

            lax.fori_loop(0, n, tile, None, unroll=2)

        do_s, kt_s, yt_s, dk_s, dq_s = h1_s, bt_s, gt_s, by_s, sum_s

        @at(last)
        def _():
            def tile(number, _):
                here = tile_at(number)
                h1 = h1_s[here, :].astype(F32)
                r = scale_of(h1)
                dh1 = (g_s[here, :].astype(F32) + normed_bwd(h1 * r, r, by_s[here, :])).astype(BF16)
                g_s[here, :] = dh1
                dk_s[here, :] = jnp.zeros((ROWS, width), F32)
                do_s[here, :] = dot(dh1, wo_ref[layer], 1, 1).astype(BF16)
                sum_s[...] = jnp.where(number == 0, 0.0, sum_s[...]) + dot(o_s[here, :].T, dh1)

            lax.fori_loop(0, n, tile, None)
            wo_o[...] = sum_s[...].astype(BF16).reshape(o_shape)

        heads = [slice(m * HEAD, (m + 1) * HEAD) for m in range(nh)]

        @at(last + 1)
        def _():
            load_qkv().wait()

            @pl.when(top)
            def _():
                for c in load_late():
                    c.wait()

            for j in range(0, t, ROWS):
                for h in heads:
                    kt_s[h, j : j + ROWS] = qkv_s[j : j + ROWS, width + h.start : width + h.stop].T

        @pl.when(phase > last)
        def _():
            i = per - 1 - phase
            here = tile_at(i)
            qs = [qkv_s[here, h] for h in heads]
            dos = [do_s[here, h] for h in heads]
            deltas = []
            for m, h in enumerate(heads):
                delta = (dos[m].astype(F32) * o_s[here, h].astype(F32)).sum(-1, keepdims=True)
                deltas.append(jnp.broadcast_to(delta, (ROWS, 128)).T[:1, :])
            lses = [lse_ref[layer, m : m + 1, here] for m in range(nh)]

            def block(keys, start, hide, first):
                span = slice(start, ROWS)
                scores = [dot(qkv_s[keys, width + h.start : width + h.stop], q[span, :], 1, 1) for h, q in zip(heads, qs)]
                dps = [dot(qkv_s[keys, 2 * width + h.start : 2 * width + h.stop], g[span, :], 1, 1) for h, g in zip(heads, dos)]
                for m, h in enumerate(heads):
                    p = jnp.exp2(scores[m] * LOG2E - lses[m][:, span])
                    if hide is not None:
                        p = jnp.where(hide, 0.0, p)
                    ds = (p * (dps[m] - deltas[m][:, span])).astype(BF16)
                    dv_s[keys, h] += dot(p.astype(BF16), dos[m][span, :])
                    dk_s[keys, h] += dot(ds, qs[m][span, :])
                    dq = dot(kt_s[h, keys], ds)
                    dq_s[h, span] = dq if first else dq_s[h, span] + dq

            wide = h_s[here, :].astype(F32)
            yt_s[:, here] = (wide * scale_of(wide)).astype(BF16).T
            half = ROWS // 2
            hide = hidden(ROWS)
            block(pl.ds(pl.multiple_of(i * ROWS, ROWS), half), 0, hide[:half, :], True)
            block(pl.ds(pl.multiple_of(i * ROWS + half, half), half), half, hide[:half, :half], False)
            lax.fori_loop(0, i, lambda j, _: block(tile_at(j), 0, None, False), None)
            cos, sin = angles(tab_ref, i)
            for h in heads:
                qkv_s[here, h] = rotated((dq_s[h, :] * HEAD**-0.5).astype(BF16).T.astype(F32), cos, -sin).astype(BF16)
                qkv_s[here, width + h.start : width + h.stop] = rotated(dk_s[here, h], cos, -sin).astype(BF16)
                qkv_s[here, 2 * width + h.start : 2 * width + h.stop] = dv_s[here, h].astype(BF16)

            @pl.when(top)
            def _():
                by = dot(qkv_s[here, : 3 * width], wqkv_s[...], 1, 1)
                wide = h_s[here, :].astype(F32)
                r = scale_of(wide)
                y = wide * r
                g_s[here, :] = (g_s[here, :].astype(F32) + normed_bwd(y, r, by)).astype(BF16)

            @pl.when(layer > 0)
            def _():
                for c in load_tile(layer - 1, i):
                    c.start()

        def qkvs(stage, of, which=(0, 1, 2)):
            for k in which:
                q_task.run(stage, Place(side), wqkv_o.at[k], gq_ref.at[of, :, k * width : (k + 1) * width], [r.at[k] for r in q_m])


        def both(chunk, stage):
            slot, source = lax.rem(chunk, SLOTS), lax.rem(chunk, 2)
            d_task.run(stage, Place(side), chunk, d_o.at[source], gd_ref.at[layer], [r.at[slot] for r in d_m])
            gu_task.run(stage, Place(side), gu_o.at[source], ggu_ref.at[layer, chunk], [r.at[slot] for r in gu_m])

        def out(stage):
            o_task.run(stage, Place(side), wo_o, go_ref.at[layer], o_m)

        when = [[], [c + 2 for c in range(side)], [c + 3 for c in range(side)], [c + 4 for c in range(side - 1)]]
        when[1][-1] = last + 1
        when[2][-2:] = last, last + 2
        when[3][-2:] = last, last + 1

        for stage in (2, 3, 1):

            @pl.when(functools.reduce(jnp.logical_or, [phase == p for p in when[stage]]))
            def _():
                both(sum(jnp.where(phase == p, c, 0) for c, p in enumerate(when[stage])), stage)

        for stage in range(3):
            at(last + stage)(lambda: out(stage))
        for stage in range(1, 4):
            at(stage, ~top)(lambda: qkvs(stage, layer + 1))

        @pl.when(hidden_units)
        def _():
            slot = lax.rem(chunk, 2)
            dv_s[tile_at(chunk, t // side), :] = jnp.zeros((t // side, width), F32)
            for c in range(0, 2 * cut, cut):
                gu_o[slot, :, :, :, c : c + cut] = dot(bt_s[...], dgu_s[:, c : c + cut]).astype(BF16).reshape(*gu_shape[:3], cut)
            d_o[slot] = dot(gt_s[...], act_s[:, 2 * cut : 3 * cut]).astype(BF16).T.reshape(d_shape)
            both(chunk, 0)

        @at(per - 1)
        def _():
            for k in range(3):
                wqkv_o[k] = dot(yt_s[...], qkv_s[:, k * width : (k + 1) * width]).astype(BF16).reshape(q_shape)
                qkvs(0, layer, (k,))
                rows = slice(t * k // 3 // 8 * 8, t * (k + 1) // 3 // 8 * 8)
                by_s[rows, :] = jnp.zeros((rows.stop - rows.start, d), F32)
            both(side - 1, 3)
            out(3)

        @pl.when(step == layers * per - 1)
        def _():
            place = Place(side)
            mine = sum(square(gq_ref[k]) for k in range(1, layers))
            for k in range(layers):
                mine += square(go_ref[k]) + square(gd_ref[k])
                for c in range(side):
                    mine += square(ggu_ref[k, c])
            qkvs(1, 0)
            qkvs(2, 0)
            qkvs(3, 0)
            mine = jnp.broadcast_to(mine + square(gq_ref[0]), part.shape)
            part[...] = mine
            slots[place.me] = mine
            for device in place.others():
                remote(part, slots.at[place.me], send.at[0], recv.at[0], device).start()
            arrived(slots.at[: group - 1], send.at[0], recv.at[0], place.others()[0])
            total_ref[...] = slots[...].sum(0)

    outs = [sds((layers, q_shape[2], 3 * width), BF16), sds((layers, o_shape[2], d), BF16), sds((layers, side, *gu_shape[2:]), BF16),
            sds((layers, *d_shape[1:]), BF16), sds((8, 128), F32)]
    return pl.pallas_call(
        body,
        grid=(layers * per,),
        in_specs=[ANY] * 10,
        out_specs=[whole(a.shape) for a in outs],
        out_shape=outs,
        scratch_shapes=[*own, *moves],
        compiler_params=pltpu.CompilerParams(dimension_semantics=("arbitrary",), vmem_limit_bytes=VMEM, has_side_effects=True, collective_id=cid),
        name="backward",
    )(h, o, lse, wo, wqkv, wgu, wd, dy, qkv, tab)


def adamw(total, count, weights, m, v, gq, go, ggu, gd):
    layers, side = ggu.shape[:2]

    def body(total_ref, gq_ref, go_ref, ggu_ref, gd_ref, *refs):
        w_refs, m_refs, v_refs, wn_refs, mn_refs, vn_refs = taken(refs, *[7] * 6)
        factor = jnp.minimum(1.0, 0.5 * lax.rsqrt(total_ref[0:1, 0:1] / count + 1e-30))

        def update(i, columns, g):
            g = g.astype(F32) * factor
            at = (0, slice(None), columns)
            mn = 0.9 * m_refs[i][at] + 0.1 * g
            vn = 0.95 * v_refs[i][at] + 0.05 * g * g
            mn_refs[i][at], vn_refs[i][at] = mn, vn
            w = w_refs[i][at].astype(F32)
            wn_refs[i][at] = (w - 0.02 * (mn * lax.rsqrt(vn + 1e-8) + 0.1 * w)).astype(BF16)

        every = slice(None)
        wide = gq_ref.shape[2] // 3
        for i in range(3):
            update(i, every, gq_ref[0, :, i * wide : (i + 1) * wide])
        update(3, every, go_ref[0])
        cut = ggu_ref.shape[3] // 2
        for c in range(side):
            for i in range(2):
                update(4 + i, slice(c * cut, (c + 1) * cut), ggu_ref[0, c, :, i * cut : (i + 1) * cut])
        update(6, every, gd_ref[0])

    one = lambda a: pl.BlockSpec((1, *a.shape[1:]), lambda l: (l,) + (0,) * (a.ndim - 1))
    own = [one(a) for a in weights]
    return pl.pallas_call(
        body,
        grid=(layers,),
        in_specs=[whole(total.shape), *(one(a) for a in (gq, go, ggu, gd)), *own * 3],
        out_specs=own * 3,
        out_shape=[*(sds(a.shape, BF16) for a in weights), *(sds(a.shape, F32) for a in (*m, *v))],
        compiler_params=pltpu.CompilerParams(dimension_semantics=("arbitrary",), vmem_limit_bytes=VMEM),
        name="adamw",
    )(total, gq, go, ggu, gd, *weights, *m, *v)


def solution(mesh):
    group = mesh.shape["dp"]
    side = side_of(group)

    def step(x, dy, *arrays):
        weights, m, v = (arrays[i : i + 7] for i in (0, 7, 14))
        x, dy = x[0], dy[0]
        qkv, o, lse, h, wqkv, wo, wgu, wd = forward(0, side, x, weights)
        *grads, total = backward(1, side, h, dy, qkv, o, lse, wqkv, wo, wgu, wd)
        return tuple(adamw(total, group * sum(w.size for w in weights), weights, m, v, *grads))

    states, cut = P(("rep", "dp"), None, None), P(None, "dp", None)
    return jax.shard_map(
        step,
        mesh=mesh,
        in_specs=(states, states) + (cut,) * 21,
        out_specs=(P("rep", "dp", None),) * 21,
        check_vma=False,
    )
```

```python
import functools

import jax
import jax.numpy as jnp
import numpy as np
from jax import lax
from jax.experimental import pallas as pl
from jax.experimental.pallas import tpu as pltpu
from jax.sharding import PartitionSpec as P

HEAD = 256
THETA = 10000
LOG2E = 1.4426950408889634
VMEM = 67_000_000
EPS = 1e-6
F32, BF16 = jnp.float32, jnp.bfloat16
MESH = pl.DeviceIdType.MESH
ANY = pl.BlockSpec(memory_space=pl.ANY)
ROWS = 512
STRIP = 256
SLOTS = 3
sds = jax.ShapeDtypeStruct


def dot(a, b, ca=1, cb=0):
    return lax.dot_general(a, b, (((ca,), (cb,)), ((), ())), preferred_element_type=F32)


def scale_of(h):
    return lax.rsqrt(jnp.mean(h * h, -1, keepdims=True) + EPS)


def normed_bwd(y, r, by):
    return r * (by - y * jnp.mean(by * y, -1, keepdims=True))


def table(tokens):
    half = HEAD // 2
    rate = np.float32(THETA) ** (-np.arange(half, dtype=np.float32) / np.float32(half))
    places = [np.arange(0, ROWS), np.arange(0, tokens, ROWS)]
    return jnp.asarray(np.concatenate([f(p[:, None] * rate.astype(np.float64)) for p in places for f in (np.cos, np.sin)]), F32)


def angles(ref, tile):
    n = ref.shape[0] // 2 - ROWS
    near_c, near_s = ref[:ROWS, :], ref[ROWS : 2 * ROWS, :]
    c, s = ref[pl.ds(2 * ROWS + tile, 1), :], ref[pl.ds(2 * ROWS + n + tile, 1), :]
    return c * near_c - s * near_s, s * near_c + c * near_s


def rotated(t, cos, sin):
    half = t.shape[-1] // 2
    a, b = t[:, :half], t[:, half:]
    return jnp.concatenate([a * cos - b * sin, b * cos + a * sin], -1)


def hidden(size):
    return lax.broadcasted_iota(jnp.int32, (size, size), 0) > lax.broadcasted_iota(jnp.int32, (size, size), 1)


def tile_at(n, size=ROWS):
    return pl.ds(pl.multiple_of(n * size, size), size)


def whole(shape):
    return pl.BlockSpec(shape, lambda *_: (0,) * len(shape), pipeline_mode=pl.Buffered(1))


def side_of(group):
    return int(round(group**0.5))


class Place:
    def __init__(self, side):
        rep, me = lax.axis_index("rep"), lax.axis_index("dp")
        self.side, self.me, self.x, self.y, self.core = side, me, lax.div(me, side), lax.rem(me, side), lax.rem(rep, 2)
        self.partner = {"rep": rep + 1 - 2 * self.core}

    def on(self, axis, k):
        at = lax.rem((self.x, self.y)[axis] + k, self.side)
        return at, {"dp": at * self.side + self.y if axis == 0 else self.x * self.side + at}

    def line(self):
        return [self.on(axis, k)[1] for axis in (0, 1) for k in range(1, self.side)]

    def others(self):
        n = self.side**2
        return [{"dp": lax.rem(self.me + k, n)} for k in range(1, n)]


def greet(devices):
    for device in devices:
        pl.semaphore_signal(pltpu.get_barrier_semaphore(), inc=1, device_id=device, device_id_type=MESH)


def remote(src, dst, send, recv, device):
    return pltpu.make_async_remote_copy(src_ref=src, dst_ref=dst, send_sem=send, recv_sem=recv, device_id=device, device_id_type=MESH)


def arrive(ref, sem):
    pltpu.make_async_copy(ref, ref, sem).wait()


def arrived(ref, send, recv, device):
    c = remote(ref, ref, recv if send is None else send, send if recv is None else recv, device)
    if recv is not None:
        c.wait_recv()
    if send is not None:
        c.wait_send()


class Gather:
    def __init__(self, side, rows, widths, by_rows, relayed):
        self.side, self.widths, self.by_rows, self.relayed = side, widths, by_rows, relayed
        n = side - 1
        self.shape = (side, side, rows, sum(widths))
        self.matrix = pltpu.VMEM(self.shape, BF16)
        self.sems = [pltpu.SemaphoreType.DMA((k,)) for k in (len(widths) + 2, 2, 2, 2 * n, 2, 2)]

    def run(self, stage, place, layer, shards, result, out, sems):
        local, send, come, across, near, far = sems
        n = self.side - 1
        copies, column = [], 0
        for k, (shard, width) in enumerate(zip(shards, self.widths, strict=True)):
            copies.append((shard.at[layer], out.at[place.x, place.y, :, column : column + width], local.at[k]))
            column += width
        size = out.shape[2] if self.by_rows else out.shape[3]
        every = slice(None)

        def copied(own):
            core = place.core if own else 1 - place.core
            piece = pl.ds(pl.multiple_of(core * (size // 2), size // 2), size // 2)
            at = (every, every, piece, every) if self.by_rows else (every, every, every, piece)
            return pltpu.make_async_copy(out.at[at], result.at[(layer, *at)], local.at[len(shards) + own])

        if stage == 0:
            for c in copies:
                pltpu.make_async_copy(*c).start()
        elif stage == 1:
            for c in copies:
                pltpu.make_async_copy(*c).wait()
        elif stage == 6:
            copied(0).wait()
            copied(1).wait()
            arrived(out.at[0, :n], send.at[0], None, place.partner)
            arrived(out.at[:n], send.at[1], None, place.partner)
        for q, waits in [(0, True), (1, True)] * (stage == 2) + [(0, False), (1, False)]:

            def view(at, core=place.core):
                piece = pl.ds(pl.multiple_of(core * (size // 2) + q * (size // 4), size // 4), size // 4)
                return out.at[at[0], at[1], piece, :] if self.by_rows else out.at[at[0], at[1], :, piece]

            along = lambda at: (at, place.y) if q == 0 else (place.x, at)
            over = lambda at: (every, at) if q == 0 else (at, every)
            here, line = view((place.x, place.y)), view(over(place.y if q == 0 else place.x))
            if stage == 1:
                for k in range(1, n + 1):
                    remote(here, here, send.at[0], come.at[q], place.on(q, k)[1]).start()
            elif waits:
                arrived(view((0, slice(0, n))), None, come.at[q], place.partner)
            elif stage == 2:
                for k in (1, n) if self.relayed else range(1, n + 1):
                    remote(line, line, send.at[1], across.at[q * n + k - 1], place.on(1 - q, k)[1]).start()
                for k in range(1, n + 1):
                    got = view(along(place.on(q, k)[0]))
                    remote(got, got, send.at[0], near.at[q], place.partner).start()
            elif stage in (3, 4):
                for k in ((1, n) if stage == 3 else (2,)) if self.relayed else range(1, n + 1) if stage == 3 else ():
                    at = place.on(1 - q, self.side - k)[0]
                    got = view(over(at))
                    arrived(got, None, across.at[q * n + k - 1], place.partner)
                    if self.relayed and stage == 3:
                        half = slice(0, self.side // 2) if k == 1 else slice(self.side // 2, self.side)
                        part = view((half, at) if q == 0 else (at, half))
                        remote(part, part, send.at[1], across.at[q * n + 1], place.on(1 - q, k)[1]).start()
                    remote(got, got, send.at[1], far.at[q], place.partner).start()
            elif stage == 5:
                arrived(view((0, slice(0, n))), None, near.at[q], place.partner)
                arrived(view((slice(0, n), every)), None, far.at[q], place.partner)
        if stage == (4 if self.relayed else 5):
            copied(1).start()
        if stage == 5:
            copied(0).start()


class Ring:
    def __init__(self, half):
        self.scratch = [pltpu.VMEM((2, *half), BF16), pltpu.VMEM((2, *half), BF16), pltpu.VMEM((2, 2, *half), BF16), pltpu.SemaphoreType.DMA((2,)),
                        pltpu.SemaphoreType.DMA((2,))]

    def start(self, place, axis, blocks, scratch, last=False):
        far, mid, near, send, recv = scratch
        opposite, _ = place.on(axis, 2)
        for relayed in (True, False):
            for d, k in enumerate((1, place.side - 1)):
                there, to = place.on(axis, k)
                if last:
                    if relayed:
                        remote(mid.at[d], near.at[d, d], send.at[1], recv.at[1], to).start()
                elif relayed:
                    remote(blocks(opposite, d), far.at[d], send.at[0], recv.at[0], to).start()
                else:
                    remote(blocks(there, 1 - d), near.at[d, 1 - d], send.at[1], recv.at[1], to).start()

    def middle(self, place, axis, blocks, scratch):
        far, mid, near, send, recv = scratch
        arrived(far, send.at[0], recv.at[0], place.on(axis, 1)[1])
        for d, k in enumerate((1, place.side - 1)):
            there, _ = place.on(axis, k)
            mid[d] = (blocks(there, d)[...].astype(F32) + far[d].astype(F32)).astype(BF16)
        self.start(place, axis, blocks, scratch, True)

    def end(self, place, axis, blocks, scratch):
        far, mid, near, send, recv = scratch
        arrived(near, send.at[1], recv.at[1], place.on(axis, 1)[1])

    def total(self, blocks, scratch, at, cut):
        near = scratch[2]
        return blocks(at, cut)[...].astype(F32) + near[0, cut].astype(F32) + near[1, cut].astype(F32)


class Crossed:
    def __init__(self, side, rows, width):
        self.side, self.width = side, width
        n, half = side - 1, width // 2
        self.ring = Ring((side // 2, rows, half))
        self.scratch = [*self.ring.scratch * 2, pltpu.VMEM((2, side, rows, half), BF16), pltpu.VMEM((2, n, rows, half), BF16),
                        pltpu.VMEM((2, rows, half), F32), pltpu.SemaphoreType.DMA((1,)), pltpu.SemaphoreType.DMA((1,))]

    def run(self, stage, place, src, out, scratch):
        *rings, (mid, two, own, send, recv) = taken(scratch, 5, 5, 5)
        n, half, cut = self.side - 1, self.width // 2, self.side // 2
        along = (lambda j, h: src.at[j, h * cut : (h + 1) * cut, :, :half]), (lambda j, h: src.at[h * cut : (h + 1) * cut, j, :, half:])
        for q in range(2):
            at = (place, q, along[q], rings[q])
            if stage == 0:
                self.ring.start(*at)
            elif stage == 1:
                self.ring.middle(*at)
            elif stage == 2:
                self.ring.end(*at)
                for h in range(2):
                    mid[q, h * cut : (h + 1) * cut] = self.ring.total(along[q], rings[q], (place.x, place.y)[q], h).astype(BF16)
                j = (place.y, place.x)[q]
                mine = (src[place.x, place.y, :, :half] if q == 0 else src[place.x, place.y, :, half:]).astype(F32)
                own[q] = mine + sum(rings[q][2][d, lax.div(j, cut), lax.rem(j, cut)].astype(F32) for d in range(2))
        if stage == 2:
            for q in range(2):
                for k in range(n):
                    there, to = place.on(1 - q, k + 1)
                    remote(mid.at[q, there], two.at[q, k], send.at[0], recv.at[0], to).start()
        elif stage == 3:
            arrived(two, send.at[0], recv.at[0], place.on(0, 1)[1])
            for q in range(2):
                t = own[q]
                for k in range(n):
                    t += two[q, k].astype(F32)
                out[:, q * half : (q + 1) * half] = t.astype(BF16)


class Lined:
    def __init__(self, side, rows, width):
        self.side, self.rows = side, rows
        n = side - 1
        self.ring = Ring((rows // 2, width))
        self.scratch = [*self.ring.scratch, pltpu.VMEM((rows, width), BF16), pltpu.VMEM((n, rows, width), BF16),
                        pltpu.VMEM((rows, width), F32), pltpu.SemaphoreType.DMA((1,)), pltpu.SemaphoreType.DMA((1,))]

    def run(self, stage, place, line, src, out, scratch):
        ring, (mid, two, own, send, recv) = taken(scratch, 5, 5)
        n, cut = self.side - 1, self.rows // 2
        ahead = lax.rem(line - place.x + self.side, self.side)
        at = (place, 1, lambda j, h: src.at[j, h * cut : (h + 1) * cut, :], ring)

        def second():
            return remote(mid, two.at[ahead - 1], send.at[0], recv.at[0], place.on(0, ahead)[1])

        if stage == 0:
            self.ring.start(*at)
        elif stage == 1:
            self.ring.middle(*at)
        elif stage == 2:
            self.ring.end(*at)
            for h in range(2):
                t = self.ring.total(at[2], ring, place.y, h)
                own[h * cut : (h + 1) * cut, :] = t
                mid[h * cut : (h + 1) * cut, :] = t.astype(BF16)
            pl.when(ahead != 0)(lambda: second().start())
        else:
            pl.when(ahead != 0)(lambda: second().wait_send())

            @pl.when(ahead == 0)
            def _():
                arrived(two, None, recv.at[0], place.on(0, 1)[1])
                t = own[...]
                for k in range(n):
                    t += two[k].astype(F32)
                out[...] = t.astype(BF16)


def taken(refs, *counts):
    out, at = [], 0
    for n in counts:
        out.append(refs[at : at + n])
        at += n
    return out


def forward(cid, side, x, weights):
    t, d = x.shape
    layers, width = weights[0].shape[0], weights[0].shape[2]
    f = weights[4].shape[2]
    nh, n = width // HEAD, t // ROWS
    shard = d // side**2
    tasks = [Gather(side, shard, [width] * 3, False, False), Gather(side, shard, [f, f, d], False, True), Gather(side, f // side**2, [d], True, True)]
    kinds = len(tasks)
    flat = [pltpu.VMEM((layers, *tasks[0].shape), BF16), *(task.matrix for _ in range(layers) for task in tasks[1:])]
    sems = [s for layer in range(layers) for task in (tasks[1:] if layer else tasks) for s in task.sems]
    own = [pltpu.VMEM((t, width), BF16), pltpu.VMEM((nh, HEAD + 8, t), BF16), pltpu.VMEM((nh, ROWS), F32), pltpu.VMEM((nh, HEAD + 8, ROWS), F32),
           pltpu.VMEM((t, width), BF16), pltpu.VMEM((t, d), BF16), pltpu.VMEM((ROWS, f), BF16), pltpu.VMEM((nh * ROWS // STRIP, ROWS, STRIP), F32),
           pltpu.VMEM((nh, ROWS), F32), pltpu.VMEM((t, d), BF16), pltpu.VMEM((2 * (ROWS + n), HEAD // 2), F32), pltpu.SemaphoreType.DMA((n + 1,))]
    tab = table(t)

    def body(*refs):
        (x_hbm, tab_hbm), shards, outs, scratch, moved = taken(refs, 2, 7, 4 + kinds, len(own), len(flat) + len(sems))
        qkv_ref, o_ref, lse_ref, h_ref, *wholes = outs
        k_s, vt_s, top_s, mix_s, o_s, h2_s, act_s, s_s, keep_s, x_s, tab_ref, load = scratch
        w_s = moved[0]
        matrices = [[w_s.at[layer], *m] for layer, m in enumerate(taken(moved[1:], *[kinds - 1] * layers))]
        flags = taken(moved[len(flat) :], *[6] * (layers * (kinds - 1) + 1))
        parts = [shards[:3], [*shards[4:6], shards[3]], shards[6:]]
        step = pl.program_id(0)

        def go(layer, which, *stages):
            for stage in stages:
                for kind in which:
                    tasks[kind].run(stage, Place(side), layer, parts[kind], wholes[kind], matrices[layer][kind], flags[kind + (kinds - 1) * layer * (kind > 0)])

        def at(number):
            return pl.when(step == number)

        attention, ffn = (0,), (1, 2)
        load_x = lambda number: pltpu.make_async_copy(x_hbm.at[tile_at(number)], x_s.at[tile_at(number)], load.at[number])
        load_tab = lambda: pltpu.make_async_copy(tab_hbm, tab_ref, load.at[n])

        @at(0)
        def _():
            place = Place(side)
            peers = [*place.line(), place.partner]
            greet(peers)
            go(0, attention + ffn, 0)
            for number in range(n):
                load_x(number).start()
            load_tab().start()
            for m in range(nh):
                vt_s[m, HEAD:, :] = jnp.ones((8, t), BF16)
            pl.semaphore_wait(pltpu.get_barrier_semaphore(), len(peers))
            go(0, attention, 1)
            go(0, ffn, 1)
            go(0, attention, 2, 3)
            go(0, ffn, 2)
            go(0, attention, 5)
            load_tab().wait()

        @pl.when(step < n)
        def _():
            load_x(step).wait()
            h_ref[0] = x_s[tile_at(step), :]

        @at(n)
        def _():
            go(0, ffn, 4, 5)

        def matrix(layer, kind):
            return matrices[layer][kind]

        second = step >= 2 * n

        @pl.when((step < n) | second)
        def _():
            i = lax.rem(step, n)
            here = tile_at(i)
            layer = lax.div(step, 2 * n)

            h = jnp.where(second, h2_s[here, :], x_s[here, :])
            h = h.astype(F32)
            a = (h * scale_of(h)).astype(BF16)
            heads = [slice(m * HEAD, (m + 1) * HEAD) for m in range(nh)]
            raw = [[dot(a, w_s[layer, :, :, :, k * width + at.start : k * width + at.stop].reshape(d, HEAD)).astype(BF16) for k in range(3)] for at in heads]
            cos, sin = angles(tab_ref, i)
            pieces = [(m, slice(c, c + STRIP)) for m in range(nh) for c in range(0, ROWS, STRIP)]
            qs = []
            for m, at in enumerate(heads):
                q = rotated(raw[m][0].astype(F32), cos, sin).astype(BF16) * jnp.asarray(HEAD**-0.5, BF16)
                k = rotated(raw[m][1].astype(F32), cos, sin).astype(BF16)
                qkv_ref[0, :, at], qkv_ref[0, :, width + at.start : width + at.stop] = q, k
                qkv_ref[0, :, 2 * width + at.start : 2 * width + at.stop] = raw[m][2]
                vt_s[m, :HEAD, here] = raw[m][2].T
                k_s[here, at] = k
                qs.append(q)
                for p, (head, cols) in enumerate(pieces):
                    if head == m:
                        s = jnp.where(hidden(ROWS)[:, cols], -1e30, dot(k, q[cols, :], 1, 1))
                        s_s[p] = s
                        top_s[m : m + 1, cols] = s.max(0, keepdims=True)

            def scores(k, j):
                m, cols = pieces[k]
                return dot(k_s[tile_at(j), m * HEAD : (m + 1) * HEAD], qs[m][cols, :], 1, 1)

            def weights(k, top):
                return jnp.exp2((s_s[k] - top) * LOG2E).astype(BF16)

            def add(k, j, p, diagonal):
                m, cols = pieces[k]
                old = jnp.where(diagonal, 0.0, mix_s[m, :, cols] * keep_s[m : m + 1, cols])
                mix_s[m, :, cols] = old + dot(vt_s[m, :, tile_at(j)], p)

            def turn(j, _):
                before = jnp.where(j == 0, i, j - 1)
                late = None
                for k, (m, cols) in enumerate(pieces):
                    s = scores(k, j)
                    top = top_s[m : m + 1, cols]
                    p = weights(k, top)
                    s_s[k] = s
                    new = jnp.maximum(top, s.max(0, keepdims=True))
                    if late:
                        add(*late)
                        keep_s[pieces[k - 1][0] : pieces[k - 1][0] + 1, pieces[k - 1][1]] = keep
                    top_s[m : m + 1, cols] = new
                    keep = jnp.exp2((top - new) * LOG2E)
                    late = k, before, p, j == 0
                add(*late)
                keep_s[m : m + 1, cols] = keep

            pl.when(step == 3 * n - 1)(lambda: go(1, ffn, 5))
            lax.fori_loop(0, i, turn, None)
            end = jnp.where(i == 0, i, i - 1)

            def out(m):
                at = heads[m]
                total = mix_s[m, HEAD : HEAD + 1, :]
                o = (mix_s[m, :HEAD, :] * (1 / total)).astype(BF16).T
                o_ref[0, :, at] = o
                o_s[here, at] = o
                lse_ref[0, m : m + 1, :] = top_s[m : m + 1, :] * LOG2E + jnp.log2(total)

            late = None
            for k, (m, cols) in enumerate(pieces):
                p = weights(k, top_s[m : m + 1, cols])
                if late:
                    add(*late)
                    if pieces[k - 1][0] != m:
                        out(m - 1)
                late = k, end, p, i == 0
            add(*late)
            out(nh - 1)

        @pl.when((step >= n) & ~second)
        def _():
            here = tile_at(step - n)
            wgu, wd = (matrix(0, kind) for kind in ffn)
            h1 = x_s[here, :] + dot(o_s[here, :], wgu[:, :, :, 2 * f :].reshape(width, d)).astype(BF16)
            wide = h1.astype(F32)
            b = (wide * scale_of(wide)).astype(BF16)
            cut = f // side
            for c in range(0, f, cut):
                gate = dot(b, wgu[:, :, :, c : c + cut].reshape(d, cut))
                up = dot(b, wgu[:, :, :, f + c : f + c + cut].reshape(d, cut))
                act_s[:, c : c + cut] = (gate * jax.nn.sigmoid(gate) * up).astype(BF16)
            h2 = h1 + dot(act_s[...], wd[...].reshape(f, d)).astype(BF16)
            h_ref[0] = h2
            h2_s[here, :] = h2

        plan = {0: [(0, attention, 6), (1, attention + ffn, 0)], n - 2: [(0, ffn, 3), (1, attention + ffn, 1)],
                n: [(1, attention + ffn, 2)], n + 2: [(1, attention, 3)], 2 * n - 1: [(1, attention, 5)], 2 * n: [(1, ffn, 3)],
                3 * n - 2: [(1, ffn, 4)], 3 * n - 1: [(0, ffn, 6), (1, attention + ffn, 6)]}
        for number, todo in plan.items():

            @at(number)
            def _():
                for what in todo:
                    go(*what)

    tile = lambda s: jnp.where(s < 2 * n, jnp.minimum(s, n - 1), s - 2 * n)
    by_layer = lambda w: pl.BlockSpec((1, ROWS, w), lambda s: (s // (2 * n), tile(s), 0))
    got = pl.pallas_call(
        body,
        grid=(3 * n,),
        in_specs=[ANY] * 9,
        out_specs=[by_layer(3 * width), by_layer(width), pl.BlockSpec((1, nh, ROWS), lambda s: (s // (2 * n), 0, tile(s))),
                   pl.BlockSpec((1, ROWS, d), lambda s: (jnp.where(s < n, 0, 1), jnp.where(s < 2 * n, lax.rem(s, n), n - 1), 0)), *[ANY] * kinds],
        out_shape=[sds((layers, t, 3 * width), BF16), sds((layers, t, width), BF16), sds((layers, nh, t), F32), sds((layers, t, d), BF16),
                   *(sds((layers, *task.shape), BF16) for task in tasks)],
        scratch_shapes=[*own, *flat, *sems],
        compiler_params=pltpu.CompilerParams(dimension_semantics=("arbitrary",), vmem_limit_bytes=VMEM, has_side_effects=True, collective_id=cid),
        name="forward",
    )(x, tab, *weights)
    return [*got[:4], *(w.reshape(layers, -1, w.shape[-1]) for w in got[4:])]


def square(g):
    wide = g.astype(F32)
    return jnp.sum(jnp.sum(wide * wide, 0, keepdims=True), 1, keepdims=True)


def backward(cid, side, h, dy, qkv, o, lse, wqkv, wgu, wd):
    layers, t, d = h.shape
    width = o.shape[2]
    f = wd.shape[1]
    n, nh, cut, group = t // ROWS, width // HEAD, f // side, side * side
    per = 2 + side + n
    gu_shape, d_shape = (side, side, d // group, 2 * cut), (side, f // group, d)
    o_shape, q_shape = (side, side, width // group, d), (side, side, d // group, width)
    gu_task, d_task = Crossed(side, gu_shape[2], gu_shape[3]), Lined(side, d_shape[1], d)
    o_task, q_task = Crossed(side, o_shape[2], d), Crossed(side, q_shape[2], width)
    several = lambda task, n: [pltpu.VMEM((n, *s.shape), s.dtype) if s.memory_space == pltpu.VMEM else pltpu.SemaphoreType.DMA((n, *s.shape)) for s in task.scratch]
    moves = [*several(gu_task, SLOTS), *several(d_task, SLOTS), *o_task.scratch, *several(q_task, 3)]
    own = [pltpu.VMEM((t, d), BF16), pltpu.VMEM((d, t), BF16), pltpu.VMEM((t, d), BF16), pltpu.VMEM((d, t), BF16), pltpu.VMEM((t, d), F32),
           pltpu.VMEM((t, d), BF16), pltpu.VMEM((t, max(3 * cut, 3 * width)), BF16), pltpu.VMEM((2, *gu_shape), BF16),
           pltpu.VMEM((2, *d_shape), BF16), pltpu.VMEM((width, d), F32), pltpu.VMEM(o_shape, BF16), pltpu.VMEM((3, *q_shape), BF16),
           pltpu.VMEM((t, width), F32), pltpu.SemaphoreType.DMA((n + 9,)),
           pltpu.VMEM((group, 8, 128), F32), pltpu.VMEM((8, 128), F32), pltpu.SemaphoreType.DMA((1,)), pltpu.SemaphoreType.DMA((1,)),
           pltpu.VMEM((d, 3 * width), BF16), pltpu.VMEM((2 * (ROWS + n), HEAD // 2), F32), pltpu.VMEM((2, d, 2 * cut), BF16), pltpu.VMEM((2, cut, d), BF16),
           pltpu.VMEM((t, d), BF16), pltpu.VMEM((t, width), BF16), pltpu.SemaphoreType.DMA((2, n)),
           pltpu.VMEM(lse.shape, F32), pltpu.VMEM((layers, width, d), BF16)]
    tab = table(t)

    def body(*refs):
        ins, outs, scratch, moved = taken(refs, 9, 5, len(own), len(moves))
        h_hbm, o_hbm, lse_hbm, wqkv_hbm, wgu_hbm, wd_hbm, dy_ref, qkv_ref, tab_hbm = ins
        gq_ref, go_ref, ggu_ref, gd_ref, total_ref = outs
        (b_s, bt_s, g_s, gt_s, by_s, h1_s, wide_s, gu_o, d_o, sum_s, wo_o, wqkv_o, dv_s, load, slots, part, send, recv, wqkv_s, tab_ref, wgu_s, wd_s, h_s, o_s, come, lse_ref, wo_ref) = scratch
        dgu_s, act_s, qkv_s = wide_s, wide_s, wide_s
        gu_m, d_m, o_m, q_m = taken(moved, *(len(task.scratch) for task in (gu_task, d_task, o_task, q_task)))
        step = pl.program_id(0)
        layer = layers - 1 - lax.div(step, per)
        phase = lax.rem(step, per)
        top = layer == layers - 1
        last = side + 1
        load_dy = lambda number: pltpu.make_async_copy(dy_ref.at[tile_at(number)], g_s.at[tile_at(number)], load.at[1 + number])

        def load_late():
            return [pltpu.make_async_copy(*c, load.at[k])
                    for k, c in ((1 + n, (wqkv_hbm.at[layers - 1], wqkv_s)), (2 + n, (tab_hbm, tab_ref)), (7 + n, (lse_hbm, lse_ref)))]

        load_wo = lambda: pltpu.make_async_copy(wgu_hbm.at[:, :, 2 * f :], wo_ref, load.at[8 + n])

        def load_chunk(layer, chunk, slot):
            for k in range(2):
                cols = pl.ds(pl.multiple_of(k * f + chunk * cut, cut), cut)
                yield pltpu.make_async_copy(wgu_hbm.at[layer, :, cols], wgu_s.at[slot, :, k * cut : (k + 1) * cut], load.at[3 + n + slot])
            yield pltpu.make_async_copy(wd_hbm.at[layer, pl.ds(pl.multiple_of(chunk * cut, cut), cut), :], wd_s.at[slot], load.at[5 + n + slot])

        def load_tile(layer, number):
            for k, (src, dst) in enumerate(((h_hbm, h_s), (o_hbm, o_s))):
                yield pltpu.make_async_copy(src.at[layer, tile_at(number)], dst.at[tile_at(number)], come.at[k, number])

        load_qkv = lambda: pltpu.make_async_copy(qkv_ref.at[layer], qkv_s.at[:, : 3 * width], load.at[0])

        def at(number, more=True):
            return pl.when((phase == number) & more)

        @pl.when(step == 0)
        def _():
            load_wo().start()
            for number in reversed(range(n)):
                for c in (*load_tile(layer, number), load_dy(number)):
                    c.start()
            for c in (*load_chunk(layer, 0, 0), *load_late()):
                c.start()
            greet(Place(side).others())
            by_s[...] = jnp.zeros((t, d), F32)
            load_wo().wait()

        @pl.when(step == 1)
        def _():
            pl.semaphore_wait(pltpu.get_barrier_semaphore(), group - 1)

        at(last)(lambda: load_qkv().start())

        @at(0)
        def _():
            def tile(k, _):
                number = n - 1 - k
                here = tile_at(number)
                for c in load_tile(layer, number):
                    c.wait()
                pl.when(top)(lambda: load_dy(number).wait())
                h1 = h_s[here, :] + dot(o_s[here, :], wo_ref[layer]).astype(BF16)
                h1_s[here, :] = h1
                wide = h1.astype(F32)
                b = (wide * scale_of(wide)).astype(BF16)
                b_s[here, :] = b
                bt_s[:, here] = b.T
                gt_s[:, here] = g_s[here, :].T

            lax.fori_loop(0, n, tile, None)

        chunk = phase - 1
        hidden_units = (phase > 0) & (phase < last)

        @pl.when(hidden_units)
        def _():
            turn = lax.rem(chunk, 2)
            arrive(wgu_s.at[turn], load.at[3 + n + turn])
            arrive(wd_s.at[turn], load.at[5 + n + turn])

            @pl.when((chunk < side - 1) | (layer > 0))
            def _():
                end = chunk == side - 1
                for c in load_chunk(jnp.where(end, layer - 1, layer), jnp.where(end, 0, chunk + 1), 1 - turn):
                    c.start()

            wg, wu, wd = wgu_s.at[turn, :, :cut], wgu_s.at[turn, :, cut:], wd_s.at[turn]

            def tile(number, _):
                here = tile_at(number)
                b, g = b_s[here, :], g_s[here, :]
                sub = HEAD
                for c in range(0, cut, sub):
                    cols = slice(c, c + sub)
                    gate, up = dot(b, wg[:, cols]), dot(b, wu[:, cols])
                    dact = dot(g, wd[cols, :], 1, 1)
                    sig = jax.nn.sigmoid(gate)
                    silu = gate * sig
                    act_s[here, 2 * cut + c : 2 * cut + c + sub] = (silu * up).astype(BF16)
                    dgu_s[here, cols] = (dact * up * (sig + silu * (1 - sig))).astype(BF16)
                    dgu_s[here, cut + c : cut + c + sub] = (dact * silu).astype(BF16)
                by_s[here, :] += dot(dgu_s[here, :cut], wg[...], 1, 1) + dot(dgu_s[here, cut : 2 * cut], wu[...], 1, 1)

            lax.fori_loop(0, n, tile, None, unroll=2)

        do_s, kt_s, yt_s, dk_s, dq_s = h1_s, bt_s, gt_s, by_s, sum_s

        @at(last)
        def _():
            def tile(number, _):
                here = tile_at(number)
                h1 = h1_s[here, :].astype(F32)
                r = scale_of(h1)
                dh1 = (g_s[here, :].astype(F32) + normed_bwd(h1 * r, r, by_s[here, :])).astype(BF16)
                g_s[here, :] = dh1
                dk_s[here, :] = jnp.zeros((ROWS, width), F32)
                do_s[here, :] = dot(dh1, wo_ref[layer], 1, 1).astype(BF16)
                sum_s[...] = jnp.where(number == 0, 0.0, sum_s[...]) + dot(o_s[here, :].T, dh1)

            lax.fori_loop(0, n, tile, None, unroll=2)
            wo_o[...] = sum_s[...].astype(BF16).reshape(o_shape)

        heads = [slice(m * HEAD, (m + 1) * HEAD) for m in range(nh)]

        @at(last + 1)
        def _():
            load_qkv().wait()

            @pl.when(top)
            def _():
                for c in load_late():
                    c.wait()

            for j in range(0, t, ROWS):
                for h in heads:
                    kt_s[h, j : j + ROWS] = qkv_s[j : j + ROWS, width + h.start : width + h.stop].T

        @pl.when(phase > last)
        def _():
            i = per - 1 - phase
            here = tile_at(i)
            qs = [qkv_s[here, h] for h in heads]
            dos = [do_s[here, h] for h in heads]
            deltas = []
            for m, h in enumerate(heads):
                delta = (dos[m].astype(F32) * o_s[here, h].astype(F32)).sum(-1, keepdims=True)
                deltas.append(jnp.broadcast_to(delta, (ROWS, 128)).T[:1, :])
            lses = [lse_ref[layer, m : m + 1, here] for m in range(nh)]

            def block(keys, start, hide, first):
                span = slice(start, ROWS)
                scores = [dot(qkv_s[keys, width + h.start : width + h.stop], q[span, :], 1, 1) for h, q in zip(heads, qs)]
                dps = [dot(qkv_s[keys, 2 * width + h.start : 2 * width + h.stop], g[span, :], 1, 1) for h, g in zip(heads, dos)]
                for m, h in enumerate(heads):
                    p = jnp.exp2(scores[m] * LOG2E - lses[m][:, span])
                    if hide is not None:
                        p = jnp.where(hide, 0.0, p)
                    ds = (p * (dps[m] - deltas[m][:, span])).astype(BF16)
                    dv_s[keys, h] += dot(p.astype(BF16), dos[m][span, :])
                    dk_s[keys, h] += dot(ds, qs[m][span, :])
                    dq = dot(kt_s[h, keys], ds)
                    dq_s[h, span] = dq if first else dq_s[h, span] + dq

            wide = h_s[here, :].astype(F32)
            yt_s[:, here] = (wide * scale_of(wide)).astype(BF16).T
            half = ROWS // 2
            hide = hidden(ROWS)
            block(pl.ds(pl.multiple_of(i * ROWS, ROWS), half), 0, hide[:half, :], True)
            block(pl.ds(pl.multiple_of(i * ROWS + half, half), half), half, hide[:half, :half], False)
            lax.fori_loop(0, i, lambda j, _: block(tile_at(j), 0, None, False), None)
            cos, sin = angles(tab_ref, i)
            for h in heads:
                qkv_s[here, h] = rotated((dq_s[h, :] * HEAD**-0.5).astype(BF16).T.astype(F32), cos, -sin).astype(BF16)
                qkv_s[here, width + h.start : width + h.stop] = rotated(dk_s[here, h], cos, -sin).astype(BF16)
                qkv_s[here, 2 * width + h.start : 2 * width + h.stop] = dv_s[here, h].astype(BF16)

            @pl.when(top)
            def _():
                by = dot(qkv_s[here, : 3 * width], wqkv_s[...], 1, 1)
                wide = h_s[here, :].astype(F32)
                r = scale_of(wide)
                y = wide * r
                g_s[here, :] = (g_s[here, :].astype(F32) + normed_bwd(y, r, by)).astype(BF16)

            @pl.when(layer > 0)
            def _():
                for c in load_tile(layer - 1, i):
                    c.start()

        def qkvs(stage, of, which=(0, 1, 2)):
            for k in which:
                q_task.run(stage, Place(side), wqkv_o.at[k], gq_ref.at[of, :, k * width : (k + 1) * width], [r.at[k] for r in q_m])


        def both(chunk, stage):
            slot, source = lax.rem(chunk, SLOTS), lax.rem(chunk, 2)
            d_task.run(stage, Place(side), chunk, d_o.at[source], gd_ref.at[layer], [r.at[slot] for r in d_m])
            gu_task.run(stage, Place(side), gu_o.at[source], ggu_ref.at[layer, chunk], [r.at[slot] for r in gu_m])

        def out(stage):
            o_task.run(stage, Place(side), wo_o, go_ref.at[layer], o_m)

        when = [[], [c + 2 for c in range(side)], [c + 3 for c in range(side)], [c + 4 for c in range(side - 1)]]
        when[1][-1] = last + 1
        when[2][-2:] = last, last + 2
        when[3][-2:] = last, last + 1

        for stage in (2, 3, 1):

            @pl.when(functools.reduce(jnp.logical_or, [phase == p for p in when[stage]]))
            def _():
                both(sum(jnp.where(phase == p, c, 0) for c, p in enumerate(when[stage])), stage)

        for stage in range(3):
            at(last + stage)(lambda: out(stage))
        for stage in range(1, 4):
            at(stage, ~top)(lambda: qkvs(stage, layer + 1))

        @pl.when(hidden_units)
        def _():
            slot = lax.rem(chunk, 2)
            dv_s[tile_at(chunk, t // side), :] = jnp.zeros((t // side, width), F32)
            for c in range(0, 2 * cut, cut):
                gu_o[slot, :, :, :, c : c + cut] = dot(bt_s[...], dgu_s[:, c : c + cut]).astype(BF16).reshape(*gu_shape[:3], cut)
            d_o[slot] = dot(gt_s[...], act_s[:, 2 * cut : 3 * cut]).astype(BF16).T.reshape(d_shape)
            both(chunk, 0)

        @at(per - 1)
        def _():
            for k in range(3):
                wqkv_o[k] = dot(yt_s[...], qkv_s[:, k * width : (k + 1) * width]).astype(BF16).reshape(q_shape)
                qkvs(0, layer, (k,))
                rows = slice(t * k // 3 // 8 * 8, t * (k + 1) // 3 // 8 * 8)
                by_s[rows, :] = jnp.zeros((rows.stop - rows.start, d), F32)
            both(side - 1, 3)
            out(3)

        @pl.when(step == layers * per - 1)
        def _():
            place = Place(side)
            mine = sum(square(gq_ref[k]) for k in range(1, layers))
            for k in range(layers):
                mine += square(go_ref[k]) + square(gd_ref[k])
                for c in range(side):
                    mine += square(ggu_ref[k, c])
            qkvs(1, 0)
            qkvs(2, 0)
            qkvs(3, 0)
            mine = jnp.broadcast_to(mine + square(gq_ref[0]), part.shape)
            part[...] = mine
            slots[place.me] = mine
            for device in place.others():
                remote(part, slots.at[place.me], send.at[0], recv.at[0], device).start()
            arrived(slots.at[: group - 1], send.at[0], recv.at[0], place.others()[0])
            total_ref[...] = slots[...].sum(0)

    outs = [sds((layers, q_shape[2], 3 * width), BF16), sds((layers, o_shape[2], d), BF16), sds((layers, side, *gu_shape[2:]), BF16),
            sds((layers, *d_shape[1:]), BF16), sds((8, 128), F32)]
    return pl.pallas_call(
        body,
        grid=(layers * per,),
        in_specs=[ANY] * 9,
        out_specs=[whole(a.shape) for a in outs],
        out_shape=outs,
        scratch_shapes=[*own, *moves],
        compiler_params=pltpu.CompilerParams(dimension_semantics=("arbitrary",), vmem_limit_bytes=VMEM, has_side_effects=True, collective_id=cid),
        name="backward",
    )(h, o, lse, wqkv, wgu, wd, dy, qkv, tab)


def adamw(total, count, weights, m, v, gq, go, ggu, gd):
    layers, side = ggu.shape[:2]

    def body(total_ref, gq_ref, go_ref, ggu_ref, gd_ref, *refs):
        w_refs, m_refs, v_refs, wn_refs, mn_refs, vn_refs = taken(refs, *[7] * 6)
        factor = jnp.minimum(1.0, 0.5 * lax.rsqrt(total_ref[0:1, 0:1] / count + 1e-30))

        def update(i, columns, g):
            g = g.astype(F32) * factor
            at = (0, slice(None), columns)
            mn = 0.9 * m_refs[i][at] + 0.1 * g
            vn = 0.95 * v_refs[i][at] + 0.05 * g * g
            mn_refs[i][at], vn_refs[i][at] = mn, vn
            w = w_refs[i][at].astype(F32)
            wn_refs[i][at] = (w - 0.02 * (mn * lax.rsqrt(vn + 1e-8) + 0.1 * w)).astype(BF16)

        every = slice(None)
        wide = gq_ref.shape[2] // 3
        for i in range(3):
            update(i, every, gq_ref[0, :, i * wide : (i + 1) * wide])
        update(3, every, go_ref[0])
        cut = ggu_ref.shape[3] // 2
        for c in range(side):
            for i in range(2):
                update(4 + i, slice(c * cut, (c + 1) * cut), ggu_ref[0, c, :, i * cut : (i + 1) * cut])
        update(6, every, gd_ref[0])

    one = lambda a: pl.BlockSpec((1, *a.shape[1:]), lambda l: (l,) + (0,) * (a.ndim - 1))
    own = [one(a) for a in weights]
    return pl.pallas_call(
        body,
        grid=(layers,),
        in_specs=[whole(total.shape), *(one(a) for a in (gq, go, ggu, gd)), *own * 3],
        out_specs=own * 3,
        out_shape=[*(sds(a.shape, BF16) for a in weights), *(sds(a.shape, F32) for a in (*m, *v))],
        compiler_params=pltpu.CompilerParams(dimension_semantics=("arbitrary",), vmem_limit_bytes=VMEM),
        name="adamw",
    )(total, gq, go, ggu, gd, *weights, *m, *v)


def solution(mesh):
    group = mesh.shape["dp"]
    side = side_of(group)

    def step(x, dy, *arrays):
        weights, m, v = (arrays[i : i + 7] for i in (0, 7, 14))
        x, dy = x[0], dy[0]
        qkv, o, lse, h, wqkv, wgu, wd = forward(0, side, x, weights)
        *grads, total = backward(1, side, h, dy, qkv, o, lse, wqkv, wgu, wd)
        return tuple(adamw(total, group * sum(w.size for w in weights), weights, m, v, *grads))

    states, cut = P(("rep", "dp"), None, None), P(None, "dp", None)
    return jax.shard_map(
        step,
        mesh=mesh,
        in_specs=(states, states) + (cut,) * 21,
        out_specs=(P("rep", "dp", None),) * 21,
        check_vma=False,
    )
```
